128 devices in a mesh: tp: 8 (over y, x_hi), dp: 16 (over z, x_lo, core).
Axes of the slice: x: 4 (x_hi: 2, x_lo: 2; x = x_hi * 2 + x_lo), y: 4, z: 4, core: 2. Of those that a mesh axis runs over, the one named last changes fastest.
Arguments:
- activations: bfloat16 [2, 16384, 8192], P(None, 'dp', 'tp'), may hold values from -72 to 72
- out_grads: bfloat16 [2, 16384, 2048], P(None, 'dp'), may hold values from -2 to 2
- master: float32 [8192, 2, 2048], P(('tp', 'dp')), may hold values from -1.2 to 1.2
- first_moment: float32 [8192, 2, 2048], P(('tp', 'dp')), may hold values from -1.8 to 1.8
- second_moment: float32 [8192, 2, 2048], P(('tp', 'dp')), may hold values from 0.01 to 1
Outputs:
- new_master: float32 [8192, 2, 2048], P(('tp', 'dp'))
- new_first: float32 [8192, 2, 2048], P(('tp', 'dp'))
- new_second: float32 [8192, 2, 2048], P(('tp', 'dp'))
- weights: bfloat16 [8192, 2, 2048], P('tp')
The draws below stay inside these ranges and needn't reach their ends.
All inputs are finite; a program needn't handle non-finite values.
Results may differ from the reference program's by a relative error of at most 0.0004.
Values may be sent and summed in bfloat16 or wider, within the bound.
A program may use at most 128 MiB of HBM per device.

```python
import math
import jax
import jax.numpy as jnp

D = 8192
KVW = 2048
LAYERS = 2
TOKENS = 16384


def shared_signs(key):
    sign_bits = jax.random.randint(jax.random.fold_in(key, 101), (LAYERS, TOKENS), 0, 2)
    return (2 * sign_bits - 1).astype(jnp.float32)


def draw_activations(key, part):
    token_signs = shared_signs(key)
    noise_key = jax.random.fold_in(key, 202)
    along_key = jax.random.fold_in(key, 203)
    noise = jnp.clip(jax.random.normal(noise_key, (LAYERS, TOKENS, D), jnp.float32), -6.0, 6.0)
    direction = jnp.clip(jax.random.normal(along_key, (LAYERS, D), jnp.float32), -3.0, 3.0)
    strength = 8.0
    values = 8.0 * noise + strength * token_signs[:, :, None] * direction[:, None, :]
    return values.astype(jnp.bfloat16)


def draw_out_grads(key, part):
    token_signs = shared_signs(key)
    noise_key = jax.random.fold_in(key, 302)
    along_key = jax.random.fold_in(key, 303)
    noise = jnp.clip(jax.random.normal(noise_key, (LAYERS, TOKENS, KVW), jnp.float32), -6.0, 6.0)
    direction = jnp.clip(jax.random.normal(along_key, (LAYERS, KVW), jnp.float32), -3.0, 3.0)
    values = noise * TOKENS ** (-0.5) + token_signs[:, :, None] * direction[:, None, :] * (1.0 / TOKENS)
    return values.astype(jnp.bfloat16)


def block_scale(own_key, shape, split, smallest, high):
    factor_of = 1.0
    for dim, blocks in split:
        steps = jax.random.uniform(jax.random.fold_in(jax.random.fold_in(own_key, 6), dim), (blocks,), jnp.float32, smallest / len(split), high / len(split))
        factor_of = factor_of * jnp.repeat(jnp.exp(steps), shape[dim] // blocks).reshape((-1,) + (1,) * (len(shape) - 1 - dim))
    return factor_of


def centred(key, dims, width, reach, pieces=(), dtype=jnp.bfloat16):
    values = width * jax.random.normal(key, dims, jnp.float32)
    if pieces:
        values = values * block_scale(key, dims, pieces, -0.22, 0.18)
    return jnp.clip(values, -reach, reach).astype(dtype)


def setup_inputs(seed: int = 0) -> dict:
    keys = jax.random.split(jax.random.key(seed), 6)
    return {
        "activations": draw_activations(jax.random.fold_in(keys[5], 71), 0),
        "out_grads": draw_out_grads(jax.random.fold_in(keys[5], 71), 0),
        "master": centred(keys[2], (D, LAYERS, KVW), 0.2, 1.2, ((0, 128),), jnp.float32),
        "first_moment": centred(keys[3], (D, LAYERS, KVW), 0.3, 1.8, ((0, 128),), jnp.float32),
        "second_moment": jnp.clip(jnp.exp(math.log(1.0) - 4.6051702 * jax.random.uniform(keys[4], (D, LAYERS, KVW), jnp.float32) ** block_scale(keys[4], (D, LAYERS, KVW), ((0, 128),), -0.2, 0.2)), 0.01, 1.0),
    }


beta_first = 0.9
beta_second = 0.95
first_fix = 1.0 - 0.9 ** 10
second_fix = 1.0 - 0.95 ** 10
learn_rate = 0.01
decay_rate = 0.1
epsilon = 1e-08
limit_scale = 2.0

def reference(activations, out_grads, master, first_moment, second_moment):
    grad = jnp.einsum('ltd,ltc->dlc', activations.astype(jnp.float32), out_grads.astype(jnp.float32))
    squares = jnp.sum(grad * grad)
    limit = limit_scale * math.sqrt(D * LAYERS * KVW)
    clip_factor = limit / jnp.maximum(jnp.sqrt(squares), limit)
    clipped = clip_factor * grad
    new_first = beta_first * first_moment + (1.0 - beta_first) * clipped
    new_second = beta_second * second_moment + (1.0 - beta_second) * clipped * clipped
    step_dir = new_first / first_fix / (jnp.sqrt(new_second / second_fix) + epsilon)
    new_master = master - learn_rate * (step_dir + decay_rate * master)
    return (new_master, new_first, new_second, new_master.astype(jnp.bfloat16))
```

```python
import functools
import math

import jax
import jax.numpy as jnp
from jax import lax
from jax.experimental import pallas as pl
from jax.experimental.pallas import tpu as pltpu
from jax.sharding import Mesh
from jax.sharding import PartitionSpec as P

DP = ("dp_0", "dp_1", "dp_2")
TP_DP = ("tp_0", "tp_1", "dp_0", "dp_1", "dp_2")
TP = ("tp_0", "tp_1")
MESH = pl.DeviceIdType.MESH
F32 = jnp.float32
BF16 = jnp.bfloat16


beta_first = 0.9
beta_second = 0.95
first_fix = 1.0 - 0.9**10
second_fix = 1.0 - 0.95**10
learn_rate = 0.01
decay_rate = 0.1
epsilon = 1e-08
limit_scale = 2.0

OWN = 64
WIDE = 256
HALF = WIDE // 2
STEPS = 8
LANES = 128
GATHERS = 4
X_ROWS = 288
Z_ROWS = 224
SUB = 32
TOP = 2.0**120
TINY = 1e-37


def encode(value):
    square = value * value
    fourth = square * square
    return (fourth * (square * (value * jnp.abs(value)))).astype(BF16)


def decode(code):
    power = code.astype(F32)
    half = lax.rsqrt(jnp.maximum(jnp.abs(power), TINY))
    eighth = lax.rsqrt(lax.rsqrt(half))
    return (power * half) * (eighth * (eighth * eighth))


def kernel(
    acts_hbm, grads_hbm, master_hbm, first_hbm, second_hbm,
    master_out, first_out, second_out, weights_out,
    acts, turned, outs, master, first, second, own_grad,
    pair_send, pair_recv, total,
    x1_send, x1_recv, xz1_send, xz1_recv, xz2_send, xz2_recv,
    zz1_send, zz1_recv, zz2_send, zz2_recv, zx_send, zx_recv,
    bound, bounds, norm_dp, norm_tp,
    load_sem, out_sem, state_sem, pair_ssem, pair_rsem, x1_ssem, x1_rsem, xz1_ssem, xz1_rsem, xz2_ssem, xz2_rsem,
    zz1_ssem, zz1_rsem, zz2_ssem, zz2_rsem, zx_ssem, zx_rsem,
    bound_ssem, bound_rsem, ndp_ssem, ndp_rsem, ntp_ssem, ntp_rsem,
    gx_ssem, gx_rsem, gz_ssem, gz_rsem, gd_ssem, gd_rsem,
):
    ny, nh = lax.axis_size("tp_0"), lax.axis_size("tp_1")
    y, h = lax.axis_index("tp_0"), lax.axis_index("tp_1")
    z, x, c = lax.axis_index("dp_0"), lax.axis_index("dp_1"), lax.axis_index("dp_2")
    nt = ny * nh
    dp_me = z * 4 + x * 2 + c
    tp_me = y * nh + h
    za, zb, zo = lax.rem(z + 1, 4), lax.rem(z + 3, 4), lax.rem(z + 2, 4)
    xo = 1 - x
    tokens = acts_hbm.shape[1]
    to_core = {"dp_2": 1 - c}
    to_x = {"dp_1": xo}
    to_za = {"dp_0": za}
    to_zb = {"dp_0": zb}

    def dp_of(k):
        other = lax.rem(dp_me + k, 16)
        return other, {"dp_0": other // 4, "dp_1": lax.rem(other // 2, 2), "dp_2": lax.rem(other, 2)}

    def tp_of(k):
        other = lax.rem(tp_me + k, nt)
        return other, {"tp_0": other // nh, "tp_1": lax.rem(other, nh)}

    def remote(src, dst, ssem, rsem, device):
        return pltpu.make_async_remote_copy(
            src_ref=src, dst_ref=dst, send_sem=ssem, recv_sem=rsem, device_id=device, device_id_type=MESH
        )

    def acts_load(l):
        return pltpu.make_async_copy(acts_hbm.at[l], acts.at[l], load_sem.at[l])

    def outs_load(i):
        return pltpu.make_async_copy(
            grads_hbm.at[i // 4, :, pl.ds(pl.multiple_of(lax.rem(i, 4) * (2 * WIDE), 2 * WIDE), 2 * WIDE)],
            outs.at[i],
            out_sem.at[i],
        )

    states = (
        pltpu.make_async_copy(master_hbm, master, state_sem.at[0]),
        pltpu.make_async_copy(first_hbm, first, state_sem.at[1]),
        pltpu.make_async_copy(second_hbm, second, state_sem.at[2]),
    )
    acts_load(0).start()
    outs_load(0).start()
    acts_load(1).start()

    def start_outs(i, carry):
        outs_load(i).start()
        return carry

    lax.fori_loop(1, STEPS, start_outs, 0)
    for copy in states:
        copy.start()

    barrier = pltpu.get_barrier_semaphore()

    def greet_dp(k, carry):
        pl.semaphore_signal(barrier, inc=1, device_id=dp_of(k)[1], device_id_type=MESH)
        return carry

    def greet_tp(k, carry):
        pl.semaphore_signal(barrier, inc=1, device_id=tp_of(k)[1], device_id_type=MESH)
        return carry

    lax.fori_loop(1, 16, greet_dp, 0)
    lax.fori_loop(1, nt, greet_tp, 0)

    def turn(l):
        for q in range(8):
            flipped = acts[l, :, q * LANES : (q + 1) * LANES].T
            turned[l, 0, q * OWN : (q + 1) * OWN, :] = flipped[:OWN]
            turned[l, 1, q * OWN : (q + 1) * OWN, :] = flipped[OWN:]

    def largest(ref, lead):
        rows, wide = ref.shape[1], ref.shape[2]

        def step(r, best):
            part = jnp.abs(ref[lead, pl.ds(pl.multiple_of(r * 64, 64), 64), :])
            return jnp.maximum(best, jnp.max(part.reshape(4, 16, wide), axis=0))

        return lax.fori_loop(0, rows // 64, step, jnp.zeros((16, wide), BF16))

    acts_load(0).wait()
    turn(0)

    def product(l, core, i, p):
        return jnp.dot(
            turned[l, core], outs[i, :, p * WIDE : (p + 1) * WIDE], preferred_element_type=F32
        ).reshape(8, OWN, WIDE)

    def pair_copy(i, p):
        slot = lax.rem(i, 2)
        return remote(
            pair_send.at[slot, p], pair_recv.at[i, p], pair_ssem.at[slot, p], pair_rsem.at[i, p], to_core
        )

    def multiply(i):
        l = i // 4

        @pl.when(i >= 2)
        def _():
            for p in range(2):
                pair_copy(i - 2, p).wait_send()

        slot = lax.rem(i, 2)
        pair_send[slot, 0] = product(l, 1 - c, i, 0)
        pair_send[slot, 1] = product(l, 1 - c, i, 1)
        pair_copy(i, 0).start()
        total[i, 0] = product(l, c, i, 0)
        pair_copy(i, 1).start()
        total[i, 1] = product(l, c, i, 1)

    outs_load(0).wait()
    pl.semaphore_wait(barrier, 15 + nt - 1)
    multiply(0)

    acts_load(1).wait()
    biggest_act = jnp.maximum(jnp.max(largest(acts, 0).astype(F32)), jnp.max(largest(acts, 1).astype(F32)))
    best = largest(outs, 0)

    def widen(i, best):
        outs_load(i).wait()
        return jnp.maximum(best, largest(outs, i))

    best = lax.fori_loop(1, STEPS, widen, best)
    biggest_out = jnp.max(best.astype(F32))
    own_bound = jnp.maximum(biggest_act * biggest_out * (1.01 * tokens), 1e-30)
    bounds[dp_me] = jnp.full((8, LANES), own_bound, F32)
    bound[...] = jnp.full((8, LANES), own_bound, F32)

    def bound_copy(k):
        return remote(bound, bounds.at[dp_me], bound_ssem.at[k], bound_rsem.at[dp_me], dp_of(k)[1])

    def bound_send(k, carry):
        bound_copy(k).start()
        return carry

    lax.fori_loop(1, 16, bound_send, 0)
    turn(1)

    def bound_wait(other):
        remote(bound, bounds.at[other], bound_ssem.at[0], bound_rsem.at[other], to_core).wait_recv()

    bound_wait(z * 4 + x * 2 + 1 - c)

    top = TOP ** 0.125
    chip_bound = (bounds[dp_me] + bounds[z * 4 + x * 2 + 1 - c])[0:1, 0:1]
    chip_scale = top / chip_bound

    def paired(i, p, q):
        return total[i, p, q] + pair_recv[i, p, q]

    def x1_copy(i):
        return remote(x1_send.at[i], x1_recv.at[i], x1_ssem.at[i], x1_rsem.at[i], to_x)

    def z_copies(send, recv, ssem, rsem, i):
        return (
            remote(send.at[i, 0], recv.at[i, 0], ssem.at[i, 0], rsem.at[i, 0], to_za),
            remote(send.at[i, 1], recv.at[i, 1], ssem.at[i, 1], rsem.at[i, 1], to_zb),
        )

    def xz1_copies(i):
        return z_copies(xz1_send, xz1_recv, xz1_ssem, xz1_rsem, i)

    def xz2_copies(i):
        return z_copies(xz2_send, xz2_recv, xz2_ssem, xz2_rsem, i)

    def zz1_copies(i):
        return z_copies(zz1_send, zz1_recv, zz1_ssem, zz1_rsem, i)

    def zz2_copies(i):
        return z_copies(zz2_send, zz2_recv, zz2_ssem, zz2_rsem, i)

    def zx_copy(i):
        return remote(zx_send.at[i], zx_recv.at[i], zx_ssem.at[i], zx_rsem.at[i], to_x)

    lo, hi = slice(0, HALF), slice(HALF, WIDE)

    def stage_one(i):
        pair_copy(i, 0).wait_recv()
        for zz in range(4):
            x1_send[i, zz] = encode(paired(i, 0, zz * 2 + xo) * chip_scale)
        x1_copy(i).start()
        pair_copy(i, 1).wait_recv()
        for xx in range(2):
            far = encode(paired(i, 1, zo * 2 + xx) * chip_scale)
            zz1_send[i, 0, 0, xx] = far[:, lo]
            zz1_send[i, 1, 0, xx] = far[:, hi]
            q = za * 2 + xx
            zz1_send[i, 0, 1, xx] = encode((total[i, 1, q, :, hi] + pair_recv[i, 1, q, :, hi]) * chip_scale)
            q = zb * 2 + xx
            zz1_send[i, 1, 1, xx] = encode((total[i, 1, q, :, lo] + pair_recv[i, 1, q, :, lo]) * chip_scale)
        for copy in zz1_copies(i):
            copy.start()

    def first_loop(i, carry):
        multiply(i)
        stage_one(i - 1)
        return carry

    lax.fori_loop(1, STEPS, first_loop, 0)
    stage_one(STEPS - 1)

    def bound_rest(k, carry):
        other = lax.rem(dp_me + k, 16)

        @pl.when(other != z * 4 + x * 2 + 1 - c)
        def _():
            bound_wait(other)

        return carry

    lax.fori_loop(1, 16, bound_rest, 0)

    def bound_of(zz, xx):
        return (bounds[zz * 4 + xx * 2] + bounds[zz * 4 + xx * 2 + 1])[0:1, 0:1]

    from_x = bound_of(z, xo) * (1.0 / top)
    from_zb = bound_of(zb, x) * (1.0 / top)
    from_za = bound_of(za, x) * (1.0 / top)
    whole = jnp.sum(bounds[...], axis=0)[0:1, 0:1] * 1.01
    scale = top / whole
    unscale = whole * (1.0 / top)

    def stage_two(i):
        x1_copy(i).wait_recv()
        for zz in range(4):
            q = zz * 2 + x
            total[i, 0, q] = paired(i, 0, q) + decode(x1_recv[i, zz]) * from_x
        far = encode(total[i, 0, zo * 2 + x] * scale)
        xz1_send[i, 0, 0] = far[:, lo]
        xz1_send[i, 1, 0] = far[:, hi]
        xz1_send[i, 0, 1] = encode(total[i, 0, za * 2 + x, :, hi] * scale)
        xz1_send[i, 1, 1] = encode(total[i, 0, zb * 2 + x, :, lo] * scale)
        for copy in xz1_copies(i):
            copy.start()
        for copy in zz1_copies(i):
            copy.wait_recv()
        for xx in range(2):
            q = za * 2 + xx
            mine = total[i, 1, q, :, lo] + pair_recv[i, 1, q, :, lo]
            zz2_send[i, 0, xx] = encode((mine + decode(zz1_recv[i, 0, 0, xx]) * from_zb) * scale)
            q = zb * 2 + xx
            mine = total[i, 1, q, :, hi] + pair_recv[i, 1, q, :, hi]
            zz2_send[i, 1, xx] = encode((mine + decode(zz1_recv[i, 1, 0, xx]) * from_za) * scale)
        for copy in zz2_copies(i):
            copy.start()

    def stage_three(i):
        for copy in zz2_copies(i):
            copy.wait_recv()

        def summed(xx):
            q = z * 2 + xx
            low = (
                total[i, 1, q, :, lo] + pair_recv[i, 1, q, :, lo]
                + decode(zz1_recv[i, 1, 1, xx]) * from_za + decode(zz2_recv[i, 0, xx]) * unscale
            )
            high = (
                total[i, 1, q, :, hi] + pair_recv[i, 1, q, :, hi]
                + decode(zz1_recv[i, 0, 1, xx]) * from_zb + decode(zz2_recv[i, 1, xx]) * unscale
            )
            return low, high

        low, high = summed(xo)
        zx_send[i, :, lo] = encode(low * scale)
        zx_send[i, :, hi] = encode(high * scale)
        zx_copy(i).start()
        for copy in xz1_copies(i):
            copy.wait_recv()
        xz2_send[i, 0] = encode(total[i, 0, za * 2 + x, :, lo] * scale + decode(xz1_recv[i, 0, 0]))
        xz2_send[i, 1] = encode(total[i, 0, zb * 2 + x, :, hi] * scale + decode(xz1_recv[i, 1, 0]))
        for copy in xz2_copies(i):
            copy.start()
        low, high = summed(x)
        total[i, 1, z * 2 + x, :, lo] = low
        total[i, 1, z * 2 + x, :, hi] = high

    def put(i, j, value):
        base = (lax.rem(i, 4) * 4 + j) * 2 + i // 4
        for r in range(OWN // 8):
            own_grad[pl.ds(base + r * 8 * 32, 8, stride=32), :] = value[r * 8 : (r + 1) * 8]
        return jnp.sum((value * value).reshape(OWN // 8, 8, LANES), axis=0)

    def final(i, squares):
        for copy in xz2_copies(i):
            copy.wait_recv()
        q = z * 2 + x
        g = total[i, 0, q, :, lo] + (decode(xz1_recv[i, 1, 1]) + decode(xz2_recv[i, 0])) * unscale
        squares = squares + put(i, 0, g)
        g = total[i, 0, q, :, hi] + (decode(xz1_recv[i, 0, 1]) + decode(xz2_recv[i, 1])) * unscale
        squares = squares + put(i, 1, g)
        zx_copy(i).wait_recv()
        g = total[i, 1, q] + decode(zx_recv[i]) * unscale
        squares = squares + put(i, 2, g[:, lo])
        return squares + put(i, 3, g[:, hi])

    stage_two(0)
    stage_two(1)
    stage_three(0)

    def second_loop(i, squares):
        stage_two(i)
        stage_three(i - 1)
        return final(i - 2, squares)

    squares = lax.fori_loop(2, STEPS, second_loop, jnp.zeros((8, LANES), F32))
    stage_three(STEPS - 1)
    squares = final(STEPS - 2, squares)
    squares = final(STEPS - 1, squares)

    norm_dp[dp_me] = squares

    def ndp_copy(k, slot):
        return remote(norm_dp.at[slot], norm_dp.at[slot], ndp_ssem.at[k], ndp_rsem.at[slot], dp_of(k)[1])

    def ntp_copy(k, slot):
        return remote(norm_tp.at[slot], norm_tp.at[slot], ntp_ssem.at[k], ntp_rsem.at[slot], tp_of(k)[1])

    def exchange(copy, count, me):
        def send(k, carry):
            copy(k, me).start()
            return carry

        def receive(k, carry):
            copy(k, lax.rem(me + k, count)).wait_recv()
            return carry

        lax.fori_loop(1, count, send, 0)
        lax.fori_loop(1, count, receive, 0)

    exchange(ndp_copy, 16, dp_me)
    norm_tp[tp_me] = jnp.sum(norm_dp[...], axis=0)
    for copy in states:
        copy.wait()
    exchange(ntp_copy, nt, tp_me)
    sum_squares = jnp.sum(jnp.sum(norm_tp[...], axis=0), keepdims=True)
    entries = OWN * 16 * nt * 2 * 2048
    limit = limit_scale * math.sqrt(entries)
    clip_factor = limit / jnp.maximum(jnp.sqrt(sum_squares), limit)

    def update(start):
        rows = pl.ds(pl.multiple_of(start, SUB), SUB)
        clipped = clip_factor * own_grad[rows, :]
        new_first = beta_first * first[rows, :] + (1.0 - beta_first) * clipped
        new_second = beta_second * second[rows, :] + (1.0 - beta_second) * clipped * clipped
        step_dir = new_first * (1.0 / first_fix) / (jnp.sqrt(new_second * (1.0 / second_fix)) + epsilon)
        old = master[rows, :]
        new_master = old - learn_rate * (step_dir + decay_rate * old)
        first_out[rows, :] = new_first
        second_out[rows, :] = new_second
        master_out[rows, :] = new_master
        weights_out[dp_me, rows, :] = new_master.astype(BF16)

    def x_part(k):
        return pl.ds(pl.multiple_of(k * X_ROWS, 16), X_ROWS)

    def z_part(k):
        return pl.ds(pl.multiple_of(GATHERS * X_ROWS + k * Z_ROWS, 16), Z_ROWS)

    def x_half(k, n):
        return pl.ds(pl.multiple_of(k * X_ROWS + n * (X_ROWS // 2), 16), X_ROWS // 2)

    def z_half(k, n):
        return pl.ds(pl.multiple_of(GATHERS * X_ROWS + k * Z_ROWS + n * (Z_ROWS // 2), 16), Z_ROWS // 2)

    def move(zz, xx, rows, ssem, rsem, device):
        place = weights_out.at[zz * 4 + xx * 2 + c, rows, :]
        return remote(place, place, ssem, rsem, device)

    def gx(k, n, zz, xx, rows):
        return move(zz, xx, rows, gx_ssem.at[k, n], gx_rsem.at[k, n], to_x)

    def gz(k, n, zz, xx, rows, device):
        return move(zz, xx, rows, gz_ssem.at[k, n], gz_rsem.at[k, n], device)

    def gd(zz, xx, rows):
        return move(zz, xx, rows, gd_ssem, gd_rsem, to_core)

    def x_own(k, xx):
        return gx(k, 0, z, xx, x_part(k))

    def z_cross(k, n, zz, xx):
        return gx(k, 1 + n, zz, xx, z_part(k))

    def x_spread(k, xx, zz_a, zz_b, n):
        return (
            gz(k, n, zz_a, xx, x_part(k), to_za),
            gz(k, n + 1, zz_b, xx, x_part(k), to_zb),
        )

    def x_halves(k, xx, zz_a, zz_b, n):
        return (
            gz(k, n, zz_a, xx, x_half(k, 0), to_za),
            gz(k, n + 1, zz_b, xx, x_half(k, 1), to_zb),
        )

    def z_spread(k, zz_a, zz_b):
        return (
            gz(k, 8, zz_a, x, z_part(k), to_za),
            gz(k, 9, zz_b, x, z_part(k), to_zb),
        )

    def z_halves(k, zz_a, zz_b):
        return (
            gz(k, 10, zz_a, x, z_half(k, 0), to_za),
            gz(k, 11, zz_b, x, z_half(k, 1), to_zb),
        )

    def update_loop(k, carry):
        def in_x(s, carry):
            update(k * X_ROWS + s * SUB)
            return carry

        def in_z(s, carry):
            update(GATHERS * X_ROWS + k * Z_ROWS + s * SUB)
            return carry

        lax.fori_loop(0, X_ROWS // SUB, in_x, 0)
        x_own(k, x).start()
        gd(z, x, x_part(k)).start()
        lax.fori_loop(0, Z_ROWS // SUB, in_z, 0)
        for copy in z_spread(k, z, z):
            copy.start()
        gd(z, x, z_part(k)).start()
        return carry

    lax.fori_loop(0, GATHERS, update_loop, 0)

    def own_loop(k, carry):
        z_cross(k, 0, z, x).start()
        for copy in x_spread(k, x, z, z, 0):
            copy.start()
        return carry

    lax.fori_loop(0, GATHERS, own_loop, 0)

    def hop_one(k):
        x_own(k, xo).wait_recv()
        for copy in x_spread(k, xo, z, z, 2):
            copy.start()
        gd(z, xo, x_part(k)).start()
        from_below, from_above = z_spread(k, zb, za)
        halves = z_halves(k, zb, za)
        from_below.wait_recv()
        halves[0].start()
        z_cross(k, 1, zb, x).start()
        gd(zb, x, z_part(k)).start()
        from_above.wait_recv()
        halves[1].start()
        z_cross(k, 2, za, x).start()
        gd(za, x, z_part(k)).start()

    def hop_two(k):
        for xx, n in ((x, 0), (xo, 2)):
            from_below, from_above = x_spread(k, xx, zb, za, n)
            halves = x_halves(k, xx, zb, za, 4 + n)
            from_below.wait_recv()
            halves[0].start()
            gd(zb, xx, x_part(k)).start()
            from_above.wait_recv()
            halves[1].start()
            gd(za, xx, x_part(k)).start()
        for copy in z_halves(k, zo, zo):
            copy.wait_recv()
        z_cross(k, 3, zo, x).start()
        gd(zo, x, z_part(k)).start()

    def hop_three(k):
        for n, zz in ((0, z), (1, zb), (2, za), (3, zo)):
            z_cross(k, n, zz, xo).wait_recv()
            gd(zz, xo, z_part(k)).start()
        for xx, n in ((x, 0), (xo, 2)):
            for copy in x_halves(k, xx, zo, zo, 4 + n):
                copy.wait_recv()
            gd(zo, xx, x_part(k)).start()

    hop_one(0)
    hop_one(1)
    hop_two(0)

    def gather_loop(k, carry):
        hop_one(k)
        hop_two(k - 1)
        hop_three(k - 2)
        return carry

    lax.fori_loop(2, GATHERS, gather_loop, 0)
    hop_two(GATHERS - 1)
    hop_three(GATHERS - 2)
    hop_three(GATHERS - 1)

    def drain_steps(i, carry):
        x1_copy(i).wait_send()
        zx_copy(i).wait_send()
        for copies in (xz1_copies, xz2_copies, zz1_copies, zz2_copies):
            for copy in copies(i):
                copy.wait_send()
        return carry

    def drain_gather(k, carry):
        x_own(k, x).wait_send()
        for n in range(4):
            z_cross(k, n, z, x).wait_send()
        for n in (0, 2):
            for copy in x_spread(k, x, z, z, n) + x_halves(k, x, z, z, 4 + n):
                copy.wait_send()
        for copy in z_spread(k, z, z) + z_halves(k, z, z):
            copy.wait_send()
        return carry

    def drain_dp(k, carry):
        bound_copy(k).wait_send()
        ndp_copy(k, dp_me).wait_send()
        return carry

    def drain_tp(k, carry):
        ntp_copy(k, tp_me).wait_send()
        return carry

    for i in (STEPS - 2, STEPS - 1):
        for p in range(2):
            pair_copy(i, p).wait_send()
    lax.fori_loop(0, STEPS, drain_steps, 0)
    lax.fori_loop(0, GATHERS, drain_gather, 0)
    lax.fori_loop(1, 16, drain_dp, 0)
    lax.fori_loop(1, nt, drain_tp, 0)
    everything = weights_out.at[pl.ds(0, 8)]
    passed = remote(everything, everything, gd_ssem, gd_rsem, to_core)
    passed.wait_send()
    passed.wait_recv()


def fused(acts, grads, master, first, second):
    tokens = acts.shape[1]
    rows = OWN * 32
    dma = pltpu.SemaphoreType.DMA
    vmem = pltpu.VMEM
    scratch = [
        vmem((2, tokens, 1024), BF16),
        vmem((2, 2, 512, tokens), BF16),
        vmem((STEPS, tokens, 2 * WIDE), BF16),
        vmem((rows, LANES), F32),
        vmem((rows, LANES), F32),
        vmem((rows, LANES), F32),
        vmem((rows, LANES), F32),
        vmem((2, 2, 8, OWN, WIDE), F32),
        vmem((STEPS, 2, 8, OWN, WIDE), F32),
        vmem((STEPS, 2, 8, OWN, WIDE), F32),
    ]
    for shape in (
        (STEPS, 4, OWN, WIDE),
        (STEPS, 2, 2, OWN, HALF),
        (STEPS, 2, OWN, HALF),
        (STEPS, 2, 2, 2, OWN, HALF),
        (STEPS, 2, 2, OWN, HALF),
        (STEPS, OWN, WIDE),
    ):
        scratch += [vmem(shape, BF16), vmem(shape, BF16)]
    tp = lax.axis_size("tp_0") * lax.axis_size("tp_1")
    scratch += [
        vmem((8, LANES), F32),
        vmem((16, 8, LANES), F32),
        vmem((16, 8, LANES), F32),
        vmem((tp, 8, LANES), F32),
        dma((2,)), dma((STEPS,)), dma((3,)),
        dma((2, 2)), dma((STEPS, 2)),
        dma((STEPS,)), dma((STEPS,)),
        dma((STEPS, 2)), dma((STEPS, 2)),
        dma((STEPS, 2)), dma((STEPS, 2)),
        dma((STEPS, 2)), dma((STEPS, 2)),
        dma((STEPS, 2)), dma((STEPS, 2)),
        dma((STEPS,)), dma((STEPS,)),
        dma((16,)), dma((16,)),
        dma((16,)), dma((16,)),
        dma((tp,)), dma((tp,)),
        dma((GATHERS, 5)), dma((GATHERS, 5)),
        dma((GATHERS, 12)), dma((GATHERS, 12)),
        dma, dma,
    ]
    anywhere = pl.BlockSpec(memory_space=pl.ANY)
    inside = pl.BlockSpec(memory_space=pltpu.VMEM)
    return pl.pallas_call(
        kernel,
        out_shape=(
            jax.ShapeDtypeStruct((rows, LANES), F32),
            jax.ShapeDtypeStruct((rows, LANES), F32),
            jax.ShapeDtypeStruct((rows, LANES), F32),
            jax.ShapeDtypeStruct((16, rows, LANES), BF16),
        ),
        in_specs=[anywhere] * 5,
        out_specs=(inside,) * 4,
        scratch_shapes=scratch,
        compiler_params=pltpu.CompilerParams(
            collective_id=0, has_side_effects=True, vmem_limit_bytes=64 * 1024 * 1024 - 64 * 1024
        ),
    )(acts, grads, master, first, second)


def to_rows(array):
    own = array.shape[0]
    return array.reshape(own, 2, 16, LANES).swapaxes(1, 2).reshape(own * 32, LANES)


def from_rows(array):
    own = array.shape[0] // 32
    return array.reshape(own, 16, 2, LANES).swapaxes(1, 2).reshape(own, 2, 2048)


def on_device(activations, out_grads, master, first_moment, second_moment):
    new_master, new_first, new_second, weights = fused(
        activations, out_grads, to_rows(master), to_rows(first_moment), to_rows(second_moment)
    )
    return (
        from_rows(new_master),
        from_rows(new_first),
        from_rows(new_second),
        from_rows(weights.reshape(-1, LANES)),
    )


def solution(mesh):
    finer = Mesh(mesh.devices.reshape(4, 2, 4, 2, 2), ("tp_0", "tp_1", "dp_0", "dp_1", "dp_2"))
    in_specs = (
        P(None, DP, TP),
        P(None, DP, None),
        P(TP_DP, None, None),
        P(TP_DP, None, None),
        P(TP_DP, None, None),
    )
    out_specs = (
        P(TP_DP, None, None),
        P(TP_DP, None, None),
        P(TP_DP, None, None),
        P(TP, None, None),
    )
    return jax.shard_map(
        on_device, mesh=finer, in_specs=in_specs, out_specs=out_specs, check_vma=False
    )
```

```python
import functools
import math

import jax
import jax.numpy as jnp
from jax import lax
from jax.experimental import pallas as pl
from jax.experimental.pallas import tpu as pltpu
from jax.sharding import Mesh
from jax.sharding import PartitionSpec as P

DP = ("dp_0", "dp_1", "dp_2")
TP_DP = ("tp_0", "tp_1", "dp_0", "dp_1", "dp_2")
TP = ("tp_0", "tp_1")
MESH = pl.DeviceIdType.MESH
F32 = jnp.float32
BF16 = jnp.bfloat16


beta_first = 0.9
beta_second = 0.95
first_fix = 1.0 - 0.9**10
second_fix = 1.0 - 0.95**10
learn_rate = 0.01
decay_rate = 0.1
epsilon = 1e-08
limit_scale = 2.0

OWN = 64
WIDE = 256
HALF = WIDE // 2
STEPS = 8
LANES = 128
GATHERS = 4
X_ROWS = 288
Z_ROWS = 224
SUB = 32
LAG_TWO = 5
LAG_THREE = 8
LAG_END = 12
TOP = 2.0**120
TINY = 1e-37


def encode(value):
    square = value * value
    fourth = square * square
    return (fourth * (square * (value * jnp.abs(value)))).astype(BF16)


def decode(code):
    power = code.astype(F32)
    half = lax.rsqrt(jnp.maximum(jnp.abs(power), TINY))
    eighth = lax.rsqrt(lax.rsqrt(half))
    return (power * half) * (eighth * (eighth * eighth))


def kernel(
    acts_hbm, grads_hbm, master_hbm, first_hbm, second_hbm,
    master_out, first_out, second_out, weights_out,
    acts, turned, outs, master, first, second, own_grad,
    pair_send, pair_recv, total,
    x1_send, x1_recv, xz1_send, xz1_recv, xz2_send, xz2_recv,
    zz1_send, zz1_recv, zz2_send, zz2_recv, zx_send, zx_recv,
    bound, bounds, norm_dp, norm_tp, squares_ref,
    load_sem, out_sem, state_sem, pair_ssem, pair_rsem, x1_ssem, x1_rsem, xz1_ssem, xz1_rsem, xz2_ssem, xz2_rsem,
    zz1_ssem, zz1_rsem, zz2_ssem, zz2_rsem, zx_ssem, zx_rsem,
    bound_ssem, bound_rsem, ndp_ssem, ndp_rsem, ntp_ssem, ntp_rsem,
    gx_ssem, gx_rsem, gz_ssem, gz_rsem, gd_ssem, gd_rsem,
):
    ny, nh = lax.axis_size("tp_0"), lax.axis_size("tp_1")
    y, h = lax.axis_index("tp_0"), lax.axis_index("tp_1")
    z, x, c = lax.axis_index("dp_0"), lax.axis_index("dp_1"), lax.axis_index("dp_2")
    nt = ny * nh
    dp_me = z * 4 + x * 2 + c
    tp_me = y * nh + h
    za, zb, zo = lax.rem(z + 1, 4), lax.rem(z + 3, 4), lax.rem(z + 2, 4)
    xo = 1 - x
    tokens = acts_hbm.shape[1]
    to_core = {"dp_2": 1 - c}
    to_x = {"dp_1": xo}
    to_za = {"dp_0": za}
    to_zb = {"dp_0": zb}

    def dp_of(k):
        other = lax.rem(dp_me + k, 16)
        return other, {"dp_0": other // 4, "dp_1": lax.rem(other // 2, 2), "dp_2": lax.rem(other, 2)}

    def tp_of(k):
        other = lax.rem(tp_me + k, nt)
        return other, {"tp_0": other // nh, "tp_1": lax.rem(other, nh)}

    def remote(src, dst, ssem, rsem, device):
        return pltpu.make_async_remote_copy(
            src_ref=src, dst_ref=dst, send_sem=ssem, recv_sem=rsem, device_id=device, device_id_type=MESH
        )

    def acts_load(l):
        return pltpu.make_async_copy(acts_hbm.at[l], acts.at[l], load_sem.at[l])

    def outs_load(i):
        return pltpu.make_async_copy(
            grads_hbm.at[i // 4, :, pl.ds(pl.multiple_of(lax.rem(i, 4) * (2 * WIDE), 2 * WIDE), 2 * WIDE)],
            outs.at[i],
            out_sem.at[i],
        )

    states = (
        pltpu.make_async_copy(master_hbm, master, state_sem.at[0]),
        pltpu.make_async_copy(first_hbm, first, state_sem.at[1]),
        pltpu.make_async_copy(second_hbm, second, state_sem.at[2]),
    )
    acts_load(0).start()
    outs_load(0).start()
    acts_load(1).start()

    def start_outs(i, carry):
        outs_load(i).start()
        return carry

    lax.fori_loop(1, STEPS, start_outs, 0)
    for copy in states:
        copy.start()

    barrier = pltpu.get_barrier_semaphore()

    def greet_dp(k, carry):
        pl.semaphore_signal(barrier, inc=1, device_id=dp_of(k)[1], device_id_type=MESH)
        return carry

    def greet_tp(k, carry):
        pl.semaphore_signal(barrier, inc=1, device_id=tp_of(k)[1], device_id_type=MESH)
        return carry

    lax.fori_loop(1, 16, greet_dp, 0)
    lax.fori_loop(1, nt, greet_tp, 0)

    def turn(l):
        for q in range(8):
            flipped = acts[l, :, q * LANES : (q + 1) * LANES].T
            turned[l, 0, q * OWN : (q + 1) * OWN, :] = flipped[:OWN]
            turned[l, 1, q * OWN : (q + 1) * OWN, :] = flipped[OWN:]

    def largest(ref, lead):
        rows, wide = ref.shape[1], ref.shape[2]

        def step(r, best):
            part = jnp.abs(ref[lead, pl.ds(pl.multiple_of(r * 64, 64), 64), :])
            return jnp.maximum(best, jnp.max(part.reshape(4, 16, wide), axis=0))

        return lax.fori_loop(0, rows // 64, step, jnp.zeros((16, wide), BF16))

    acts_load(0).wait()
    turn(0)

    def product(l, core, i, p):
        return jnp.dot(
            turned[l, core], outs[i, :, p * WIDE : (p + 1) * WIDE], preferred_element_type=F32
        ).reshape(8, OWN, WIDE)

    def pair_copy(i, p):
        slot = lax.rem(i, 2)
        return remote(
            pair_send.at[slot, p], pair_recv.at[i, p], pair_ssem.at[slot, p], pair_rsem.at[i, p], to_core
        )

    def multiply(i):
        l = i // 4

        @pl.when(i >= 2)
        def _():
            for p in range(2):
                pair_copy(i - 2, p).wait_send()

        slot = lax.rem(i, 2)
        pair_send[slot, 0] = product(l, 1 - c, i, 0)
        pair_send[slot, 1] = product(l, 1 - c, i, 1)
        pair_copy(i, 0).start()
        total[i, 0] = product(l, c, i, 0)
        pair_copy(i, 1).start()
        total[i, 1] = product(l, c, i, 1)

    outs_load(0).wait()
    pl.semaphore_wait(barrier, 15 + nt - 1)
    multiply(0)

    acts_load(1).wait()
    biggest_act = jnp.maximum(jnp.max(largest(acts, 0).astype(F32)), jnp.max(largest(acts, 1).astype(F32)))
    best = largest(outs, 0)

    def widen(i, best):
        outs_load(i).wait()
        return jnp.maximum(best, largest(outs, i))

    best = lax.fori_loop(1, STEPS, widen, best)
    biggest_out = jnp.max(best.astype(F32))
    own_bound = jnp.maximum(biggest_act * biggest_out * (1.01 * tokens), 1e-30)
    bounds[dp_me] = jnp.full((8, LANES), own_bound, F32)
    bound[...] = jnp.full((8, LANES), own_bound, F32)

    def bound_copy(k):
        return remote(bound, bounds.at[dp_me], bound_ssem.at[k], bound_rsem.at[dp_me], dp_of(k)[1])

    def bound_send(k, carry):
        bound_copy(k).start()
        return carry

    lax.fori_loop(1, 16, bound_send, 0)
    turn(1)

    def bound_wait(other):
        remote(bound, bounds.at[other], bound_ssem.at[0], bound_rsem.at[other], to_core).wait_recv()

    bound_wait(z * 4 + x * 2 + 1 - c)

    top = TOP ** 0.125
    chip_bound = (bounds[dp_me] + bounds[z * 4 + x * 2 + 1 - c])[0:1, 0:1]
    chip_scale = top / chip_bound

    def paired(i, p, q):
        return total[i, p, q] + pair_recv[i, p, q]

    def x1_copy(i):
        return remote(x1_send.at[i], x1_recv.at[i], x1_ssem.at[i], x1_rsem.at[i], to_x)

    def z_copies(send, recv, ssem, rsem, i):
        return (
            remote(send.at[i, 0], recv.at[i, 0], ssem.at[i, 0], rsem.at[i, 0], to_za),
            remote(send.at[i, 1], recv.at[i, 1], ssem.at[i, 1], rsem.at[i, 1], to_zb),
        )

    def xz1_copies(i):
        return z_copies(xz1_send, xz1_recv, xz1_ssem, xz1_rsem, i)

    def xz2_copies(i):
        return z_copies(xz2_send, xz2_recv, xz2_ssem, xz2_rsem, i)

    def zz1_copies(i):
        return z_copies(zz1_send, zz1_recv, zz1_ssem, zz1_rsem, i)

    def zz2_copies(i):
        return z_copies(zz2_send, zz2_recv, zz2_ssem, zz2_rsem, i)

    def zx_copy(i):
        return remote(zx_send.at[i], zx_recv.at[i], zx_ssem.at[i], zx_rsem.at[i], to_x)

    lo, hi = slice(0, HALF), slice(HALF, WIDE)

    def stage_one(i):
        pair_copy(i, 0).wait_recv()
        for zz in range(4):
            x1_send[i, zz] = encode(paired(i, 0, zz * 2 + xo) * chip_scale)
        x1_copy(i).start()
        pair_copy(i, 1).wait_recv()
        for xx in range(2):
            far = encode(paired(i, 1, zo * 2 + xx) * chip_scale)
            zz1_send[i, 0, 0, xx] = far[:, lo]
            zz1_send[i, 1, 0, xx] = far[:, hi]
            q = za * 2 + xx
            zz1_send[i, 0, 1, xx] = encode((total[i, 1, q, :, hi] + pair_recv[i, 1, q, :, hi]) * chip_scale)
            q = zb * 2 + xx
            zz1_send[i, 1, 1, xx] = encode((total[i, 1, q, :, lo] + pair_recv[i, 1, q, :, lo]) * chip_scale)
        for copy in zz1_copies(i):
            copy.start()

    def bound_rest(k, carry):
        other = lax.rem(dp_me + k, 16)

        @pl.when(other != z * 4 + x * 2 + 1 - c)
        def _():
            bound_wait(other)

        return carry

    def bound_of(zz, xx):
        return (bounds[zz * 4 + xx * 2] + bounds[zz * 4 + xx * 2 + 1])[0:1, 0:1]

    def scales():
        whole = jnp.sum(bounds[...], axis=0)[0:1, 0:1] * 1.01
        return top / whole, whole * (1.0 / top)

    def from_z():
        return bound_of(za, x) * (1.0 / top), bound_of(zb, x) * (1.0 / top)

    def stage_two(i):
        scale, unscale = scales()
        from_za, from_zb = from_z()
        from_x = bound_of(z, xo) * (1.0 / top)
        x1_copy(i).wait_recv()
        for zz in range(4):
            q = zz * 2 + x
            total[i, 0, q] = paired(i, 0, q) + decode(x1_recv[i, zz]) * from_x
        far = encode(total[i, 0, zo * 2 + x] * scale)
        xz1_send[i, 0, 0] = far[:, lo]
        xz1_send[i, 1, 0] = far[:, hi]
        xz1_send[i, 0, 1] = encode(total[i, 0, za * 2 + x, :, hi] * scale)
        xz1_send[i, 1, 1] = encode(total[i, 0, zb * 2 + x, :, lo] * scale)
        for copy in xz1_copies(i):
            copy.start()
        for copy in zz1_copies(i):
            copy.wait_recv()
        for xx in range(2):
            q = za * 2 + xx
            mine = total[i, 1, q, :, lo] + pair_recv[i, 1, q, :, lo]
            zz2_send[i, 0, xx] = encode((mine + decode(zz1_recv[i, 0, 0, xx]) * from_zb) * scale)
            q = zb * 2 + xx
            mine = total[i, 1, q, :, hi] + pair_recv[i, 1, q, :, hi]
            zz2_send[i, 1, xx] = encode((mine + decode(zz1_recv[i, 1, 0, xx]) * from_za) * scale)
        for copy in zz2_copies(i):
            copy.start()

    def stage_three(i):
        scale, unscale = scales()
        from_za, from_zb = from_z()
        for copy in zz2_copies(i):
            copy.wait_recv()

        def summed(xx):
            q = z * 2 + xx
            low = (
                total[i, 1, q, :, lo] + pair_recv[i, 1, q, :, lo]
                + decode(zz1_recv[i, 1, 1, xx]) * from_za + decode(zz2_recv[i, 0, xx]) * unscale
            )
            high = (
                total[i, 1, q, :, hi] + pair_recv[i, 1, q, :, hi]
                + decode(zz1_recv[i, 0, 1, xx]) * from_zb + decode(zz2_recv[i, 1, xx]) * unscale
            )
            return low, high

        low, high = summed(xo)
        zx_send[i, :, lo] = encode(low * scale)
        zx_send[i, :, hi] = encode(high * scale)
        zx_copy(i).start()
        for copy in xz1_copies(i):
            copy.wait_recv()
        xz2_send[i, 0] = encode(total[i, 0, za * 2 + x, :, lo] * scale + decode(xz1_recv[i, 0, 0]))
        xz2_send[i, 1] = encode(total[i, 0, zb * 2 + x, :, hi] * scale + decode(xz1_recv[i, 1, 0]))
        for copy in xz2_copies(i):
            copy.start()
        low, high = summed(x)
        total[i, 1, z * 2 + x, :, lo] = low
        total[i, 1, z * 2 + x, :, hi] = high

    def put(i, j, value):
        base = (lax.rem(i, 4) * 4 + j) * 2 + i // 4
        for r in range(OWN // 8):
            own_grad[pl.ds(base + r * 8 * 32, 8, stride=32), :] = value[r * 8 : (r + 1) * 8]
        return jnp.sum((value * value).reshape(OWN // 8, 8, LANES), axis=0)

    def final(i):
        unscale = scales()[1]
        squares = squares_ref[...]
        for copy in xz2_copies(i):
            copy.wait_recv()
        q = z * 2 + x
        g = total[i, 0, q, :, lo] + (decode(xz1_recv[i, 1, 1]) + decode(xz2_recv[i, 0])) * unscale
        squares = squares + put(i, 0, g)
        g = total[i, 0, q, :, hi] + (decode(xz1_recv[i, 0, 1]) + decode(xz2_recv[i, 1])) * unscale
        squares = squares + put(i, 1, g)
        zx_copy(i).wait_recv()
        g = total[i, 1, q] + decode(zx_recv[i]) * unscale
        squares = squares + put(i, 2, g[:, lo])
        squares_ref[...] = squares + put(i, 3, g[:, hi])

    def turn_of(t, squares):
        def during(first, last, work, argument):
            @pl.when((t >= first) & (t < last))
            def _():
                work(argument)

        during(1, STEPS, multiply, t)
        during(1, STEPS + 1, stage_one, t - 1)

        @pl.when(t == LAG_TWO)
        def _():
            lax.fori_loop(1, 16, bound_rest, 0)

        during(LAG_TWO, LAG_TWO + STEPS, stage_two, t - LAG_TWO)
        during(LAG_THREE, LAG_THREE + STEPS, stage_three, t - LAG_THREE)
        during(LAG_END, LAG_END + STEPS, final, t - LAG_END)
        return squares

    squares_ref[...] = jnp.zeros((8, LANES), F32)
    lax.fori_loop(1, LAG_END + STEPS, turn_of, 0)
    squares = squares_ref[...]

    norm_dp[dp_me] = squares

    def ndp_copy(k, slot):
        return remote(norm_dp.at[slot], norm_dp.at[slot], ndp_ssem.at[k], ndp_rsem.at[slot], dp_of(k)[1])

    def ntp_copy(k, slot):
        return remote(norm_tp.at[slot], norm_tp.at[slot], ntp_ssem.at[k], ntp_rsem.at[slot], tp_of(k)[1])

    def exchange(copy, count, me):
        def send(k, carry):
            copy(k, me).start()
            return carry

        def receive(k, carry):
            copy(k, lax.rem(me + k, count)).wait_recv()
            return carry

        lax.fori_loop(1, count, send, 0)
        lax.fori_loop(1, count, receive, 0)

    exchange(ndp_copy, 16, dp_me)
    norm_tp[tp_me] = jnp.sum(norm_dp[...], axis=0)
    for copy in states:
        copy.wait()
    exchange(ntp_copy, nt, tp_me)
    sum_squares = jnp.sum(jnp.sum(norm_tp[...], axis=0), keepdims=True)
    entries = OWN * 16 * nt * 2 * 2048
    limit = limit_scale * math.sqrt(entries)
    clip_factor = limit / jnp.maximum(jnp.sqrt(sum_squares), limit)

    def update(start):
        rows = pl.ds(pl.multiple_of(start, SUB), SUB)
        clipped = clip_factor * own_grad[rows, :]
        new_first = beta_first * first[rows, :] + (1.0 - beta_first) * clipped
        new_second = beta_second * second[rows, :] + (1.0 - beta_second) * clipped * clipped
        step_dir = new_first * (1.0 / first_fix) / (jnp.sqrt(new_second * (1.0 / second_fix)) + epsilon)
        old = master[rows, :]
        new_master = old - learn_rate * (step_dir + decay_rate * old)
        first_out[rows, :] = new_first
        second_out[rows, :] = new_second
        master_out[rows, :] = new_master
        weights_out[dp_me, rows, :] = new_master.astype(BF16)

    def x_part(k):
        return pl.ds(pl.multiple_of(k * X_ROWS, 16), X_ROWS)

    def z_part(k):
        return pl.ds(pl.multiple_of(GATHERS * X_ROWS + k * Z_ROWS, 16), Z_ROWS)

    def x_half(k, n):
        return pl.ds(pl.multiple_of(k * X_ROWS + n * (X_ROWS // 2), 16), X_ROWS // 2)

    def z_half(k, n):
        return pl.ds(pl.multiple_of(GATHERS * X_ROWS + k * Z_ROWS + n * (Z_ROWS // 2), 16), Z_ROWS // 2)

    def move(zz, xx, rows, ssem, rsem, device):
        place = weights_out.at[zz * 4 + xx * 2 + c, rows, :]
        return remote(place, place, ssem, rsem, device)

    def gx(k, n, zz, xx, rows):
        return move(zz, xx, rows, gx_ssem.at[k, n], gx_rsem.at[k, n], to_x)

    def gz(k, n, zz, xx, rows, device):
        return move(zz, xx, rows, gz_ssem.at[k, n], gz_rsem.at[k, n], device)

    def gd(zz, xx, rows):
        return move(zz, xx, rows, gd_ssem, gd_rsem, to_core)

    def x_own(k, xx):
        return gx(k, 0, z, xx, x_part(k))

    def z_cross(k, n, zz, xx):
        return gx(k, 1 + n, zz, xx, z_part(k))

    def x_spread(k, xx, zz_a, zz_b, n):
        return (
            gz(k, n, zz_a, xx, x_part(k), to_za),
            gz(k, n + 1, zz_b, xx, x_part(k), to_zb),
        )

    def x_halves(k, xx, zz_a, zz_b, n):
        return (
            gz(k, n, zz_a, xx, x_half(k, 0), to_za),
            gz(k, n + 1, zz_b, xx, x_half(k, 1), to_zb),
        )

    def z_spread(k, zz_a, zz_b):
        return (
            gz(k, 8, zz_a, x, z_part(k), to_za),
            gz(k, 9, zz_b, x, z_part(k), to_zb),
        )

    def z_halves(k, zz_a, zz_b):
        return (
            gz(k, 10, zz_a, x, z_half(k, 0), to_za),
            gz(k, 11, zz_b, x, z_half(k, 1), to_zb),
        )

    def update_loop(k, carry):
        def in_x(s, carry):
            update(k * X_ROWS + s * SUB)
            return carry

        def in_z(s, carry):
            update(GATHERS * X_ROWS + k * Z_ROWS + s * SUB)
            return carry

        lax.fori_loop(0, X_ROWS // SUB, in_x, 0)
        x_own(k, x).start()
        gd(z, x, x_part(k)).start()
        lax.fori_loop(0, Z_ROWS // SUB, in_z, 0)
        for copy in z_spread(k, z, z):
            copy.start()
        gd(z, x, z_part(k)).start()
        return carry

    lax.fori_loop(0, GATHERS, update_loop, 0)

    def own_loop(k, carry):
        z_cross(k, 0, z, x).start()
        for copy in x_spread(k, x, z, z, 0):
            copy.start()
        return carry

    lax.fori_loop(0, GATHERS, own_loop, 0)

    def hop_one(k):
        x_own(k, xo).wait_recv()
        for copy in x_spread(k, xo, z, z, 2):
            copy.start()
        gd(z, xo, x_part(k)).start()
        from_below, from_above = z_spread(k, zb, za)
        halves = z_halves(k, zb, za)
        from_below.wait_recv()
        halves[0].start()
        z_cross(k, 1, zb, x).start()
        gd(zb, x, z_part(k)).start()
        from_above.wait_recv()
        halves[1].start()
        z_cross(k, 2, za, x).start()
        gd(za, x, z_part(k)).start()

    def hop_two(k):
        for xx, n in ((x, 0), (xo, 2)):
            from_below, from_above = x_spread(k, xx, zb, za, n)
            halves = x_halves(k, xx, zb, za, 4 + n)
            from_below.wait_recv()
            halves[0].start()
            gd(zb, xx, x_part(k)).start()
            from_above.wait_recv()
            halves[1].start()
            gd(za, xx, x_part(k)).start()
        for copy in z_halves(k, zo, zo):
            copy.wait_recv()
        z_cross(k, 3, zo, x).start()
        gd(zo, x, z_part(k)).start()

    def hop_three(k):
        for n, zz in ((0, z), (1, zb), (2, za), (3, zo)):
            z_cross(k, n, zz, xo).wait_recv()
            gd(zz, xo, z_part(k)).start()
        for xx, n in ((x, 0), (xo, 2)):
            for copy in x_halves(k, xx, zo, zo, 4 + n):
                copy.wait_recv()
            gd(zo, xx, x_part(k)).start()

    hop_one(0)
    hop_one(1)
    hop_two(0)

    def gather_loop(k, carry):
        hop_one(k)
        hop_two(k - 1)
        hop_three(k - 2)
        return carry

    lax.fori_loop(2, GATHERS, gather_loop, 0)
    hop_two(GATHERS - 1)
    hop_three(GATHERS - 2)
    hop_three(GATHERS - 1)

    def drain_steps(i, carry):
        x1_copy(i).wait_send()
        zx_copy(i).wait_send()
        for copies in (xz1_copies, xz2_copies, zz1_copies, zz2_copies):
            for copy in copies(i):
                copy.wait_send()
        return carry

    def drain_gather(k, carry):
        x_own(k, x).wait_send()
        for n in range(4):
            z_cross(k, n, z, x).wait_send()
        for n in (0, 2):
            for copy in x_spread(k, x, z, z, n) + x_halves(k, x, z, z, 4 + n):
                copy.wait_send()
        for copy in z_spread(k, z, z) + z_halves(k, z, z):
            copy.wait_send()
        return carry

    def drain_dp(k, carry):
        bound_copy(k).wait_send()
        ndp_copy(k, dp_me).wait_send()
        return carry

    def drain_tp(k, carry):
        ntp_copy(k, tp_me).wait_send()
        return carry

    for i in (STEPS - 2, STEPS - 1):
        for p in range(2):
            pair_copy(i, p).wait_send()
    lax.fori_loop(0, STEPS, drain_steps, 0)
    lax.fori_loop(0, GATHERS, drain_gather, 0)
    lax.fori_loop(1, 16, drain_dp, 0)
    lax.fori_loop(1, nt, drain_tp, 0)
    everything = weights_out.at[pl.ds(0, 8)]
    passed = remote(everything, everything, gd_ssem, gd_rsem, to_core)
    passed.wait_send()
    passed.wait_recv()


def fused(acts, grads, master, first, second):
    tokens = acts.shape[1]
    rows = OWN * 32
    dma = pltpu.SemaphoreType.DMA
    vmem = pltpu.VMEM
    scratch = [
        vmem((2, tokens, 1024), BF16),
        vmem((2, 2, 512, tokens), BF16),
        vmem((STEPS, tokens, 2 * WIDE), BF16),
        vmem((rows, LANES), F32),
        vmem((rows, LANES), F32),
        vmem((rows, LANES), F32),
        vmem((rows, LANES), F32),
        vmem((2, 2, 8, OWN, WIDE), F32),
        vmem((STEPS, 2, 8, OWN, WIDE), F32),
        vmem((STEPS, 2, 8, OWN, WIDE), F32),
    ]
    for shape in (
        (STEPS, 4, OWN, WIDE),
        (STEPS, 2, 2, OWN, HALF),
        (STEPS, 2, OWN, HALF),
        (STEPS, 2, 2, 2, OWN, HALF),
        (STEPS, 2, 2, OWN, HALF),
        (STEPS, OWN, WIDE),
    ):
        scratch += [vmem(shape, BF16), vmem(shape, BF16)]
    tp = lax.axis_size("tp_0") * lax.axis_size("tp_1")
    scratch += [
        vmem((8, LANES), F32),
        vmem((16, 8, LANES), F32),
        vmem((16, 8, LANES), F32),
        vmem((tp, 8, LANES), F32),
        vmem((8, LANES), F32),
        dma((2,)), dma((STEPS,)), dma((3,)),
        dma((2, 2)), dma((STEPS, 2)),
        dma((STEPS,)), dma((STEPS,)),
        dma((STEPS, 2)), dma((STEPS, 2)),
        dma((STEPS, 2)), dma((STEPS, 2)),
        dma((STEPS, 2)), dma((STEPS, 2)),
        dma((STEPS, 2)), dma((STEPS, 2)),
        dma((STEPS,)), dma((STEPS,)),
        dma((16,)), dma((16,)),
        dma((16,)), dma((16,)),
        dma((tp,)), dma((tp,)),
        dma((GATHERS, 5)), dma((GATHERS, 5)),
        dma((GATHERS, 12)), dma((GATHERS, 12)),
        dma, dma,
    ]
    anywhere = pl.BlockSpec(memory_space=pl.ANY)
    inside = pl.BlockSpec(memory_space=pltpu.VMEM)
    return pl.pallas_call(
        kernel,
        out_shape=(
            vmem((rows, LANES), F32),
            vmem((rows, LANES), F32),
            vmem((rows, LANES), F32),
            vmem((16, rows, LANES), BF16),
        ),
        in_specs=[anywhere] * 5,
        out_specs=(inside,) * 4,
        scratch_shapes=scratch,
        compiler_params=pltpu.CompilerParams(
            collective_id=0, has_side_effects=True, vmem_limit_bytes=50 * 1024 * 1024
        ),
    )(acts, grads, master, first, second)


def store_kernel(master, first, second, weights, master_out, first_out, second_out, weights_out, sems):
    copies = [
        pltpu.make_async_copy(weights.at[pl.ds(4 * n, 4)], weights_out.at[pl.ds(4 * n, 4)], sems.at[n])
        for n in range(4)
    ]
    for n, (value, out) in enumerate(((master, master_out), (first, first_out), (second, second_out))):
        copies.append(pltpu.make_async_copy(value, out, sems.at[4 + n]))
    for copy in copies:
        copy.start()
    for copy in copies:
        copy.wait()


def stored(master, first, second, weights):
    return pl.pallas_call(
        store_kernel,
        out_shape=tuple(jax.ShapeDtypeStruct(v.shape, v.dtype) for v in (master, first, second, weights)),
        in_specs=[pl.BlockSpec(memory_space=pltpu.VMEM)] * 4,
        out_specs=(pl.BlockSpec(memory_space=pltpu.HBM),) * 4,
        scratch_shapes=[pltpu.SemaphoreType.DMA((7,))],
        compiler_params=pltpu.CompilerParams(vmem_limit_bytes=2 * 1024 * 1024),
    )(master, first, second, weights)


def to_rows(array):
    own = array.shape[0]
    return array.reshape(own, 2, 16, LANES).swapaxes(1, 2).reshape(own * 32, LANES)


def from_rows(array):
    own = array.shape[0] // 32
    return array.reshape(own, 16, 2, LANES).swapaxes(1, 2).reshape(own, 2, 2048)


def on_device(activations, out_grads, master, first_moment, second_moment):
    new_master, new_first, new_second, weights = stored(
        *fused(activations, out_grads, to_rows(master), to_rows(first_moment), to_rows(second_moment))
    )
    return (
        from_rows(new_master),
        from_rows(new_first),
        from_rows(new_second),
        from_rows(weights.reshape(-1, LANES)),
    )


def solution(mesh):
    finer = Mesh(mesh.devices.reshape(4, 2, 4, 2, 2), ("tp_0", "tp_1", "dp_0", "dp_1", "dp_2"))
    in_specs = (
        P(None, DP, TP),
        P(None, DP, None),
        P(TP_DP, None, None),
        P(TP_DP, None, None),
        P(TP_DP, None, None),
    )
    out_specs = (
        P(TP_DP, None, None),
        P(TP_DP, None, None),
        P(TP_DP, None, None),
        P(TP, None, None),
    )
    return jax.shard_map(
        on_device, mesh=finer, in_specs=in_specs, out_specs=out_specs, check_vma=False
    )
```

```python
import functools
import math

import jax
import jax.numpy as jnp
from jax import lax
from jax.experimental import pallas as pl
from jax.experimental.pallas import tpu as pltpu
from jax.sharding import Mesh
from jax.sharding import PartitionSpec as P

DP = ("dp_0", "dp_1", "dp_2")
TP_DP = ("tp_0", "tp_1", "dp_0", "dp_1", "dp_2")
TP = ("tp_0", "tp_1")
MESH = pl.DeviceIdType.MESH
F32 = jnp.float32
BF16 = jnp.bfloat16


beta_first = 0.9
beta_second = 0.95
first_fix = 1.0 - 0.9**10
second_fix = 1.0 - 0.95**10
learn_rate = 0.01
decay_rate = 0.1
epsilon = 1e-08
limit_scale = 2.0

OWN = 64
WIDE = 256
HALF = WIDE // 2
STEPS = 8
X_PIECES = STEPS - 1
Z_PIECES = STEPS + 1
LANES = 128
GATHERS = 4
X_ROWS = 288
Z_ROWS = 224
SUB = 32
LAG_TWO = 5
LAG_THREE = 8
LAG_END = 12
TOP = 2.0**120
TINY = 1e-37


def encode(value):
    square = value * value
    fourth = square * square
    return (fourth * (square * (value * jnp.abs(value)))).astype(BF16)


def decode(code):
    power = code.astype(F32)
    half = lax.rsqrt(jnp.maximum(jnp.abs(power), TINY))
    eighth = lax.rsqrt(lax.rsqrt(half))
    return (power * half) * (eighth * (eighth * eighth))


def kernel(
    acts_hbm, grads_hbm, master_hbm, first_hbm, second_hbm,
    master_out, first_out, second_out, weights_out,
    acts, turned, outs, master, first, second, own_grad,
    pair_send, pair_recv, total,
    x1_send, x1_recv, xz1_send, xz1_recv, xz2_send, xz2_recv,
    zz1_send, zz1_recv, zz2_send, zz2_recv, zx_send, zx_recv,
    bound, bounds, norm_dp, norm_tp, squares_ref,
    load_sem, out_sem, state_sem, pair_ssem, pair_rsem, x1_ssem, x1_rsem, xz1_ssem, xz1_rsem, xz2_ssem, xz2_rsem,
    zz1_ssem, zz1_rsem, zz2_ssem, zz2_rsem, zx_ssem, zx_rsem,
    bound_ssem, bound_rsem, ndp_ssem, ndp_rsem, ntp_ssem, ntp_rsem,
    gx_ssem, gx_rsem, gz_ssem, gz_rsem, gd_ssem, gd_rsem,
):
    ny, nh = lax.axis_size("tp_0"), lax.axis_size("tp_1")
    y, h = lax.axis_index("tp_0"), lax.axis_index("tp_1")
    z, x, c = lax.axis_index("dp_0"), lax.axis_index("dp_1"), lax.axis_index("dp_2")
    nt = ny * nh
    dp_me = z * 4 + x * 2 + c
    tp_me = y * nh + h
    za, zb, zo = lax.rem(z + 1, 4), lax.rem(z + 3, 4), lax.rem(z + 2, 4)
    xo = 1 - x
    tokens = acts_hbm.shape[1]
    to_core = {"dp_2": 1 - c}
    to_x = {"dp_1": xo}
    to_za = {"dp_0": za}
    to_zb = {"dp_0": zb}

    def dp_of(k):
        other = lax.rem(dp_me + k, 16)
        return other, {"dp_0": other // 4, "dp_1": lax.rem(other // 2, 2), "dp_2": lax.rem(other, 2)}

    def tp_of(k):
        other = lax.rem(tp_me + k, nt)
        return other, {"tp_0": other // nh, "tp_1": lax.rem(other, nh)}

    def remote(src, dst, ssem, rsem, device):
        return pltpu.make_async_remote_copy(
            src_ref=src, dst_ref=dst, send_sem=ssem, recv_sem=rsem, device_id=device, device_id_type=MESH
        )

    def arrived(ref, rsem):
        remote(ref, ref, gd_ssem, rsem, to_core).wait_recv()

    def left(ref, ssem):
        remote(ref, ref, ssem, gd_rsem, to_core).wait_send()

    def acts_load(l):
        return pltpu.make_async_copy(acts_hbm.at[l], acts.at[l], load_sem.at[l])

    def outs_load(i):
        return pltpu.make_async_copy(
            grads_hbm.at[i // 4, :, pl.ds(pl.multiple_of(lax.rem(i, 4) * (2 * WIDE), 2 * WIDE), 2 * WIDE)],
            outs.at[i],
            out_sem.at[i],
        )

    states = (
        pltpu.make_async_copy(master_hbm, master, state_sem.at[0]),
        pltpu.make_async_copy(first_hbm, first, state_sem.at[1]),
        pltpu.make_async_copy(second_hbm, second, state_sem.at[2]),
    )
    acts_load(0).start()
    outs_load(0).start()
    acts_load(1).start()

    def start_outs(i, carry):
        outs_load(i).start()
        return carry

    lax.fori_loop(1, STEPS, start_outs, 0)
    for copy in states:
        copy.start()

    barrier = pltpu.get_barrier_semaphore()

    def greet_dp(k, carry):
        pl.semaphore_signal(barrier, inc=1, device_id=dp_of(k)[1], device_id_type=MESH)
        return carry

    def greet_tp(k, carry):
        pl.semaphore_signal(barrier, inc=1, device_id=tp_of(k)[1], device_id_type=MESH)
        return carry

    lax.fori_loop(1, 16, greet_dp, 0)
    lax.fori_loop(1, nt, greet_tp, 0)

    def turn(l):
        for q in range(8):
            flipped = acts[l, :, q * LANES : (q + 1) * LANES].T
            turned[l, 0, q * OWN : (q + 1) * OWN, :] = flipped[:OWN]
            turned[l, 1, q * OWN : (q + 1) * OWN, :] = flipped[OWN:]

    def largest(ref, lead):
        rows, wide = ref.shape[1], ref.shape[2]

        def step(r, best):
            part = jnp.abs(ref[lead, pl.ds(pl.multiple_of(r * 64, 64), 64), :])
            return jnp.maximum(best, jnp.max(part.reshape(4, 16, wide), axis=0))

        return lax.fori_loop(0, rows // 64, step, jnp.zeros((16, wide), BF16))

    acts_load(0).wait()
    turn(0)

    def product(l, core, i, p):
        return jnp.dot(
            turned[l, core], outs[i, :, p * WIDE : (p + 1) * WIDE], preferred_element_type=F32
        ).reshape(8, OWN, WIDE)

    def pair_copy(i, p):
        slot = lax.rem(i, 2)
        return remote(pair_send.at[slot, p], pair_recv.at[i, p], pair_ssem.at[slot], pair_rsem.at[i, p], to_core)

    def multiply(i):
        l = i // 4
        slot = lax.rem(i, 2)

        @pl.when(i >= 2)
        def _():
            left(pair_send.at[slot], pair_ssem.at[slot])

        pair_send[slot, 0] = product(l, 1 - c, i, 0)
        pair_send[slot, 1] = product(l, 1 - c, i, 1)
        pair_copy(i, 0).start()
        total[i, 0] = product(l, c, i, 0)
        pair_copy(i, 1).start()
        total[i, 1] = product(l, c, i, 1)

    outs_load(0).wait()
    for p in range(2):
        pair_send[0, p] = product(0, 1 - c, 0, p)
        total[0, p] = product(0, c, 0, p)

    acts_load(1).wait()
    turn(1)
    biggest_act = jnp.maximum(jnp.max(largest(acts, 0).astype(F32)), jnp.max(largest(acts, 1).astype(F32)))
    best = largest(outs, 0)

    def widen(i, best):
        outs_load(i).wait()
        return jnp.maximum(best, largest(outs, i))

    best = lax.fori_loop(1, STEPS, widen, best)
    biggest_out = jnp.max(best.astype(F32))
    own_bound = jnp.maximum(biggest_act * biggest_out * (1.01 * tokens), 1e-30)
    bounds[dp_me] = jnp.full((8, LANES), own_bound, F32)
    bound[...] = jnp.full((8, LANES), own_bound, F32)
    mate = z * 4 + x * 2 + 1 - c

    pl.semaphore_wait(barrier, 15 + nt - 1)
    remote(bound, bounds.at[dp_me], bound_ssem, bound_rsem.at[0], to_core).start()
    for p in range(2):
        pair_copy(0, p).start()

    def bound_send(k, carry):
        other, device = dp_of(k)

        @pl.when(other != mate)
        def _():
            remote(bound, bounds.at[dp_me], bound_ssem, bound_rsem.at[1], device).start()

        return carry

    lax.fori_loop(1, 16, bound_send, 0)

    top = TOP**0.125

    def chip_scale():
        return top / (bounds[dp_me] + bounds[mate])[0:1, 0:1]

    def paired(i, p, q):
        return total[i, p, q] + pair_recv[i, p, q]

    def x1_copy(i):
        return remote(x1_send.at[i], x1_recv.at[i], x1_ssem, x1_rsem.at[i], to_x)

    def send_z(send, recv, ssem, rsem, n):
        remote(send.at[n, 0], recv.at[n, 0], ssem, rsem.at[n], to_za).start()
        remote(send.at[n, 1], recv.at[n, 1], ssem, rsem.at[n], to_zb).start()

    def zx_copy(n):
        return remote(zx_send.at[n], zx_recv.at[n], zx_ssem, zx_rsem.at[n], to_x)

    lo, hi = slice(0, HALF), slice(HALF, WIDE)

    def z_pieces(work, i):
        def one(k, carry):
            work(i + k, i, 1 - k)
            return carry

        lax.fori_loop(0, 1 + i // (STEPS - 1), one, 0)

    def x_one(i):
        scale = chip_scale()
        pair_copy(i, 0).wait_recv()
        for zz in range(4):
            x1_send[i, zz] = encode(paired(i, 0, zz * 2 + xo) * scale)
        x1_copy(i).start()

    def z_one(n, i, p):
        scale = chip_scale()
        pair_copy(i, p).wait_recv()
        for xx in range(2):
            far = encode(paired(i, p, zo * 2 + xx) * scale)
            zz1_send[n, 0, 0, xx] = far[:, lo]
            zz1_send[n, 1, 0, xx] = far[:, hi]
            q = za * 2 + xx
            zz1_send[n, 0, 1, xx] = encode((total[i, p, q, :, hi] + pair_recv[i, p, q, :, hi]) * scale)
            q = zb * 2 + xx
            zz1_send[n, 1, 1, xx] = encode((total[i, p, q, :, lo] + pair_recv[i, p, q, :, lo]) * scale)
        send_z(zz1_send, zz1_recv, zz1_ssem, zz1_rsem, n)

    def bound_of(zz, xx):
        return (bounds[zz * 4 + xx * 2] + bounds[zz * 4 + xx * 2 + 1])[0:1, 0:1]

    def scales():
        whole = jnp.sum(bounds[...], axis=0)[0:1, 0:1] * 1.01
        return top / whole, whole * (1.0 / top)

    def from_z():
        return bound_of(za, x) * (1.0 / top), bound_of(zb, x) * (1.0 / top)

    def x_two(i):
        scale, unscale = scales()
        from_x = bound_of(z, xo) * (1.0 / top)
        x1_copy(i).wait_recv()
        for zz in range(4):
            q = zz * 2 + x
            total[i, 0, q] = paired(i, 0, q) + decode(x1_recv[i, zz]) * from_x
        far = encode(total[i, 0, zo * 2 + x] * scale)
        xz1_send[i, 0, 0] = far[:, lo]
        xz1_send[i, 1, 0] = far[:, hi]
        xz1_send[i, 0, 1] = encode(total[i, 0, za * 2 + x, :, hi] * scale)
        xz1_send[i, 1, 1] = encode(total[i, 0, zb * 2 + x, :, lo] * scale)
        send_z(xz1_send, xz1_recv, xz1_ssem, xz1_rsem, i)

    def z_two(n, i, p):
        scale, unscale = scales()
        from_za, from_zb = from_z()
        arrived(zz1_recv.at[n], zz1_rsem.at[n])
        for xx in range(2):
            q = za * 2 + xx
            mine = total[i, p, q, :, lo] + pair_recv[i, p, q, :, lo]
            zz2_send[n, 0, xx] = encode((mine + decode(zz1_recv[n, 0, 0, xx]) * from_zb) * scale)
            q = zb * 2 + xx
            mine = total[i, p, q, :, hi] + pair_recv[i, p, q, :, hi]
            zz2_send[n, 1, xx] = encode((mine + decode(zz1_recv[n, 1, 0, xx]) * from_za) * scale)
        send_z(zz2_send, zz2_recv, zz2_ssem, zz2_rsem, n)

    def x_three(i):
        scale, unscale = scales()
        arrived(xz1_recv.at[i], xz1_rsem.at[i])
        xz2_send[i, 0] = encode(total[i, 0, za * 2 + x, :, lo] * scale + decode(xz1_recv[i, 0, 0]))
        xz2_send[i, 1] = encode(total[i, 0, zb * 2 + x, :, hi] * scale + decode(xz1_recv[i, 1, 0]))
        send_z(xz2_send, xz2_recv, xz2_ssem, xz2_rsem, i)

    def z_three(n, i, p):
        scale, unscale = scales()
        from_za, from_zb = from_z()
        arrived(zz2_recv.at[n], zz2_rsem.at[n])

        def summed(xx):
            q = z * 2 + xx
            low = (
                total[i, p, q, :, lo] + pair_recv[i, p, q, :, lo]
                + decode(zz1_recv[n, 1, 1, xx]) * from_za + decode(zz2_recv[n, 0, xx]) * unscale
            )
            high = (
                total[i, p, q, :, hi] + pair_recv[i, p, q, :, hi]
                + decode(zz1_recv[n, 0, 1, xx]) * from_zb + decode(zz2_recv[n, 1, xx]) * unscale
            )
            return low, high

        low, high = summed(xo)
        zx_send[n, :, lo] = encode(low * scale)
        zx_send[n, :, hi] = encode(high * scale)
        zx_copy(n).start()
        low, high = summed(x)
        total[i, p, z * 2 + x, :, lo] = low
        total[i, p, z * 2 + x, :, hi] = high

    def put(i, j, value):
        base = (lax.rem(i, 4) * 4 + j) * 2 + i // 4
        for r in range(OWN // 8):
            own_grad[pl.ds(base + r * 8 * 32, 8, stride=32), :] = value[r * 8 : (r + 1) * 8]
        return jnp.sum((value * value).reshape(OWN // 8, 8, LANES), axis=0)

    def x_end(i):
        unscale = scales()[1]
        arrived(xz2_recv.at[i], xz2_rsem.at[i])
        q = z * 2 + x
        g = total[i, 0, q, :, lo] + (decode(xz1_recv[i, 1, 1]) + decode(xz2_recv[i, 0])) * unscale
        squares = squares_ref[...] + put(i, 0, g)
        g = total[i, 0, q, :, hi] + (decode(xz1_recv[i, 0, 1]) + decode(xz2_recv[i, 1])) * unscale
        squares_ref[...] = squares + put(i, 1, g)

    def z_end(n, i, p):
        unscale = scales()[1]
        zx_copy(n).wait_recv()
        g = total[i, p, z * 2 + x] + decode(zx_recv[n]) * unscale
        squares = squares_ref[...] + put(i, 2 * p, g[:, lo])
        squares_ref[...] = squares + put(i, 2 * p + 1, g[:, hi])

    def turn_of(t, carry):
        def during(lag, count, work):
            @pl.when((t >= lag) & (t < lag + count))
            def _():
                work(t - lag)

        during(0, STEPS, multiply)

        @pl.when(t == 1)
        def _():
            arrived(bound, bound_rsem.at[0])

        during(1, X_PIECES, x_one)
        during(1, STEPS, functools.partial(z_pieces, z_one))

        @pl.when(t == LAG_TWO)
        def _():
            arrived(bounds.at[pl.ds(0, 14)], bound_rsem.at[1])

        during(LAG_TWO, X_PIECES, x_two)
        during(LAG_TWO, STEPS, functools.partial(z_pieces, z_two))
        during(LAG_THREE, X_PIECES, x_three)
        during(LAG_THREE, STEPS, functools.partial(z_pieces, z_three))
        during(LAG_END, X_PIECES, x_end)
        during(LAG_END, STEPS, functools.partial(z_pieces, z_end))
        return carry

    squares_ref[...] = jnp.zeros((8, LANES), F32)
    lax.fori_loop(1, LAG_END + STEPS, turn_of, 0)

    norm_dp[dp_me] = squares_ref[...]

    def ndp_send(k, carry):
        place = norm_dp.at[dp_me]
        remote(place, place, ndp_ssem, ndp_rsem, dp_of(k)[1]).start()
        return carry

    def ntp_send(k, carry):
        place = norm_tp.at[tp_me]
        remote(place, place, ntp_ssem, ntp_rsem, tp_of(k)[1]).start()
        return carry

    lax.fori_loop(1, 16, ndp_send, 0)
    arrived(norm_dp.at[pl.ds(0, 15)], ndp_rsem)
    norm_tp[tp_me] = jnp.sum(norm_dp[...], axis=0)
    lax.fori_loop(1, nt, ntp_send, 0)
    for copy in states:
        copy.wait()
    if nt > 1:
        arrived(norm_tp.at[pl.ds(0, nt - 1)], ntp_rsem)
    sum_squares = jnp.sum(jnp.sum(norm_tp[...], axis=0), keepdims=True)
    entries = OWN * 16 * nt * 2 * 2048
    limit = limit_scale * math.sqrt(entries)
    clip_factor = limit / jnp.maximum(jnp.sqrt(sum_squares), limit)

    def update(start):
        rows = pl.ds(pl.multiple_of(start, SUB), SUB)
        clipped = clip_factor * own_grad[rows, :]
        new_first = beta_first * first[rows, :] + (1.0 - beta_first) * clipped
        new_second = beta_second * second[rows, :] + (1.0 - beta_second) * clipped * clipped
        step_dir = new_first * (1.0 / first_fix) / (jnp.sqrt(new_second * (1.0 / second_fix)) + epsilon)
        old = master[rows, :]
        new_master = old - learn_rate * (step_dir + decay_rate * old)
        first_out[rows, :] = new_first
        second_out[rows, :] = new_second
        master_out[rows, :] = new_master
        weights_out[dp_me, rows, :] = new_master.astype(BF16)

    def x_part(k):
        return pl.ds(pl.multiple_of(k * X_ROWS, 16), X_ROWS)

    def z_part(k):
        return pl.ds(pl.multiple_of(GATHERS * X_ROWS + k * Z_ROWS, 16), Z_ROWS)

    def x_half(k, n):
        return pl.ds(pl.multiple_of(k * X_ROWS + n * (X_ROWS // 2), 16), X_ROWS // 2)

    def z_half(k, n):
        return pl.ds(pl.multiple_of(GATHERS * X_ROWS + k * Z_ROWS + n * (Z_ROWS // 2), 16), Z_ROWS // 2)

    def move(zz, xx, rows, ssem, rsem, device):
        place = weights_out.at[zz * 4 + xx * 2 + c, rows, :]
        return remote(place, place, ssem, rsem, device)

    def gx(k, n, zz, xx, rows):
        return move(zz, xx, rows, gx_ssem, gx_rsem.at[k, n], to_x)

    def gz(k, n, zz, xx, rows, device):
        return move(zz, xx, rows, gz_ssem, gz_rsem.at[k, n], device)

    def gd(zz, xx, rows):
        return move(zz, xx, rows, gd_ssem, gd_rsem, to_core)

    def z_cross(k, zz):
        gx(k, 1, zz, x, z_part(k)).start()

    def blocks(count, rows):
        return weights_out.at[pl.ds(0, count), pl.ds(0, rows), :]

    def spread(k, n, xx, rows):
        gz(k, n, z, xx, rows, to_za).start()
        gz(k, n, z, xx, rows, to_zb).start()

    def halves(k, n, xx, half):
        gz(k, n, zb, xx, half(k, 0), to_za).start()
        gz(k, n, za, xx, half(k, 1), to_zb).start()

    def update_loop(k, carry):
        def in_x(s, carry):
            update(k * X_ROWS + s * SUB)
            return carry

        def in_z(s, carry):
            update(GATHERS * X_ROWS + k * Z_ROWS + s * SUB)
            return carry

        lax.fori_loop(0, X_ROWS // SUB, in_x, 0)
        gx(k, 0, z, x, x_part(k)).start()
        gd(z, x, x_part(k)).start()
        lax.fori_loop(0, Z_ROWS // SUB, in_z, 0)
        spread(k, 3, x, z_part(k))
        gd(z, x, z_part(k)).start()
        return carry

    lax.fori_loop(0, GATHERS, update_loop, 0)

    def own_loop(k, carry):
        z_cross(k, z)
        spread(k, 0, x, x_part(k))
        return carry

    lax.fori_loop(0, GATHERS, own_loop, 0)

    def hop_one(k):
        arrived(blocks(1, X_ROWS), gx_rsem.at[k, 0])
        spread(k, 1, xo, x_part(k))
        gd(z, xo, x_part(k)).start()
        arrived(blocks(2, Z_ROWS), gz_rsem.at[k, 3])
        halves(k, 4, x, z_half)
        for zz in (zb, za):
            z_cross(k, zz)
            gd(zz, x, z_part(k)).start()

    def hop_two(k):
        for n, xx in ((0, x), (1, xo)):
            arrived(blocks(2, X_ROWS), gz_rsem.at[k, n])
            halves(k, 2, xx, x_half)
            for zz in (zb, za):
                gd(zz, xx, x_part(k)).start()
        arrived(blocks(1, Z_ROWS), gz_rsem.at[k, 4])
        z_cross(k, zo)
        gd(zo, x, z_part(k)).start()

    def hop_three(k):
        arrived(blocks(4, Z_ROWS), gx_rsem.at[k, 1])
        for zz in (z, zb, za, zo):
            gd(zz, xo, z_part(k)).start()
        arrived(blocks(2, X_ROWS), gz_rsem.at[k, 2])
        for xx in (x, xo):
            gd(zo, xx, x_part(k)).start()

    hop_one(0)
    hop_one(1)
    hop_two(0)

    def gather_loop(k, carry):
        hop_one(k)
        hop_two(k - 1)
        hop_three(k - 2)
        return carry

    lax.fori_loop(2, GATHERS, gather_loop, 0)
    hop_two(GATHERS - 1)
    hop_three(GATHERS - 2)
    hop_three(GATHERS - 1)

    for slot in range(2):
        left(pair_send.at[slot], pair_ssem.at[slot])
    for sent, ssem in (
        (x1_send, x1_ssem), (xz1_send, xz1_ssem), (xz2_send, xz2_ssem), (zz1_send, zz1_ssem), (zz2_send, zz2_ssem),
        (zx_send, zx_ssem), (bounds.at[pl.ds(0, 15)], bound_ssem), (norm_dp.at[pl.ds(0, 15)], ndp_ssem),
        (blocks(4, X_ROWS + 4 * Z_ROWS), gx_ssem), (blocks(8, GATHERS * (6 * X_ROWS + 3 * Z_ROWS) // 8), gz_ssem),
        (blocks(8, OWN * 32), gd_ssem),
    ):
        left(sent, ssem)
    if nt > 1:
        left(norm_tp.at[pl.ds(0, nt - 1)], ntp_ssem)
    arrived(blocks(8, OWN * 32), gd_rsem)


def fused(acts, grads, master, first, second):
    tokens = acts.shape[1]
    rows = OWN * 32
    dma = pltpu.SemaphoreType.DMA
    vmem = pltpu.VMEM
    scratch = [
        vmem((2, tokens, 1024), BF16),
        vmem((2, 2, 512, tokens), BF16),
        vmem((STEPS, tokens, 2 * WIDE), BF16),
        vmem((rows, LANES), F32),
        vmem((rows, LANES), F32),
        vmem((rows, LANES), F32),
        vmem((rows, LANES), F32),
        vmem((2, 2, 8, OWN, WIDE), F32),
        vmem((STEPS, 2, 8, OWN, WIDE), F32),
        vmem((STEPS, 2, 8, OWN, WIDE), F32),
    ]
    for shape in (
        (X_PIECES, 4, OWN, WIDE),
        (X_PIECES, 2, 2, OWN, HALF),
        (X_PIECES, 2, OWN, HALF),
        (Z_PIECES, 2, 2, 2, OWN, HALF),
        (Z_PIECES, 2, 2, OWN, HALF),
        (Z_PIECES, OWN, WIDE),
    ):
        scratch += [vmem(shape, BF16), vmem(shape, BF16)]
    tp = lax.axis_size("tp_0") * lax.axis_size("tp_1")
    scratch += [
        vmem((8, LANES), F32),
        vmem((16, 8, LANES), F32),
        vmem((16, 8, LANES), F32),
        vmem((tp, 8, LANES), F32),
        vmem((8, LANES), F32),
        dma((2,)), dma((STEPS,)), dma((3,)),
        dma((2,)), dma((STEPS, 2)),
        dma, dma((X_PIECES,)),
        dma, dma((X_PIECES,)),
        dma, dma((X_PIECES,)),
        dma, dma((Z_PIECES,)),
        dma, dma((Z_PIECES,)),
        dma, dma((Z_PIECES,)),
        dma, dma((2,)),
        dma, dma,
        dma, dma,
        dma, dma((GATHERS, 2)),
        dma, dma((GATHERS, 5)),
        dma, dma,
    ]
    anywhere = pl.BlockSpec(memory_space=pl.ANY)
    inside = pl.BlockSpec(memory_space=pltpu.VMEM)
    return pl.pallas_call(
        kernel,
        out_shape=(
            vmem((rows, LANES), F32),
            vmem((rows, LANES), F32),
            vmem((rows, LANES), F32),
            vmem((16, rows, LANES), BF16),
        ),
        in_specs=[anywhere] * 5,
        out_specs=(inside,) * 4,
        scratch_shapes=scratch,
        compiler_params=pltpu.CompilerParams(
            collective_id=0, has_side_effects=True, vmem_limit_bytes=50 * 1024 * 1024
        ),
    )(acts, grads, master, first, second)


def store_kernel(master, first, second, weights, master_out, first_out, second_out, weights_out, sems):
    copies = [
        pltpu.make_async_copy(weights.at[pl.ds(4 * n, 4)], weights_out.at[pl.ds(4 * n, 4)], sems.at[n])
        for n in range(4)
    ]
    for n, (value, out) in enumerate(((master, master_out), (first, first_out), (second, second_out))):
        copies.append(pltpu.make_async_copy(value, out, sems.at[4 + n]))
    for copy in copies:
        copy.start()
    for copy in copies:
        copy.wait()


def stored(master, first, second, weights):
    return pl.pallas_call(
        store_kernel,
        out_shape=tuple(jax.ShapeDtypeStruct(v.shape, v.dtype) for v in (master, first, second, weights)),
        in_specs=[pl.BlockSpec(memory_space=pltpu.VMEM)] * 4,
        out_specs=(pl.BlockSpec(memory_space=pltpu.HBM),) * 4,
        scratch_shapes=[pltpu.SemaphoreType.DMA((7,))],
        compiler_params=pltpu.CompilerParams(vmem_limit_bytes=2 * 1024 * 1024),
    )(master, first, second, weights)


def to_rows(array):
    own = array.shape[0]
    return array.reshape(own, 2, 16, LANES).swapaxes(1, 2).reshape(own * 32, LANES)


def from_rows(array):
    own = array.shape[0] // 32
    return array.reshape(own, 16, 2, LANES).swapaxes(1, 2).reshape(own, 2, 2048)


def on_device(activations, out_grads, master, first_moment, second_moment):
    new_master, new_first, new_second, weights = stored(
        *fused(activations, out_grads, to_rows(master), to_rows(first_moment), to_rows(second_moment))
    )
    return (
        from_rows(new_master),
        from_rows(new_first),
        from_rows(new_second),
        from_rows(weights.reshape(-1, LANES)),
    )


def solution(mesh):
    finer = Mesh(mesh.devices.reshape(4, 2, 4, 2, 2), ("tp_0", "tp_1", "dp_0", "dp_1", "dp_2"))
    in_specs = (
        P(None, DP, TP),
        P(None, DP, None),
        P(TP_DP, None, None),
        P(TP_DP, None, None),
        P(TP_DP, None, None),
    )
    out_specs = (
        P(TP_DP, None, None),
        P(TP_DP, None, None),
        P(TP_DP, None, None),
        P(TP, None, None),
    )
    return jax.shard_map(
        on_device, mesh=finer, in_specs=in_specs, out_specs=out_specs, check_vma=False
    )
```

```python
import functools
import math

import jax
import jax.numpy as jnp
from jax import lax
from jax.experimental import pallas as pl
from jax.experimental.pallas import tpu as pltpu
from jax.sharding import Mesh
from jax.sharding import PartitionSpec as P

DP = ("dp_0", "dp_1", "dp_2")
TP_DP = ("tp_0", "tp_1", "dp_0", "dp_1", "dp_2")
TP = ("tp_0", "tp_1")
MESH = pl.DeviceIdType.MESH
F32 = jnp.float32
BF16 = jnp.bfloat16


beta_first = 0.9
beta_second = 0.95
first_fix = 1.0 - 0.9**10
second_fix = 1.0 - 0.95**10
learn_rate = 0.01
decay_rate = 0.1
epsilon = 1e-08
limit_scale = 2.0

OWN = 64
WIDE = 256
HALF = WIDE // 2
STEPS = 8
X_PIECES = STEPS - 1
Z_PIECES = STEPS + 1
LANES = 128
GATHERS = 4
X_ROWS = 288
Z_ROWS = 224
SUB = 32
LAG_TWO = 3
LAG_THREE = 6
LAG_END = 9
TOP = 2.0**120
TINY = 1e-37


def encode(value):
    square = value * value
    fourth = square * square
    return (fourth * (square * (value * jnp.abs(value)))).astype(BF16)


def decode(code):
    power = code.astype(F32)
    half = lax.rsqrt(jnp.maximum(jnp.abs(power), TINY))
    eighth = lax.rsqrt(lax.rsqrt(half))
    return (power * half) * (eighth * (eighth * eighth))


def kernel(
    acts_hbm, grads_hbm, master_hbm, first_hbm, second_hbm,
    master_out, first_out, second_out, weights_out,
    acts, turned, outs, master, first, second, own_grad,
    pair_send, pair_recv, total,
    x1_send, x1_recv, xz1_send, xz1_recv, xz2_send, xz2_recv,
    zz1_send, zz1_recv, zz2_send, zz2_recv, zx_send, zx_recv,
    bound, bounds, norm_dp, norm_tp, squares_ref,
    load_sem, out_sem, state_sem, pair_ssem, pair_rsem, x1_ssem, x1_rsem, xz1_ssem, xz1_rsem, xz2_ssem, xz2_rsem,
    zz1_ssem, zz1_rsem, zz2_ssem, zz2_rsem, zx_ssem, zx_rsem,
    bound_ssem, bound_rsem, ndp_ssem, ndp_rsem, ntp_ssem, ntp_rsem,
    gx_ssem, gx_rsem, gz_ssem, gz_rsem, gd_ssem, gd_rsem,
):
    ny, nh = lax.axis_size("tp_0"), lax.axis_size("tp_1")
    y, h = lax.axis_index("tp_0"), lax.axis_index("tp_1")
    z, x, c = lax.axis_index("dp_0"), lax.axis_index("dp_1"), lax.axis_index("dp_2")
    nt = ny * nh
    dp_me = z * 4 + x * 2 + c
    tp_me = y * nh + h
    za, zb, zo = lax.rem(z + 1, 4), lax.rem(z + 3, 4), lax.rem(z + 2, 4)
    xo = 1 - x
    tokens = acts_hbm.shape[1]
    to_core = {"dp_2": 1 - c}
    to_x = {"dp_1": xo}
    to_za = {"dp_0": za}
    to_zb = {"dp_0": zb}

    def dp_of(k):
        other = lax.rem(dp_me + k, 16)
        return other, {"dp_0": other // 4, "dp_1": lax.rem(other // 2, 2), "dp_2": lax.rem(other, 2)}

    def tp_of(k):
        other = lax.rem(tp_me + k, nt)
        return other, {"tp_0": other // nh, "tp_1": lax.rem(other, nh)}

    def remote(src, dst, ssem, rsem, device):
        return pltpu.make_async_remote_copy(
            src_ref=src, dst_ref=dst, send_sem=ssem, recv_sem=rsem, device_id=device, device_id_type=MESH
        )

    def arrived(ref, rsem):
        remote(ref, ref, gd_ssem, rsem, to_core).wait_recv()

    def left(ref, ssem):
        remote(ref, ref, ssem, gd_rsem, to_core).wait_send()

    def acts_load(l):
        return pltpu.make_async_copy(acts_hbm.at[l], acts.at[l], load_sem.at[l])

    def outs_load(i):
        return pltpu.make_async_copy(
            grads_hbm.at[i // 4, :, pl.ds(pl.multiple_of(lax.rem(i, 4) * (2 * WIDE), 2 * WIDE), 2 * WIDE)],
            outs.at[i],
            out_sem.at[i],
        )

    states = (
        pltpu.make_async_copy(master_hbm, master, state_sem.at[0]),
        pltpu.make_async_copy(first_hbm, first, state_sem.at[1]),
        pltpu.make_async_copy(second_hbm, second, state_sem.at[2]),
    )
    acts_load(0).start()
    outs_load(0).start()
    acts_load(1).start()

    def start_outs(i, carry):
        outs_load(i).start()
        return carry

    lax.fori_loop(1, STEPS, start_outs, 0)
    for copy in states:
        copy.start()

    barrier = pltpu.get_barrier_semaphore()

    def greet_dp(k, carry):
        pl.semaphore_signal(barrier, inc=1, device_id=dp_of(k)[1], device_id_type=MESH)
        return carry

    def greet_tp(k, carry):
        pl.semaphore_signal(barrier, inc=1, device_id=tp_of(k)[1], device_id_type=MESH)
        return carry

    lax.fori_loop(1, 16, greet_dp, 0)
    lax.fori_loop(1, nt, greet_tp, 0)

    def turn(l):
        for q in range(8):
            flipped = acts[l, :, q * LANES : (q + 1) * LANES].T
            turned[l, 0, q * OWN : (q + 1) * OWN, :] = flipped[:OWN]
            turned[l, 1, q * OWN : (q + 1) * OWN, :] = flipped[OWN:]

    def largest(ref, lead):
        rows, wide = ref.shape[1], ref.shape[2]

        def step(r, best):
            part = jnp.abs(ref[lead, pl.ds(pl.multiple_of(r * 64, 64), 64), :])
            return jnp.maximum(best, jnp.max(part.reshape(4, 16, wide), axis=0))

        return lax.fori_loop(0, rows // 64, step, jnp.zeros((16, wide), BF16))

    acts_load(0).wait()
    turn(0)

    def product(l, core, i, p):
        return jnp.dot(
            turned[l, core], outs[i, :, p * WIDE : (p + 1) * WIDE], preferred_element_type=F32
        ).reshape(8, OWN, WIDE)

    def pair_copy(i, p):
        slot = lax.rem(i, 2)
        return remote(pair_send.at[slot, p], pair_recv.at[i, p], pair_ssem.at[slot], pair_rsem.at[i, p], to_core)

    def multiply(i):
        l = i // 4
        slot = lax.rem(i, 2)

        @pl.when(i >= 2)
        def _():
            left(pair_send.at[slot], pair_ssem.at[slot])

        pair_send[slot, 0] = product(l, 1 - c, i, 0)
        pair_send[slot, 1] = product(l, 1 - c, i, 1)
        pair_copy(i, 0).start()
        total[i, 0] = product(l, c, i, 0)
        pair_copy(i, 1).start()
        total[i, 1] = product(l, c, i, 1)

    outs_load(0).wait()
    for p in range(2):
        pair_send[0, p] = product(0, 1 - c, 0, p)
        total[0, p] = product(0, c, 0, p)

    acts_load(1).wait()
    turn(1)
    biggest_act = jnp.maximum(jnp.max(largest(acts, 0).astype(F32)), jnp.max(largest(acts, 1).astype(F32)))
    best = largest(outs, 0)

    def widen(i, best):
        outs_load(i).wait()
        return jnp.maximum(best, largest(outs, i))

    best = lax.fori_loop(1, STEPS, widen, best)
    biggest_out = jnp.max(best.astype(F32))
    own_bound = jnp.maximum(biggest_act * biggest_out * (1.01 * tokens), 1e-30)
    bounds[dp_me] = jnp.full((8, LANES), own_bound, F32)
    bound[...] = jnp.full((8, LANES), own_bound, F32)
    mate = z * 4 + x * 2 + 1 - c

    pl.semaphore_wait(barrier, 15 + nt - 1)
    remote(bound, bounds.at[dp_me], bound_ssem, bound_rsem.at[0], to_core).start()
    for p in range(2):
        pair_copy(0, p).start()

    def bound_send(k, carry):
        other, device = dp_of(k)

        @pl.when(other != mate)
        def _():
            remote(bound, bounds.at[dp_me], bound_ssem, bound_rsem.at[1], device).start()

        return carry

    lax.fori_loop(1, 16, bound_send, 0)

    top = TOP**0.125

    def chip_scale():
        return top / (bounds[dp_me] + bounds[mate])[0:1, 0:1]

    def paired(i, p, q):
        return total[i, p, q] + pair_recv[i, p, q]

    def x1_copy(i):
        return remote(x1_send.at[i], x1_recv.at[i], x1_ssem, x1_rsem.at[i], to_x)

    def send_z(send, recv, ssem, rsem, n):
        remote(send.at[n, 0], recv.at[n, 0], ssem, rsem.at[n], to_za).start()
        remote(send.at[n, 1], recv.at[n, 1], ssem, rsem.at[n], to_zb).start()

    def zx_copy(n):
        return remote(zx_send.at[n], zx_recv.at[n], zx_ssem, zx_rsem.at[n], to_x)

    lo, hi = slice(0, HALF), slice(HALF, WIDE)

    def z_pieces(work, i):
        def one(k, carry):
            work(i + k, i, 1 - k)
            return carry

        lax.fori_loop(0, 1 + i // (STEPS - 1), one, 0)

    def x_one(i):
        scale = chip_scale()
        pair_copy(i, 0).wait_recv()
        for zz in range(4):
            x1_send[i, zz] = encode(paired(i, 0, zz * 2 + xo) * scale)
        x1_copy(i).start()

    def z_one(n, i, p):
        scale = chip_scale()
        pair_copy(i, p).wait_recv()
        for xx in range(2):
            far = encode(paired(i, p, zo * 2 + xx) * scale)
            zz1_send[n, 0, 0, xx] = far[:, lo]
            zz1_send[n, 1, 0, xx] = far[:, hi]
            q = za * 2 + xx
            zz1_send[n, 0, 1, xx] = encode((total[i, p, q, :, hi] + pair_recv[i, p, q, :, hi]) * scale)
            q = zb * 2 + xx
            zz1_send[n, 1, 1, xx] = encode((total[i, p, q, :, lo] + pair_recv[i, p, q, :, lo]) * scale)
        send_z(zz1_send, zz1_recv, zz1_ssem, zz1_rsem, n)

    def bound_of(zz, xx):
        return (bounds[zz * 4 + xx * 2] + bounds[zz * 4 + xx * 2 + 1])[0:1, 0:1]

    def scales():
        whole = jnp.sum(bounds[...], axis=0)[0:1, 0:1] * 1.01
        return top / whole, whole * (1.0 / top)

    def from_z():
        return bound_of(za, x) * (1.0 / top), bound_of(zb, x) * (1.0 / top)

    def x_two(i):
        scale, unscale = scales()
        from_x = bound_of(z, xo) * (1.0 / top)
        x1_copy(i).wait_recv()
        for zz in range(4):
            q = zz * 2 + x
            total[i, 0, q] = paired(i, 0, q) + decode(x1_recv[i, zz]) * from_x
        far = encode(total[i, 0, zo * 2 + x] * scale)
        xz1_send[i, 0, 0] = far[:, lo]
        xz1_send[i, 1, 0] = far[:, hi]
        xz1_send[i, 0, 1] = encode(total[i, 0, za * 2 + x, :, hi] * scale)
        xz1_send[i, 1, 1] = encode(total[i, 0, zb * 2 + x, :, lo] * scale)
        send_z(xz1_send, xz1_recv, xz1_ssem, xz1_rsem, i)

    def z_two(n, i, p):
        scale, unscale = scales()
        from_za, from_zb = from_z()
        arrived(zz1_recv.at[n], zz1_rsem.at[n])
        for xx in range(2):
            q = za * 2 + xx
            mine = total[i, p, q, :, lo] + pair_recv[i, p, q, :, lo]
            zz2_send[n, 0, xx] = encode((mine + decode(zz1_recv[n, 0, 0, xx]) * from_zb) * scale)
            q = zb * 2 + xx
            mine = total[i, p, q, :, hi] + pair_recv[i, p, q, :, hi]
            zz2_send[n, 1, xx] = encode((mine + decode(zz1_recv[n, 1, 0, xx]) * from_za) * scale)
        send_z(zz2_send, zz2_recv, zz2_ssem, zz2_rsem, n)

    def x_three(i):
        scale, unscale = scales()
        arrived(xz1_recv.at[i], xz1_rsem.at[i])
        xz2_send[i, 0] = encode(total[i, 0, za * 2 + x, :, lo] * scale + decode(xz1_recv[i, 0, 0]))
        xz2_send[i, 1] = encode(total[i, 0, zb * 2 + x, :, hi] * scale + decode(xz1_recv[i, 1, 0]))
        send_z(xz2_send, xz2_recv, xz2_ssem, xz2_rsem, i)

    def z_three(n, i, p):
        scale, unscale = scales()
        from_za, from_zb = from_z()
        arrived(zz2_recv.at[n], zz2_rsem.at[n])

        def summed(xx):
            q = z * 2 + xx
            low = (
                total[i, p, q, :, lo] + pair_recv[i, p, q, :, lo]
                + decode(zz1_recv[n, 1, 1, xx]) * from_za + decode(zz2_recv[n, 0, xx]) * unscale
            )
            high = (
                total[i, p, q, :, hi] + pair_recv[i, p, q, :, hi]
                + decode(zz1_recv[n, 0, 1, xx]) * from_zb + decode(zz2_recv[n, 1, xx]) * unscale
            )
            return low, high

        low, high = summed(xo)
        zx_send[n, :, lo] = encode(low * scale)
        zx_send[n, :, hi] = encode(high * scale)
        zx_copy(n).start()
        low, high = summed(x)
        total[i, p, z * 2 + x, :, lo] = low
        total[i, p, z * 2 + x, :, hi] = high

    def put(i, j, value):
        base = (lax.rem(i, 4) * 4 + j) * 2 + i // 4
        for r in range(OWN // 8):
            own_grad[pl.ds(base + r * 8 * 32, 8, stride=32), :] = value[r * 8 : (r + 1) * 8]
        return jnp.sum((value * value).reshape(OWN // 8, 8, LANES), axis=0)

    def x_end(i):
        unscale = scales()[1]
        arrived(xz2_recv.at[i], xz2_rsem.at[i])
        q = z * 2 + x
        g = total[i, 0, q, :, lo] + (decode(xz1_recv[i, 1, 1]) + decode(xz2_recv[i, 0])) * unscale
        squares = squares_ref[...] + put(i, 0, g)
        g = total[i, 0, q, :, hi] + (decode(xz1_recv[i, 0, 1]) + decode(xz2_recv[i, 1])) * unscale
        squares_ref[...] = squares + put(i, 1, g)

    def z_end(n, i, p):
        unscale = scales()[1]
        zx_copy(n).wait_recv()
        g = total[i, p, z * 2 + x] + decode(zx_recv[n]) * unscale
        squares = squares_ref[...] + put(i, 2 * p, g[:, lo])
        squares_ref[...] = squares + put(i, 2 * p + 1, g[:, hi])

    def turn_of(t, carry):
        def during(lag, count, work):
            @pl.when((t >= lag) & (t < lag + count))
            def _():
                work(t - lag)

        during(0, STEPS, multiply)

        @pl.when(t == 1)
        def _():
            arrived(bound, bound_rsem.at[0])

        during(1, X_PIECES, x_one)
        during(1, STEPS, functools.partial(z_pieces, z_one))

        @pl.when(t == LAG_TWO)
        def _():
            arrived(bounds.at[pl.ds(0, 14)], bound_rsem.at[1])

        during(LAG_TWO, X_PIECES, x_two)
        during(LAG_TWO, STEPS, functools.partial(z_pieces, z_two))
        during(LAG_THREE, X_PIECES, x_three)
        during(LAG_THREE, STEPS, functools.partial(z_pieces, z_three))
        during(LAG_END, X_PIECES, x_end)
        during(LAG_END, STEPS, functools.partial(z_pieces, z_end))
        return carry

    squares_ref[...] = jnp.zeros((8, LANES), F32)
    lax.fori_loop(1, LAG_END + STEPS, turn_of, 0)

    norm_dp[dp_me] = squares_ref[...]

    def ndp_send(k, carry):
        place = norm_dp.at[dp_me]
        remote(place, place, ndp_ssem, ndp_rsem, dp_of(k)[1]).start()
        return carry

    def ntp_send(k, carry):
        place = norm_tp.at[tp_me]
        remote(place, place, ntp_ssem, ntp_rsem, tp_of(k)[1]).start()
        return carry

    lax.fori_loop(1, 16, ndp_send, 0)
    arrived(norm_dp.at[pl.ds(0, 15)], ndp_rsem)
    norm_tp[tp_me] = jnp.sum(norm_dp[...], axis=0)
    lax.fori_loop(1, nt, ntp_send, 0)
    for copy in states:
        copy.wait()
    if nt > 1:
        arrived(norm_tp.at[pl.ds(0, nt - 1)], ntp_rsem)
    sum_squares = jnp.sum(jnp.sum(norm_tp[...], axis=0), keepdims=True)
    entries = OWN * 16 * nt * 2 * 2048
    limit = limit_scale * math.sqrt(entries)
    clip_factor = limit / jnp.maximum(jnp.sqrt(sum_squares), limit)

    def update(start):
        rows = pl.ds(pl.multiple_of(start, SUB), SUB)
        clipped = clip_factor * own_grad[rows, :]
        new_first = beta_first * first[rows, :] + (1.0 - beta_first) * clipped
        new_second = beta_second * second[rows, :] + (1.0 - beta_second) * clipped * clipped
        step_dir = new_first * (1.0 / first_fix) / (jnp.sqrt(new_second * (1.0 / second_fix)) + epsilon)
        old = master[rows, :]
        new_master = old - learn_rate * (step_dir + decay_rate * old)
        first_out[rows, :] = new_first
        second_out[rows, :] = new_second
        master_out[rows, :] = new_master
        weights_out[dp_me, rows, :] = new_master.astype(BF16)

    def x_part(k):
        return pl.ds(pl.multiple_of(k * X_ROWS, 16), X_ROWS)

    def z_part(k):
        return pl.ds(pl.multiple_of(GATHERS * X_ROWS + k * Z_ROWS, 16), Z_ROWS)

    def x_half(k, n):
        return pl.ds(pl.multiple_of(k * X_ROWS + n * (X_ROWS // 2), 16), X_ROWS // 2)

    def z_half(k, n):
        return pl.ds(pl.multiple_of(GATHERS * X_ROWS + k * Z_ROWS + n * (Z_ROWS // 2), 16), Z_ROWS // 2)

    def move(zz, xx, rows, ssem, rsem, device):
        place = weights_out.at[zz * 4 + xx * 2 + c, rows, :]
        return remote(place, place, ssem, rsem, device)

    def gx(k, n, zz, xx, rows):
        return move(zz, xx, rows, gx_ssem, gx_rsem.at[k, n], to_x)

    def gz(k, n, zz, xx, rows, device):
        return move(zz, xx, rows, gz_ssem, gz_rsem.at[k, n], device)

    def gd(zz, xx, rows):
        return move(zz, xx, rows, gd_ssem, gd_rsem, to_core)

    def z_cross(k, zz):
        gx(k, 1, zz, x, z_part(k)).start()

    def blocks(count, rows):
        return weights_out.at[pl.ds(0, count), pl.ds(0, rows), :]

    def spread(k, n, xx, rows):
        gz(k, n, z, xx, rows, to_za).start()
        gz(k, n, z, xx, rows, to_zb).start()

    def halves(k, n, xx, half):
        gz(k, n, zb, xx, half(k, 0), to_za).start()
        gz(k, n, za, xx, half(k, 1), to_zb).start()

    def update_loop(k, carry):
        def in_x(s, carry):
            update(k * X_ROWS + s * SUB)
            return carry

        def in_z(s, carry):
            update(GATHERS * X_ROWS + k * Z_ROWS + s * SUB)
            return carry

        lax.fori_loop(0, X_ROWS // SUB, in_x, 0)
        gx(k, 0, z, x, x_part(k)).start()
        gd(z, x, x_part(k)).start()
        lax.fori_loop(0, Z_ROWS // SUB, in_z, 0)
        spread(k, 3, x, z_part(k))
        gd(z, x, z_part(k)).start()
        return carry

    lax.fori_loop(0, GATHERS, update_loop, 0)

    def own_loop(k, carry):
        z_cross(k, z)
        spread(k, 0, x, x_part(k))
        return carry

    lax.fori_loop(0, GATHERS, own_loop, 0)

    def hop_one(k):
        arrived(blocks(1, X_ROWS), gx_rsem.at[k, 0])
        spread(k, 1, xo, x_part(k))
        gd(z, xo, x_part(k)).start()
        arrived(blocks(2, Z_ROWS), gz_rsem.at[k, 3])
        halves(k, 4, x, z_half)
        for zz in (zb, za):
            z_cross(k, zz)
            gd(zz, x, z_part(k)).start()

    def hop_two(k):
        for n, xx in ((0, x), (1, xo)):
            arrived(blocks(2, X_ROWS), gz_rsem.at[k, n])
            halves(k, 2, xx, x_half)
            for zz in (zb, za):
                gd(zz, xx, x_part(k)).start()
        arrived(blocks(1, Z_ROWS), gz_rsem.at[k, 4])
        z_cross(k, zo)
        gd(zo, x, z_part(k)).start()

    def hop_three(k):
        arrived(blocks(4, Z_ROWS), gx_rsem.at[k, 1])
        for zz in (z, zb, za, zo):
            gd(zz, xo, z_part(k)).start()
        arrived(blocks(2, X_ROWS), gz_rsem.at[k, 2])
        for xx in (x, xo):
            gd(zo, xx, x_part(k)).start()

    def first_hops(k, carry):
        hop_one(k)
        return carry

    lax.fori_loop(0, GATHERS, first_hops, 0)
    hop_two(0)
    hop_two(1)

    def gather_loop(k, carry):
        hop_two(k)
        hop_three(k - 2)
        return carry

    lax.fori_loop(2, GATHERS, gather_loop, 0)
    hop_three(GATHERS - 2)
    hop_three(GATHERS - 1)

    for slot in range(2):
        left(pair_send.at[slot], pair_ssem.at[slot])
    for sent, ssem in (
        (x1_send, x1_ssem), (xz1_send, xz1_ssem), (xz2_send, xz2_ssem), (zz1_send, zz1_ssem), (zz2_send, zz2_ssem),
        (zx_send, zx_ssem), (bounds.at[pl.ds(0, 15)], bound_ssem), (norm_dp.at[pl.ds(0, 15)], ndp_ssem),
        (blocks(8, GATHERS * (X_ROWS + 4 * Z_ROWS) // 8), gx_ssem), (blocks(8, GATHERS * (6 * X_ROWS + 3 * Z_ROWS) // 8), gz_ssem),
        (blocks(8, OWN * 32), gd_ssem),
    ):
        left(sent, ssem)
    if nt > 1:
        left(norm_tp.at[pl.ds(0, nt - 1)], ntp_ssem)
    arrived(blocks(8, OWN * 32), gd_rsem)


def fused(acts, grads, master, first, second):
    tokens = acts.shape[1]
    rows = OWN * 32
    dma = pltpu.SemaphoreType.DMA
    vmem = pltpu.VMEM
    scratch = [
        vmem((2, tokens, 1024), BF16),
        vmem((2, 2, 512, tokens), BF16),
        vmem((STEPS, tokens, 2 * WIDE), BF16),
        vmem((rows, LANES), F32),
        vmem((rows, LANES), F32),
        vmem((rows, LANES), F32),
        vmem((rows, LANES), F32),
        vmem((2, 2, 8, OWN, WIDE), F32),
        vmem((STEPS, 2, 8, OWN, WIDE), F32),
        vmem((STEPS, 2, 8, OWN, WIDE), F32),
    ]
    for shape in (
        (X_PIECES, 4, OWN, WIDE),
        (X_PIECES, 2, 2, OWN, HALF),
        (X_PIECES, 2, OWN, HALF),
        (Z_PIECES, 2, 2, 2, OWN, HALF),
        (Z_PIECES, 2, 2, OWN, HALF),
        (Z_PIECES, OWN, WIDE),
    ):
        scratch += [vmem(shape, BF16), vmem(shape, BF16)]
    tp = lax.axis_size("tp_0") * lax.axis_size("tp_1")
    scratch += [
        vmem((8, LANES), F32),
        vmem((16, 8, LANES), F32),
        vmem((16, 8, LANES), F32),
        vmem((tp, 8, LANES), F32),
        vmem((8, LANES), F32),
        dma((2,)), dma((STEPS,)), dma((3,)),
        dma((2,)), dma((STEPS, 2)),
        dma, dma((X_PIECES,)),
        dma, dma((X_PIECES,)),
        dma, dma((X_PIECES,)),
        dma, dma((Z_PIECES,)),
        dma, dma((Z_PIECES,)),
        dma, dma((Z_PIECES,)),
        dma, dma((2,)),
        dma, dma,
        dma, dma,
        dma, dma((GATHERS, 2)),
        dma, dma((GATHERS, 5)),
        dma, dma,
    ]
    anywhere = pl.BlockSpec(memory_space=pl.ANY)
    inside = pl.BlockSpec(memory_space=pltpu.VMEM)
    return pl.pallas_call(
        kernel,
        out_shape=(
            vmem((rows, LANES), F32),
            vmem((rows, LANES), F32),
            vmem((rows, LANES), F32),
            vmem((16, rows, LANES), BF16),
        ),
        in_specs=[anywhere] * 5,
        out_specs=(inside,) * 4,
        scratch_shapes=scratch,
        compiler_params=pltpu.CompilerParams(
            collective_id=0, has_side_effects=True, vmem_limit_bytes=50 * 1024 * 1024
        ),
    )(acts, grads, master, first, second)


def store_kernel(master, first, second, weights, master_out, first_out, second_out, weights_out, sems):
    copies = [
        pltpu.make_async_copy(weights.at[pl.ds(4 * n, 4)], weights_out.at[pl.ds(4 * n, 4)], sems.at[n])
        for n in range(4)
    ]
    for n, (value, out) in enumerate(((master, master_out), (first, first_out), (second, second_out))):
        copies.append(pltpu.make_async_copy(value, out, sems.at[4 + n]))
    for copy in copies:
        copy.start()
    for copy in copies:
        copy.wait()


def stored(master, first, second, weights):
    return pl.pallas_call(
        store_kernel,
        out_shape=tuple(jax.ShapeDtypeStruct(v.shape, v.dtype) for v in (master, first, second, weights)),
        in_specs=[pl.BlockSpec(memory_space=pltpu.VMEM)] * 4,
        out_specs=(pl.BlockSpec(memory_space=pltpu.HBM),) * 4,
        scratch_shapes=[pltpu.SemaphoreType.DMA((7,))],
        compiler_params=pltpu.CompilerParams(vmem_limit_bytes=2 * 1024 * 1024),
    )(master, first, second, weights)


def to_rows(array):
    own = array.shape[0]
    return array.reshape(own, 2, 16, LANES).swapaxes(1, 2).reshape(own * 32, LANES)


def from_rows(array):
    own = array.shape[0] // 32
    return array.reshape(own, 16, 2, LANES).swapaxes(1, 2).reshape(own, 2, 2048)


def on_device(activations, out_grads, master, first_moment, second_moment):
    new_master, new_first, new_second, weights = stored(
        *fused(activations, out_grads, to_rows(master), to_rows(first_moment), to_rows(second_moment))
    )
    return (
        from_rows(new_master),
        from_rows(new_first),
        from_rows(new_second),
        from_rows(weights.reshape(-1, LANES)),
    )


def solution(mesh):
    finer = Mesh(mesh.devices.reshape(4, 2, 4, 2, 2), ("tp_0", "tp_1", "dp_0", "dp_1", "dp_2"))
    in_specs = (
        P(None, DP, TP),
        P(None, DP, None),
        P(TP_DP, None, None),
        P(TP_DP, None, None),
        P(TP_DP, None, None),
    )
    out_specs = (
        P(TP_DP, None, None),
        P(TP_DP, None, None),
        P(TP_DP, None, None),
        P(TP, None, None),
    )
    return jax.shard_map(
        on_device, mesh=finer, in_specs=in_specs, out_specs=out_specs, check_vma=False
    )
```

```python
import functools
import math

import jax
import jax.numpy as jnp
from jax import lax
from jax.experimental import pallas as pl
from jax.experimental.pallas import tpu as pltpu
from jax.sharding import Mesh
from jax.sharding import PartitionSpec as P

DP = ("dp_0", "dp_1", "dp_2")
TP_DP = ("tp_0", "tp_1", "dp_0", "dp_1", "dp_2")
TP = ("tp_0", "tp_1")
MESH = pl.DeviceIdType.MESH
F32 = jnp.float32
BF16 = jnp.bfloat16


beta_first = 0.9
beta_second = 0.95
first_fix = 1.0 - 0.9**10
second_fix = 1.0 - 0.95**10
learn_rate = 0.01
decay_rate = 0.1
epsilon = 1e-08
limit_scale = 2.0

OWN = 64
WIDE = 256
HALF = WIDE // 2
STEPS = 8
X_PIECES = STEPS - 1
Z_PIECES = STEPS + 1
LANES = 128
GATHERS = 4
X_ROWS = 288
Z_ROWS = 224
X_SUB = 96
Z_SUB = 112
LAG_TWO = 3
LAG_THREE = 6
LAG_END = 9
TOP = 2.0**120
TINY = 1e-37


def encode(value):
    square = value * value
    fourth = square * square
    return (fourth * (square * (value * jnp.abs(value)))).astype(BF16)


def decode(code):
    power = code.astype(F32)
    half = lax.rsqrt(jnp.maximum(jnp.abs(power), TINY))
    eighth = lax.rsqrt(lax.rsqrt(half))
    return (power * half) * (eighth * (eighth * eighth))


def kernel(
    acts_hbm, grads_hbm, master_hbm, first_hbm, second_hbm,
    master_out, first_out, second_out, weights_out,
    acts, turned, outs, master, first, second, own_grad,
    pair_send, pair_recv, total,
    x1_send, x1_recv, xz1_send, xz1_recv, xz2_send, xz2_recv,
    zz1_send, zz1_recv, zz2_send, zz2_recv, zx_send, zx_recv,
    bound, bounds, norm_dp, norm_tp, squares_ref,
    load_sem, out_sem, state_sem, pair_ssem, pair_rsem, x1_ssem, x1_rsem, xz1_ssem, xz1_rsem, xz2_ssem, xz2_rsem,
    zz1_ssem, zz1_rsem, zz2_ssem, zz2_rsem, zx_ssem, zx_rsem,
    bound_ssem, bound_rsem, ndp_ssem, ndp_rsem, ntp_ssem, ntp_rsem,
    gx_ssem, gx_rsem, gz_ssem, gz_rsem, gd_ssem, gd_rsem,
):
    ny, nh = lax.axis_size("tp_0"), lax.axis_size("tp_1")
    y, h = lax.axis_index("tp_0"), lax.axis_index("tp_1")
    z, x, c = lax.axis_index("dp_0"), lax.axis_index("dp_1"), lax.axis_index("dp_2")
    nt = ny * nh
    dp_me = z * 4 + x * 2 + c
    tp_me = y * nh + h
    za, zb, zo = lax.rem(z + 1, 4), lax.rem(z + 3, 4), lax.rem(z + 2, 4)
    xo = 1 - x
    tokens = acts_hbm.shape[1]
    to_core = {"dp_2": 1 - c}
    to_x = {"dp_1": xo}
    to_za = {"dp_0": za}
    to_zb = {"dp_0": zb}

    def dp_of(k):
        other = lax.rem(dp_me + k, 16)
        return other, {"dp_0": other // 4, "dp_1": lax.rem(other // 2, 2), "dp_2": lax.rem(other, 2)}

    def tp_of(k):
        other = lax.rem(tp_me + k, nt)
        return other, {"tp_0": other // nh, "tp_1": lax.rem(other, nh)}

    def remote(src, dst, ssem, rsem, device):
        return pltpu.make_async_remote_copy(
            src_ref=src, dst_ref=dst, send_sem=ssem, recv_sem=rsem, device_id=device, device_id_type=MESH
        )

    def arrived(ref, rsem):
        remote(ref, ref, gd_ssem, rsem, to_core).wait_recv()

    def left(ref, ssem):
        remote(ref, ref, ssem, gd_rsem, to_core).wait_send()

    def acts_load(l):
        return pltpu.make_async_copy(acts_hbm.at[l], acts.at[l], load_sem.at[l])

    def outs_load(i):
        return pltpu.make_async_copy(
            grads_hbm.at[i // 4, :, pl.ds(pl.multiple_of(lax.rem(i, 4) * (2 * WIDE), 2 * WIDE), 2 * WIDE)],
            outs.at[i],
            out_sem.at[i],
        )

    states = (
        pltpu.make_async_copy(master_hbm, master, state_sem.at[0]),
        pltpu.make_async_copy(first_hbm, first, state_sem.at[1]),
        pltpu.make_async_copy(second_hbm, second, state_sem.at[2]),
    )
    acts_load(0).start()
    outs_load(0).start()
    acts_load(1).start()

    def start_outs(i, carry):
        outs_load(i).start()
        return carry

    lax.fori_loop(1, STEPS, start_outs, 0)
    for copy in states:
        copy.start()

    barrier = pltpu.get_barrier_semaphore()

    def greet_dp(k, carry):
        pl.semaphore_signal(barrier, inc=1, device_id=dp_of(k)[1], device_id_type=MESH)
        return carry

    def greet_tp(k, carry):
        pl.semaphore_signal(barrier, inc=1, device_id=tp_of(k)[1], device_id_type=MESH)
        return carry

    lax.fori_loop(1, 16, greet_dp, 0)
    lax.fori_loop(1, nt, greet_tp, 0)

    def turn(l):
        for q in range(8):
            flipped = acts[l, :, q * LANES : (q + 1) * LANES].T
            turned[l, 0, q * OWN : (q + 1) * OWN, :] = flipped[:OWN]
            turned[l, 1, q * OWN : (q + 1) * OWN, :] = flipped[OWN:]

    def largest(ref, lead):
        rows, wide = ref.shape[1], ref.shape[2]

        def step(r, best):
            part = jnp.abs(ref[lead, pl.ds(pl.multiple_of(r * 64, 64), 64), :])
            return jnp.maximum(best, jnp.max(part.reshape(4, 16, wide), axis=0))

        return lax.fori_loop(0, rows // 64, step, jnp.zeros((16, wide), BF16))

    acts_load(0).wait()
    turn(0)

    def product(l, core, i, p):
        return jnp.dot(
            turned[l, core], outs[i, :, p * WIDE : (p + 1) * WIDE], preferred_element_type=F32
        ).reshape(8, OWN, WIDE)

    def pair_copy(i, p):
        slot = lax.rem(i, 2)
        return remote(pair_send.at[slot, p], pair_recv.at[i, p], pair_ssem.at[slot], pair_rsem.at[i, p], to_core)

    def multiply(i):
        l = i // 4
        slot = lax.rem(i, 2)

        @pl.when(i >= 2)
        def _():
            left(pair_send.at[slot], pair_ssem.at[slot])

        pair_send[slot, 0] = product(l, 1 - c, i, 0)
        pair_send[slot, 1] = product(l, 1 - c, i, 1)
        pair_copy(i, 0).start()
        total[i, 0] = product(l, c, i, 0)
        pair_copy(i, 1).start()
        total[i, 1] = product(l, c, i, 1)

    outs_load(0).wait()
    for p in range(2):
        pair_send[0, p] = product(0, 1 - c, 0, p)
        total[0, p] = product(0, c, 0, p)

    acts_load(1).wait()
    turn(1)
    biggest_act = jnp.maximum(jnp.max(largest(acts, 0).astype(F32)), jnp.max(largest(acts, 1).astype(F32)))
    best = largest(outs, 0)

    def widen(i, best):
        outs_load(i).wait()
        return jnp.maximum(best, largest(outs, i))

    best = lax.fori_loop(1, STEPS, widen, best)
    biggest_out = jnp.max(best.astype(F32))
    own_bound = jnp.maximum(biggest_act * biggest_out * (1.01 * tokens), 1e-30)
    bounds[dp_me] = jnp.full((8, LANES), own_bound, F32)
    bound[...] = jnp.full((8, LANES), own_bound, F32)
    mate = z * 4 + x * 2 + 1 - c

    pl.semaphore_wait(barrier, 15 + nt - 1)
    remote(bound, bounds.at[dp_me], bound_ssem, bound_rsem.at[0], to_core).start()
    for p in range(2):
        pair_copy(0, p).start()

    def bound_send(k, carry):
        other, device = dp_of(k)

        @pl.when(other != mate)
        def _():
            remote(bound, bounds.at[dp_me], bound_ssem, bound_rsem.at[1], device).start()

        return carry

    lax.fori_loop(1, 16, bound_send, 0)

    top = TOP**0.125

    def chip_scale():
        return top / (bounds[dp_me] + bounds[mate])[0:1, 0:1]

    def paired(i, p, q):
        return total[i, p, q] + pair_recv[i, p, q]

    def x1_copy(i):
        return remote(x1_send.at[i], x1_recv.at[i], x1_ssem, x1_rsem.at[i], to_x)

    def send_z(send, recv, ssem, rsem, n):
        remote(send.at[n, 0], recv.at[n, 0], ssem, rsem.at[n], to_za).start()
        remote(send.at[n, 1], recv.at[n, 1], ssem, rsem.at[n], to_zb).start()

    def zx_copy(n):
        return remote(zx_send.at[n], zx_recv.at[n], zx_ssem, zx_rsem.at[n], to_x)

    lo, hi = slice(0, HALF), slice(HALF, WIDE)

    def z_pieces(work, i):
        def one(k, carry):
            work(i + k, i, 1 - k)
            return carry

        lax.fori_loop(0, 1 + i // (STEPS - 1), one, 0)

    def x_one(i):
        scale = chip_scale()
        pair_copy(i, 0).wait_recv()
        for zz in range(4):
            x1_send[i, zz] = encode(paired(i, 0, zz * 2 + xo) * scale)
        x1_copy(i).start()

    def z_one(n, i, p):
        scale = chip_scale()
        pair_copy(i, p).wait_recv()
        for xx in range(2):
            far = encode(paired(i, p, zo * 2 + xx) * scale)
            zz1_send[n, 0, 0, xx] = far[:, lo]
            zz1_send[n, 1, 0, xx] = far[:, hi]
            q = za * 2 + xx
            zz1_send[n, 0, 1, xx] = encode((total[i, p, q, :, hi] + pair_recv[i, p, q, :, hi]) * scale)
            q = zb * 2 + xx
            zz1_send[n, 1, 1, xx] = encode((total[i, p, q, :, lo] + pair_recv[i, p, q, :, lo]) * scale)
        send_z(zz1_send, zz1_recv, zz1_ssem, zz1_rsem, n)

    def bound_of(zz, xx):
        return (bounds[zz * 4 + xx * 2] + bounds[zz * 4 + xx * 2 + 1])[0:1, 0:1]

    def scales():
        whole = jnp.sum(bounds[...], axis=0)[0:1, 0:1] * 1.01
        return top / whole, whole * (1.0 / top)

    def from_z():
        return bound_of(za, x) * (1.0 / top), bound_of(zb, x) * (1.0 / top)

    def x_two(i):
        scale, unscale = scales()
        from_x = bound_of(z, xo) * (1.0 / top)
        x1_copy(i).wait_recv()
        for zz in range(4):
            q = zz * 2 + x
            total[i, 0, q] = paired(i, 0, q) + decode(x1_recv[i, zz]) * from_x
        far = encode(total[i, 0, zo * 2 + x] * scale)
        xz1_send[i, 0, 0] = far[:, lo]
        xz1_send[i, 1, 0] = far[:, hi]
        xz1_send[i, 0, 1] = encode(total[i, 0, za * 2 + x, :, hi] * scale)
        xz1_send[i, 1, 1] = encode(total[i, 0, zb * 2 + x, :, lo] * scale)
        send_z(xz1_send, xz1_recv, xz1_ssem, xz1_rsem, i)

    def z_two(n, i, p):
        scale, unscale = scales()
        from_za, from_zb = from_z()
        arrived(zz1_recv.at[n], zz1_rsem.at[n])
        for xx in range(2):
            q = za * 2 + xx
            mine = total[i, p, q, :, lo] + pair_recv[i, p, q, :, lo]
            zz2_send[n, 0, xx] = encode((mine + decode(zz1_recv[n, 0, 0, xx]) * from_zb) * scale)
            q = zb * 2 + xx
            mine = total[i, p, q, :, hi] + pair_recv[i, p, q, :, hi]
            zz2_send[n, 1, xx] = encode((mine + decode(zz1_recv[n, 1, 0, xx]) * from_za) * scale)
        send_z(zz2_send, zz2_recv, zz2_ssem, zz2_rsem, n)

    def x_three(i):
        scale, unscale = scales()
        arrived(xz1_recv.at[i], xz1_rsem.at[i])
        xz2_send[i, 0] = encode(total[i, 0, za * 2 + x, :, lo] * scale + decode(xz1_recv[i, 0, 0]))
        xz2_send[i, 1] = encode(total[i, 0, zb * 2 + x, :, hi] * scale + decode(xz1_recv[i, 1, 0]))
        send_z(xz2_send, xz2_recv, xz2_ssem, xz2_rsem, i)

    def z_three(n, i, p):
        scale, unscale = scales()
        from_za, from_zb = from_z()
        arrived(zz2_recv.at[n], zz2_rsem.at[n])

        def summed(xx):
            q = z * 2 + xx
            low = (
                total[i, p, q, :, lo] + pair_recv[i, p, q, :, lo]
                + decode(zz1_recv[n, 1, 1, xx]) * from_za + decode(zz2_recv[n, 0, xx]) * unscale
            )
            high = (
                total[i, p, q, :, hi] + pair_recv[i, p, q, :, hi]
                + decode(zz1_recv[n, 0, 1, xx]) * from_zb + decode(zz2_recv[n, 1, xx]) * unscale
            )
            return low, high

        low, high = summed(xo)
        zx_send[n, :, lo] = encode(low * scale)
        zx_send[n, :, hi] = encode(high * scale)
        zx_copy(n).start()
        low, high = summed(x)
        total[i, p, z * 2 + x, :, lo] = low
        total[i, p, z * 2 + x, :, hi] = high

    def put(i, j, value):
        base = (lax.rem(i, 4) * 4 + j) * 2 + i // 4
        for r in range(OWN // 8):
            own_grad[pl.ds(base + r * 8 * 32, 8, stride=32), :] = value[r * 8 : (r + 1) * 8]
        return jnp.sum((value * value).reshape(OWN // 8, 8, LANES), axis=0)

    def x_end(i):
        unscale = scales()[1]
        arrived(xz2_recv.at[i], xz2_rsem.at[i])
        q = z * 2 + x
        g = total[i, 0, q, :, lo] + (decode(xz1_recv[i, 1, 1]) + decode(xz2_recv[i, 0])) * unscale
        squares = squares_ref[...] + put(i, 0, g)
        g = total[i, 0, q, :, hi] + (decode(xz1_recv[i, 0, 1]) + decode(xz2_recv[i, 1])) * unscale
        squares_ref[...] = squares + put(i, 1, g)

    def z_end(n, i, p):
        unscale = scales()[1]
        zx_copy(n).wait_recv()
        g = total[i, p, z * 2 + x] + decode(zx_recv[n]) * unscale
        squares = squares_ref[...] + put(i, 2 * p, g[:, lo])
        squares_ref[...] = squares + put(i, 2 * p + 1, g[:, hi])

    def turn_of(t, carry):
        def during(lag, count, work):
            @pl.when((t >= lag) & (t < lag + count))
            def _():
                work(t - lag)

        during(0, STEPS, multiply)

        @pl.when(t == 1)
        def _():
            arrived(bound, bound_rsem.at[0])

        during(1, X_PIECES, x_one)
        during(1, STEPS, functools.partial(z_pieces, z_one))

        @pl.when(t == LAG_TWO)
        def _():
            arrived(bounds.at[pl.ds(0, 14)], bound_rsem.at[1])

        during(LAG_TWO, STEPS, functools.partial(z_pieces, z_two))
        during(LAG_THREE, STEPS, functools.partial(z_pieces, z_three))
        during(LAG_END, STEPS, functools.partial(z_pieces, z_end))
        during(LAG_TWO, X_PIECES, x_two)
        during(LAG_THREE, X_PIECES, x_three)
        during(LAG_END, X_PIECES, x_end)
        return carry

    squares_ref[...] = jnp.zeros((8, LANES), F32)
    lax.fori_loop(1, LAG_END + STEPS, turn_of, 0)

    norm_dp[dp_me] = squares_ref[...]

    def ndp_send(k, carry):
        place = norm_dp.at[dp_me]
        remote(place, place, ndp_ssem, ndp_rsem, dp_of(k)[1]).start()
        return carry

    def ntp_send(k, carry):
        place = norm_tp.at[tp_me]
        remote(place, place, ntp_ssem, ntp_rsem, tp_of(k)[1]).start()
        return carry

    lax.fori_loop(1, 16, ndp_send, 0)
    arrived(norm_dp.at[pl.ds(0, 15)], ndp_rsem)
    norm_tp[tp_me] = jnp.sum(norm_dp[...], axis=0)
    lax.fori_loop(1, nt, ntp_send, 0)
    for copy in states:
        copy.wait()
    if nt > 1:
        arrived(norm_tp.at[pl.ds(0, nt - 1)], ntp_rsem)
    sum_squares = jnp.sum(jnp.sum(norm_tp[...], axis=0), keepdims=True)
    entries = OWN * 16 * nt * 2 * 2048
    limit = limit_scale * math.sqrt(entries)
    clip_factor = limit / jnp.maximum(jnp.sqrt(sum_squares), limit)

    def update(start, count):
        rows = pl.ds(pl.multiple_of(start, 16), count)
        clipped = clip_factor * own_grad[rows, :]
        new_first = beta_first * first[rows, :] + (1.0 - beta_first) * clipped
        new_second = beta_second * second[rows, :] + (1.0 - beta_second) * clipped * clipped
        step_dir = new_first * (1.0 / first_fix) / (jnp.sqrt(new_second * (1.0 / second_fix)) + epsilon)
        old = master[rows, :]
        new_master = old - learn_rate * (step_dir + decay_rate * old)
        first_out[rows, :] = new_first
        second_out[rows, :] = new_second
        master_out[rows, :] = new_master
        weights_out[dp_me, rows, :] = new_master.astype(BF16)

    def x_part(k):
        return pl.ds(pl.multiple_of(k * X_ROWS, 16), X_ROWS)

    def z_part(k):
        return pl.ds(pl.multiple_of(GATHERS * X_ROWS + k * Z_ROWS, 16), Z_ROWS)

    def x_half(k, n):
        return pl.ds(pl.multiple_of(k * X_ROWS + n * (X_ROWS // 2), 16), X_ROWS // 2)

    def z_half(k, n):
        return pl.ds(pl.multiple_of(GATHERS * X_ROWS + k * Z_ROWS + n * (Z_ROWS // 2), 16), Z_ROWS // 2)

    def move(zz, xx, rows, ssem, rsem, device):
        place = weights_out.at[zz * 4 + xx * 2 + c, rows, :]
        return remote(place, place, ssem, rsem, device)

    def gx(k, n, zz, xx, rows):
        return move(zz, xx, rows, gx_ssem, gx_rsem.at[k, n], to_x)

    def gz(k, n, zz, xx, rows, device):
        return move(zz, xx, rows, gz_ssem, gz_rsem.at[k, n], device)

    def gd(zz, xx, rows):
        return move(zz, xx, rows, gd_ssem, gd_rsem, to_core)

    def z_cross(k, zz):
        gx(k, 1, zz, x, z_part(k)).start()

    def blocks(count, rows):
        return weights_out.at[pl.ds(0, count), pl.ds(0, rows), :]

    def spread(k, n, xx, rows):
        gz(k, n, z, xx, rows, to_za).start()
        gz(k, n, z, xx, rows, to_zb).start()

    def halves(k, n, xx, half):
        gz(k, n, zb, xx, half(k, 0), to_za).start()
        gz(k, n, za, xx, half(k, 1), to_zb).start()

    def update_loop(k, carry):
        def in_x(s, carry):
            update(k * X_ROWS + s * X_SUB, X_SUB)
            return carry

        def in_z(s, carry):
            update(GATHERS * X_ROWS + k * Z_ROWS + s * Z_SUB, Z_SUB)
            return carry

        lax.fori_loop(0, X_ROWS // X_SUB, in_x, 0)
        gx(k, 0, z, x, x_part(k)).start()
        gd(z, x, x_part(k)).start()
        lax.fori_loop(0, Z_ROWS // Z_SUB, in_z, 0)
        spread(k, 3, x, z_part(k))
        gd(z, x, z_part(k)).start()
        return carry

    lax.fori_loop(0, GATHERS, update_loop, 0)

    def own_loop(k, carry):
        z_cross(k, z)
        spread(k, 0, x, x_part(k))
        return carry

    lax.fori_loop(0, GATHERS, own_loop, 0)

    def hop_one(k):
        arrived(blocks(1, X_ROWS), gx_rsem.at[k, 0])
        spread(k, 1, xo, x_part(k))
        gd(z, xo, x_part(k)).start()
        arrived(blocks(2, Z_ROWS), gz_rsem.at[k, 3])
        halves(k, 4, x, z_half)
        for zz in (zb, za):
            z_cross(k, zz)
            gd(zz, x, z_part(k)).start()

    def hop_two(k):
        for n, xx in ((0, x), (1, xo)):
            arrived(blocks(2, X_ROWS), gz_rsem.at[k, n])
            halves(k, 2, xx, x_half)
            for zz in (zb, za):
                gd(zz, xx, x_part(k)).start()
        arrived(blocks(1, Z_ROWS), gz_rsem.at[k, 4])
        z_cross(k, zo)
        gd(zo, x, z_part(k)).start()

    def hop_three(k):
        arrived(blocks(4, Z_ROWS), gx_rsem.at[k, 1])
        for zz in (z, zb, za, zo):
            gd(zz, xo, z_part(k)).start()
        arrived(blocks(2, X_ROWS), gz_rsem.at[k, 2])
        for xx in (x, xo):
            gd(zo, xx, x_part(k)).start()

    def first_hops(k, carry):
        hop_one(k)
        return carry

    lax.fori_loop(0, GATHERS, first_hops, 0)
    hop_two(0)
    hop_two(1)

    def gather_loop(k, carry):
        hop_two(k)
        hop_three(k - 2)
        return carry

    lax.fori_loop(2, GATHERS, gather_loop, 0)
    hop_three(GATHERS - 2)
    hop_three(GATHERS - 1)

    for slot in range(2):
        left(pair_send.at[slot], pair_ssem.at[slot])
    for sent, ssem in (
        (x1_send, x1_ssem), (xz1_send, xz1_ssem), (xz2_send, xz2_ssem), (zz1_send, zz1_ssem), (zz2_send, zz2_ssem),
        (zx_send, zx_ssem), (bounds.at[pl.ds(0, 15)], bound_ssem), (norm_dp.at[pl.ds(0, 15)], ndp_ssem),
        (blocks(8, GATHERS * (X_ROWS + 4 * Z_ROWS) // 8), gx_ssem), (blocks(8, GATHERS * (6 * X_ROWS + 3 * Z_ROWS) // 8), gz_ssem),
        (blocks(8, OWN * 32), gd_ssem),
    ):
        left(sent, ssem)
    if nt > 1:
        left(norm_tp.at[pl.ds(0, nt - 1)], ntp_ssem)
    arrived(blocks(8, OWN * 32), gd_rsem)


def fused(acts, grads, master, first, second):
    tokens = acts.shape[1]
    rows = OWN * 32
    dma = pltpu.SemaphoreType.DMA
    vmem = pltpu.VMEM
    scratch = [
        vmem((2, tokens, 1024), BF16),
        vmem((2, 2, 512, tokens), BF16),
        vmem((STEPS, tokens, 2 * WIDE), BF16),
        vmem((rows, LANES), F32),
        vmem((rows, LANES), F32),
        vmem((rows, LANES), F32),
        vmem((rows, LANES), F32),
        vmem((2, 2, 8, OWN, WIDE), F32),
        vmem((STEPS, 2, 8, OWN, WIDE), F32),
        vmem((STEPS, 2, 8, OWN, WIDE), F32),
    ]
    for shape in (
        (X_PIECES, 4, OWN, WIDE),
        (X_PIECES, 2, 2, OWN, HALF),
        (X_PIECES, 2, OWN, HALF),
        (Z_PIECES, 2, 2, 2, OWN, HALF),
        (Z_PIECES, 2, 2, OWN, HALF),
        (Z_PIECES, OWN, WIDE),
    ):
        scratch += [vmem(shape, BF16), vmem(shape, BF16)]
    tp = lax.axis_size("tp_0") * lax.axis_size("tp_1")
    scratch += [
        vmem((8, LANES), F32),
        vmem((16, 8, LANES), F32),
        vmem((16, 8, LANES), F32),
        vmem((tp, 8, LANES), F32),
        vmem((8, LANES), F32),
        dma((2,)), dma((STEPS,)), dma((3,)),
        dma((2,)), dma((STEPS, 2)),
        dma, dma((X_PIECES,)),
        dma, dma((X_PIECES,)),
        dma, dma((X_PIECES,)),
        dma, dma((Z_PIECES,)),
        dma, dma((Z_PIECES,)),
        dma, dma((Z_PIECES,)),
        dma, dma((2,)),
        dma, dma,
        dma, dma,
        dma, dma((GATHERS, 2)),
        dma, dma((GATHERS, 5)),
        dma, dma,
    ]
    anywhere = pl.BlockSpec(memory_space=pl.ANY)
    inside = pl.BlockSpec(memory_space=pltpu.VMEM)
    return pl.pallas_call(
        kernel,
        out_shape=(
            vmem((rows, LANES), F32),
            vmem((rows, LANES), F32),
            vmem((rows, LANES), F32),
            vmem((16, rows, LANES), BF16),
        ),
        in_specs=[anywhere] * 5,
        out_specs=(inside,) * 4,
        scratch_shapes=scratch,
        compiler_params=pltpu.CompilerParams(
            collective_id=0, has_side_effects=True, vmem_limit_bytes=50 * 1024 * 1024
        ),
    )(acts, grads, master, first, second)


def store_kernel(master, first, second, weights, master_out, first_out, second_out, weights_out, sems):
    copies = [
        pltpu.make_async_copy(weights.at[pl.ds(4 * n, 4)], weights_out.at[pl.ds(4 * n, 4)], sems.at[n])
        for n in range(4)
    ]
    for n, (value, out) in enumerate(((master, master_out), (first, first_out), (second, second_out))):
        copies.append(pltpu.make_async_copy(value, out, sems.at[4 + n]))
    for copy in copies:
        copy.start()
    for copy in copies:
        copy.wait()


def stored(master, first, second, weights):
    return pl.pallas_call(
        store_kernel,
        out_shape=tuple(jax.ShapeDtypeStruct(v.shape, v.dtype) for v in (master, first, second, weights)),
        in_specs=[pl.BlockSpec(memory_space=pltpu.VMEM)] * 4,
        out_specs=(pl.BlockSpec(memory_space=pltpu.HBM),) * 4,
        scratch_shapes=[pltpu.SemaphoreType.DMA((7,))],
        compiler_params=pltpu.CompilerParams(vmem_limit_bytes=2 * 1024 * 1024),
    )(master, first, second, weights)


def to_rows(array):
    own = array.shape[0]
    return array.reshape(own, 2, 16, LANES).swapaxes(1, 2).reshape(own * 32, LANES)


def from_rows(array):
    own = array.shape[0] // 32
    return array.reshape(own, 16, 2, LANES).swapaxes(1, 2).reshape(own, 2, 2048)


def on_device(activations, out_grads, master, first_moment, second_moment):
    new_master, new_first, new_second, weights = stored(
        *fused(activations, out_grads, to_rows(master), to_rows(first_moment), to_rows(second_moment))
    )
    return (
        from_rows(new_master),
        from_rows(new_first),
        from_rows(new_second),
        from_rows(weights.reshape(-1, LANES)),
    )


def solution(mesh):
    finer = Mesh(mesh.devices.reshape(4, 2, 4, 2, 2), ("tp_0", "tp_1", "dp_0", "dp_1", "dp_2"))
    in_specs = (
        P(None, DP, TP),
        P(None, DP, None),
        P(TP_DP, None, None),
        P(TP_DP, None, None),
        P(TP_DP, None, None),
    )
    out_specs = (
        P(TP_DP, None, None),
        P(TP_DP, None, None),
        P(TP_DP, None, None),
        P(TP, None, None),
    )
    return jax.shard_map(
        on_device, mesh=finer, in_specs=in_specs, out_specs=out_specs, check_vma=False
    )
```

```python
import functools
import math

import jax
import jax.numpy as jnp
from jax import lax
from jax.experimental import pallas as pl
from jax.experimental.pallas import tpu as pltpu
from jax.sharding import Mesh
from jax.sharding import PartitionSpec as P

DP = ("dp_0", "dp_1", "dp_2")
TP_DP = ("tp_0", "tp_1", "dp_0", "dp_1", "dp_2")
TP = ("tp_0", "tp_1")
MESH = pl.DeviceIdType.MESH
F32 = jnp.float32
BF16 = jnp.bfloat16


beta_first = 0.9
beta_second = 0.95
first_fix = 1.0 - 0.9**10
second_fix = 1.0 - 0.95**10
learn_rate = 0.01
decay_rate = 0.1
epsilon = 1e-08
limit_scale = 2.0

OWN = 64
WIDE = 256
HALF = WIDE // 2
STEPS = 8
X_PIECES = STEPS - 1
Z_PIECES = STEPS + 1
LANES = 128
GATHERS = 2
X_ROWS = 576
Z_ROWS = 448
X_SUB = 96
Z_SUB = 112
LAG_TWO = 3
LAG_THREE = 6
LAG_END = 9
TOP = 2.0**120
TINY = 1e-37


def encode(value):
    square = value * value
    fourth = square * square
    return (fourth * (square * (value * jnp.abs(value)))).astype(BF16)


def decode(code):
    power = code.astype(F32)
    half = lax.rsqrt(jnp.maximum(jnp.abs(power), TINY))
    eighth = lax.rsqrt(lax.rsqrt(half))
    return (power * half) * (eighth * (eighth * eighth))


def kernel(
    acts_hbm, grads_hbm, master_hbm, first_hbm, second_hbm,
    master_out, first_out, second_out, weights_out,
    acts, turned, outs, master, first, second, own_grad,
    pair_send, pair_recv, total,
    x1_send, x1_recv, xz1_send, xz1_recv, xz2_send, xz2_recv,
    zz1_send, zz1_recv, zz2_send, zz2_recv, zx_send, zx_recv,
    bound, bounds, norm_dp, norm_tp, squares_ref,
    load_sem, out_sem, state_sem, pair_ssem, pair_rsem, x1_ssem, x1_rsem, xz1_ssem, xz1_rsem, xz2_ssem, xz2_rsem,
    zz1_ssem, zz1_rsem, zz2_ssem, zz2_rsem, zx_ssem, zx_rsem,
    bound_ssem, bound_rsem, ndp_ssem, ndp_rsem, ntp_ssem, ntp_rsem,
    gx_ssem, gx_rsem, gz_ssem, gz_rsem, gd_ssem, gd_rsem,
):
    ny, nh = lax.axis_size("tp_0"), lax.axis_size("tp_1")
    y, h = lax.axis_index("tp_0"), lax.axis_index("tp_1")
    z, x, c = lax.axis_index("dp_0"), lax.axis_index("dp_1"), lax.axis_index("dp_2")
    nt = ny * nh
    dp_me = z * 4 + x * 2 + c
    tp_me = y * nh + h
    za, zb, zo = lax.rem(z + 1, 4), lax.rem(z + 3, 4), lax.rem(z + 2, 4)
    xo = 1 - x
    tokens = acts_hbm.shape[1]
    to_core = {"dp_2": 1 - c}
    to_x = {"dp_1": xo}
    to_za = {"dp_0": za}
    to_zb = {"dp_0": zb}

    def dp_of(k):
        other = lax.rem(dp_me + k, 16)
        return other, {"dp_0": other // 4, "dp_1": lax.rem(other // 2, 2), "dp_2": lax.rem(other, 2)}

    def tp_of(k):
        other = lax.rem(tp_me + k, nt)
        return other, {"tp_0": other // nh, "tp_1": lax.rem(other, nh)}

    def remote(src, dst, ssem, rsem, device):
        return pltpu.make_async_remote_copy(
            src_ref=src, dst_ref=dst, send_sem=ssem, recv_sem=rsem, device_id=device, device_id_type=MESH
        )

    def arrived(ref, rsem):
        remote(ref, ref, gd_ssem, rsem, to_core).wait_recv()

    def left(ref, ssem):
        remote(ref, ref, ssem, gd_rsem, to_core).wait_send()

    def acts_load(l):
        return pltpu.make_async_copy(acts_hbm.at[l], acts.at[l], load_sem.at[l])

    def outs_load(i):
        return pltpu.make_async_copy(
            grads_hbm.at[i // 4, :, pl.ds(pl.multiple_of(lax.rem(i, 4) * (2 * WIDE), 2 * WIDE), 2 * WIDE)],
            outs.at[i],
            out_sem.at[i],
        )

    states = (
        pltpu.make_async_copy(master_hbm, master, state_sem.at[0]),
        pltpu.make_async_copy(first_hbm, first, state_sem.at[1]),
        pltpu.make_async_copy(second_hbm, second, state_sem.at[2]),
    )
    acts_load(0).start()
    outs_load(0).start()
    acts_load(1).start()

    def start_outs(i, carry):
        outs_load(i).start()
        return carry

    lax.fori_loop(1, STEPS, start_outs, 0)
    for copy in states:
        copy.start()

    barrier = pltpu.get_barrier_semaphore()

    def greet_dp(k, carry):
        pl.semaphore_signal(barrier, inc=1, device_id=dp_of(k)[1], device_id_type=MESH)
        return carry

    def greet_tp(k, carry):
        pl.semaphore_signal(barrier, inc=1, device_id=tp_of(k)[1], device_id_type=MESH)
        return carry

    lax.fori_loop(1, 16, greet_dp, 0)
    lax.fori_loop(1, nt, greet_tp, 0)

    def turn(l):
        for q in range(8):
            flipped = acts[l, :, q * LANES : (q + 1) * LANES].T
            turned[l, 0, q * OWN : (q + 1) * OWN, :] = flipped[:OWN]
            turned[l, 1, q * OWN : (q + 1) * OWN, :] = flipped[OWN:]

    def largest(ref, lead):
        rows, wide = ref.shape[1], ref.shape[2]

        def step(r, best):
            part = jnp.abs(ref[lead, pl.ds(pl.multiple_of(r * 64, 64), 64), :])
            return jnp.maximum(best, jnp.max(part.reshape(4, 16, wide), axis=0))

        return lax.fori_loop(0, rows // 64, step, jnp.zeros((16, wide), BF16))

    acts_load(0).wait()
    turn(0)

    def product(l, core, i, p):
        return jnp.dot(
            turned[l, core], outs[i, :, p * WIDE : (p + 1) * WIDE], preferred_element_type=F32
        ).reshape(8, OWN, WIDE)

    def pair_copy(i, p):
        slot = lax.rem(i, 2)
        return remote(pair_send.at[slot, p], pair_recv.at[i, p], pair_ssem.at[slot], pair_rsem.at[i, p], to_core)

    def multiply(i):
        l = i // 4
        slot = lax.rem(i, 2)

        @pl.when(i >= 2)
        def _():
            left(pair_send.at[slot], pair_ssem.at[slot])

        pair_send[slot, 0] = product(l, 1 - c, i, 0)
        pair_send[slot, 1] = product(l, 1 - c, i, 1)
        pair_copy(i, 0).start()
        total[i, 0] = product(l, c, i, 0)
        pair_copy(i, 1).start()
        total[i, 1] = product(l, c, i, 1)

    outs_load(0).wait()
    for p in range(2):
        pair_send[0, p] = product(0, 1 - c, 0, p)
        total[0, p] = product(0, c, 0, p)

    acts_load(1).wait()
    turn(1)
    biggest_act = jnp.maximum(jnp.max(largest(acts, 0).astype(F32)), jnp.max(largest(acts, 1).astype(F32)))
    best = largest(outs, 0)

    def widen(i, best):
        outs_load(i).wait()
        return jnp.maximum(best, largest(outs, i))

    best = lax.fori_loop(1, STEPS, widen, best)
    biggest_out = jnp.max(best.astype(F32))
    own_bound = jnp.maximum(biggest_act * biggest_out * (1.01 * tokens), 1e-30)
    bounds[dp_me] = jnp.full((8, LANES), own_bound, F32)
    bound[...] = jnp.full((8, LANES), own_bound, F32)
    mate = z * 4 + x * 2 + 1 - c

    pl.semaphore_wait(barrier, 15 + nt - 1)
    remote(bound, bounds.at[dp_me], bound_ssem, bound_rsem.at[0], to_core).start()
    for p in range(2):
        pair_copy(0, p).start()

    def bound_send(k, carry):
        other, device = dp_of(k)

        @pl.when(other != mate)
        def _():
            remote(bound, bounds.at[dp_me], bound_ssem, bound_rsem.at[1], device).start()

        return carry

    lax.fori_loop(1, 16, bound_send, 0)

    top = TOP**0.125

    def chip_scale():
        return top / (bounds[dp_me] + bounds[mate])[0:1, 0:1]

    def paired(i, p, q):
        return total[i, p, q] + pair_recv[i, p, q]

    def x1_copy(i):
        return remote(x1_send.at[i], x1_recv.at[i], x1_ssem, x1_rsem.at[i], to_x)

    def send_z(send, recv, ssem, rsem, n):
        remote(send.at[n, 0], recv.at[n, 0], ssem, rsem.at[n], to_za).start()
        remote(send.at[n, 1], recv.at[n, 1], ssem, rsem.at[n], to_zb).start()

    def zx_copy(n):
        return remote(zx_send.at[n], zx_recv.at[n], zx_ssem, zx_rsem.at[n], to_x)

    lo, hi = slice(0, HALF), slice(HALF, WIDE)

    def z_pieces(work, i):
        def one(k, carry):
            work(i + k, i, 1 - k)
            return carry

        lax.fori_loop(0, 1 + i // (STEPS - 1), one, 0)

    def x_one(i):
        scale = chip_scale()
        pair_copy(i, 0).wait_recv()
        for zz in range(4):
            x1_send[i, zz] = encode(paired(i, 0, zz * 2 + xo) * scale)
        x1_copy(i).start()

    def z_one(n, i, p):
        scale = chip_scale()
        pair_copy(i, p).wait_recv()
        for xx in range(2):
            far = encode(paired(i, p, zo * 2 + xx) * scale)
            zz1_send[n, 0, 0, xx] = far[:, lo]
            zz1_send[n, 1, 0, xx] = far[:, hi]
            q = za * 2 + xx
            zz1_send[n, 0, 1, xx] = encode((total[i, p, q, :, hi] + pair_recv[i, p, q, :, hi]) * scale)
            q = zb * 2 + xx
            zz1_send[n, 1, 1, xx] = encode((total[i, p, q, :, lo] + pair_recv[i, p, q, :, lo]) * scale)
        send_z(zz1_send, zz1_recv, zz1_ssem, zz1_rsem, n)

    def bound_of(zz, xx):
        return (bounds[zz * 4 + xx * 2] + bounds[zz * 4 + xx * 2 + 1])[0:1, 0:1]

    def scales():
        whole = jnp.sum(bounds[...], axis=0)[0:1, 0:1] * 1.01
        return top / whole, whole * (1.0 / top)

    def from_z():
        return bound_of(za, x) * (1.0 / top), bound_of(zb, x) * (1.0 / top)

    def x_two(i):
        scale, unscale = scales()
        from_x = bound_of(z, xo) * (1.0 / top)
        x1_copy(i).wait_recv()
        for zz in range(4):
            q = zz * 2 + x
            total[i, 0, q] = paired(i, 0, q) + decode(x1_recv[i, zz]) * from_x
        far = encode(total[i, 0, zo * 2 + x] * scale)
        xz1_send[i, 0, 0] = far[:, lo]
        xz1_send[i, 1, 0] = far[:, hi]
        xz1_send[i, 0, 1] = encode(total[i, 0, za * 2 + x, :, hi] * scale)
        xz1_send[i, 1, 1] = encode(total[i, 0, zb * 2 + x, :, lo] * scale)
        send_z(xz1_send, xz1_recv, xz1_ssem, xz1_rsem, i)

    def z_two(n, i, p):
        scale, unscale = scales()
        from_za, from_zb = from_z()
        arrived(zz1_recv.at[n], zz1_rsem.at[n])
        for xx in range(2):
            q = za * 2 + xx
            mine = total[i, p, q, :, lo] + pair_recv[i, p, q, :, lo]
            zz2_send[n, 0, xx] = encode((mine + decode(zz1_recv[n, 0, 0, xx]) * from_zb) * scale)
            q = zb * 2 + xx
            mine = total[i, p, q, :, hi] + pair_recv[i, p, q, :, hi]
            zz2_send[n, 1, xx] = encode((mine + decode(zz1_recv[n, 1, 0, xx]) * from_za) * scale)
        send_z(zz2_send, zz2_recv, zz2_ssem, zz2_rsem, n)

    def x_three(i):
        scale, unscale = scales()
        arrived(xz1_recv.at[i], xz1_rsem.at[i])
        xz2_send[i, 0] = encode(total[i, 0, za * 2 + x, :, lo] * scale + decode(xz1_recv[i, 0, 0]))
        xz2_send[i, 1] = encode(total[i, 0, zb * 2 + x, :, hi] * scale + decode(xz1_recv[i, 1, 0]))
        send_z(xz2_send, xz2_recv, xz2_ssem, xz2_rsem, i)

    def z_three(n, i, p):
        scale, unscale = scales()
        from_za, from_zb = from_z()
        arrived(zz2_recv.at[n], zz2_rsem.at[n])

        def summed(xx):
            q = z * 2 + xx
            low = (
                total[i, p, q, :, lo] + pair_recv[i, p, q, :, lo]
                + decode(zz1_recv[n, 1, 1, xx]) * from_za + decode(zz2_recv[n, 0, xx]) * unscale
            )
            high = (
                total[i, p, q, :, hi] + pair_recv[i, p, q, :, hi]
                + decode(zz1_recv[n, 0, 1, xx]) * from_zb + decode(zz2_recv[n, 1, xx]) * unscale
            )
            return low, high

        low, high = summed(xo)
        zx_send[n, :, lo] = encode(low * scale)
        zx_send[n, :, hi] = encode(high * scale)
        zx_copy(n).start()
        low, high = summed(x)
        total[i, p, z * 2 + x, :, lo] = low
        total[i, p, z * 2 + x, :, hi] = high

    def put(i, j, value):
        base = (lax.rem(i, 4) * 4 + j) * 2 + i // 4
        for r in range(OWN // 8):
            own_grad[pl.ds(base + r * 8 * 32, 8, stride=32), :] = value[r * 8 : (r + 1) * 8]
        return jnp.sum((value * value).reshape(OWN // 8, 8, LANES), axis=0)

    def x_end(i):
        unscale = scales()[1]
        arrived(xz2_recv.at[i], xz2_rsem.at[i])
        q = z * 2 + x
        g = total[i, 0, q, :, lo] + (decode(xz1_recv[i, 1, 1]) + decode(xz2_recv[i, 0])) * unscale
        squares = squares_ref[...] + put(i, 0, g)
        g = total[i, 0, q, :, hi] + (decode(xz1_recv[i, 0, 1]) + decode(xz2_recv[i, 1])) * unscale
        squares_ref[...] = squares + put(i, 1, g)

    def z_end(n, i, p):
        unscale = scales()[1]
        zx_copy(n).wait_recv()
        g = total[i, p, z * 2 + x] + decode(zx_recv[n]) * unscale
        squares = squares_ref[...] + put(i, 2 * p, g[:, lo])
        squares_ref[...] = squares + put(i, 2 * p + 1, g[:, hi])

    def turn_of(t, carry):
        def during(lag, count, work):
            @pl.when((t >= lag) & (t < lag + count))
            def _():
                work(t - lag)

        during(0, STEPS, multiply)

        @pl.when(t == 1)
        def _():
            arrived(bound, bound_rsem.at[0])

        during(1, X_PIECES, x_one)
        during(1, STEPS, functools.partial(z_pieces, z_one))

        @pl.when(t == LAG_TWO)
        def _():
            arrived(bounds.at[pl.ds(0, 14)], bound_rsem.at[1])

        during(LAG_TWO, STEPS, functools.partial(z_pieces, z_two))
        during(LAG_THREE, STEPS, functools.partial(z_pieces, z_three))
        during(LAG_END, STEPS, functools.partial(z_pieces, z_end))
        during(LAG_TWO, X_PIECES, x_two)
        during(LAG_THREE, X_PIECES, x_three)
        during(LAG_END, X_PIECES, x_end)
        return carry

    squares_ref[...] = jnp.zeros((8, LANES), F32)
    lax.fori_loop(1, LAG_END + STEPS, turn_of, 0)

    norm_dp[dp_me] = squares_ref[...]

    def ndp_send(k, carry):
        place = norm_dp.at[dp_me]
        remote(place, place, ndp_ssem, ndp_rsem, dp_of(k)[1]).start()
        return carry

    def ntp_send(k, carry):
        place = norm_tp.at[tp_me]
        remote(place, place, ntp_ssem, ntp_rsem, tp_of(k)[1]).start()
        return carry

    for k in range(1, 16):
        ndp_send(k, 0)
    arrived(norm_dp.at[pl.ds(0, 15)], ndp_rsem)
    norm_tp[tp_me] = jnp.sum(norm_dp[...], axis=0)
    for k in range(1, nt):
        ntp_send(k, 0)
    for copy in states:
        copy.wait()
    if nt > 1:
        arrived(norm_tp.at[pl.ds(0, nt - 1)], ntp_rsem)
    sum_squares = jnp.sum(jnp.sum(norm_tp[...], axis=0), keepdims=True)
    entries = OWN * 16 * nt * 2 * 2048
    limit = limit_scale * math.sqrt(entries)
    clip_factor = limit / jnp.maximum(jnp.sqrt(sum_squares), limit)

    def update(start, count):
        rows = pl.ds(pl.multiple_of(start, 16), count)
        clipped = clip_factor * own_grad[rows, :]
        new_first = beta_first * first[rows, :] + (1.0 - beta_first) * clipped
        new_second = beta_second * second[rows, :] + (1.0 - beta_second) * clipped * clipped
        step_dir = new_first * (1.0 / first_fix) / (jnp.sqrt(new_second * (1.0 / second_fix)) + epsilon)
        old = master[rows, :]
        new_master = old - learn_rate * (step_dir + decay_rate * old)
        first_out[rows, :] = new_first
        second_out[rows, :] = new_second
        master_out[rows, :] = new_master
        weights_out[dp_me, rows, :] = new_master.astype(BF16)

    def x_part(k):
        return pl.ds(pl.multiple_of(k * X_ROWS, 16), X_ROWS)

    def z_part(k):
        return pl.ds(pl.multiple_of(GATHERS * X_ROWS + k * Z_ROWS, 16), Z_ROWS)

    def x_half(k, n):
        return pl.ds(pl.multiple_of(k * X_ROWS + n * (X_ROWS // 2), 16), X_ROWS // 2)

    def z_half(k, n):
        return pl.ds(pl.multiple_of(GATHERS * X_ROWS + k * Z_ROWS + n * (Z_ROWS // 2), 16), Z_ROWS // 2)

    def move(zz, xx, rows, ssem, rsem, device):
        place = weights_out.at[zz * 4 + xx * 2 + c, rows, :]
        return remote(place, place, ssem, rsem, device)

    def gx(k, n, zz, xx, rows):
        return move(zz, xx, rows, gx_ssem, gx_rsem.at[k, n], to_x)

    def gz(k, n, zz, xx, rows, device):
        return move(zz, xx, rows, gz_ssem, gz_rsem.at[k, n], device)

    def gd(zz, xx, rows):
        return move(zz, xx, rows, gd_ssem, gd_rsem, to_core)

    def z_cross(k, n, zz):
        gx(k, n, zz, x, z_part(k)).start()

    def blocks(count, rows):
        return weights_out.at[pl.ds(0, count), pl.ds(0, rows), :]

    def spread(k, n, xx, rows):
        gz(k, n, z, xx, rows, to_za).start()
        gz(k, n + 1, z, xx, rows, to_zb).start()

    def update_loop(k, carry):
        def in_x(s, carry):
            update(k * X_ROWS + s * X_SUB, X_SUB)
            return carry

        def in_z(s, carry):
            update(GATHERS * X_ROWS + k * Z_ROWS + s * Z_SUB, Z_SUB)
            return carry

        lax.fori_loop(0, X_ROWS // X_SUB, in_x, 0)
        gx(k, 0, z, x, x_part(k)).start()
        gd(z, x, x_part(k)).start()
        lax.fori_loop(0, Z_ROWS // Z_SUB, in_z, 0)
        spread(k, 4, x, z_part(k))
        gd(z, x, z_part(k)).start()
        return carry

    lax.fori_loop(0, GATHERS, update_loop, 0)

    def own_loop(k, carry):
        z_cross(k, 1, z)
        spread(k, 0, x, x_part(k))
        return carry

    lax.fori_loop(0, GATHERS, own_loop, 0)

    def hop_one(k):
        arrived(blocks(1, X_ROWS), gx_rsem.at[k, 0])
        spread(k, 2, xo, x_part(k))
        gd(z, xo, x_part(k)).start()
        arrived(blocks(1, Z_ROWS), gz_rsem.at[k, 4])
        gz(k, 8, zb, x, z_half(k, 0), to_za).start()
        z_cross(k, 2, zb)
        gd(zb, x, z_part(k)).start()
        arrived(blocks(1, Z_ROWS), gz_rsem.at[k, 5])
        gz(k, 8, za, x, z_half(k, 1), to_zb).start()
        z_cross(k, 3, za)
        gd(za, x, z_part(k)).start()

    def hop_two(k):
        for n, xx in ((0, x), (1, xo)):
            arrived(blocks(1, X_ROWS), gz_rsem.at[k, 2 * n])
            gz(k, 6 + n, zb, xx, x_half(k, 0), to_za).start()
            gd(zb, xx, x_part(k)).start()
            arrived(blocks(1, X_ROWS), gz_rsem.at[k, 2 * n + 1])
            gz(k, 6 + n, za, xx, x_half(k, 1), to_zb).start()
            gd(za, xx, x_part(k)).start()
        arrived(blocks(1, Z_ROWS), gz_rsem.at[k, 8])
        z_cross(k, 4, zo)
        gd(zo, x, z_part(k)).start()

    def hop_three(k):
        for n, zz in ((1, z), (2, zb), (3, za), (4, zo)):
            arrived(blocks(1, Z_ROWS), gx_rsem.at[k, n])
            gd(zz, xo, z_part(k)).start()
        for n, xx in ((6, x), (7, xo)):
            arrived(blocks(1, X_ROWS), gz_rsem.at[k, n])
            gd(zo, xx, x_part(k)).start()

    def first_hops(k, carry):
        hop_one(k)
        return carry

    lax.fori_loop(0, GATHERS, first_hops, 0)
    hop_two(0)
    hop_two(1)

    def gather_loop(k, carry):
        hop_two(k)
        hop_three(k - 2)
        return carry

    lax.fori_loop(2, GATHERS, gather_loop, 0)
    hop_three(GATHERS - 2)
    hop_three(GATHERS - 1)

    for slot in range(2):
        left(pair_send.at[slot], pair_ssem.at[slot])
    for sent, ssem in (
        (x1_send, x1_ssem), (xz1_send, xz1_ssem), (xz2_send, xz2_ssem), (zz1_send, zz1_ssem), (zz2_send, zz2_ssem),
        (zx_send, zx_ssem), (bounds.at[pl.ds(0, 15)], bound_ssem), (norm_dp.at[pl.ds(0, 15)], ndp_ssem),
        (blocks(8, GATHERS * (X_ROWS + 4 * Z_ROWS) // 8), gx_ssem), (blocks(8, GATHERS * (6 * X_ROWS + 3 * Z_ROWS) // 8), gz_ssem),
        (blocks(8, OWN * 32), gd_ssem),
    ):
        left(sent, ssem)
    if nt > 1:
        left(norm_tp.at[pl.ds(0, nt - 1)], ntp_ssem)
    arrived(blocks(8, OWN * 32), gd_rsem)


def fused(acts, grads, master, first, second):
    tokens = acts.shape[1]
    rows = OWN * 32
    dma = pltpu.SemaphoreType.DMA
    vmem = pltpu.VMEM
    scratch = [
        vmem((2, tokens, 1024), BF16),
        vmem((2, 2, 512, tokens), BF16),
        vmem((STEPS, tokens, 2 * WIDE), BF16),
        vmem((rows, LANES), F32),
        vmem((rows, LANES), F32),
        vmem((rows, LANES), F32),
        vmem((rows, LANES), F32),
        vmem((2, 2, 8, OWN, WIDE), F32),
        vmem((STEPS, 2, 8, OWN, WIDE), F32),
        vmem((STEPS, 2, 8, OWN, WIDE), F32),
    ]
    for shape in (
        (X_PIECES, 4, OWN, WIDE),
        (X_PIECES, 2, 2, OWN, HALF),
        (X_PIECES, 2, OWN, HALF),
        (Z_PIECES, 2, 2, 2, OWN, HALF),
        (Z_PIECES, 2, 2, OWN, HALF),
        (Z_PIECES, OWN, WIDE),
    ):
        scratch += [vmem(shape, BF16), vmem(shape, BF16)]
    tp = lax.axis_size("tp_0") * lax.axis_size("tp_1")
    scratch += [
        vmem((8, LANES), F32),
        vmem((16, 8, LANES), F32),
        vmem((16, 8, LANES), F32),
        vmem((tp, 8, LANES), F32),
        vmem((8, LANES), F32),
        dma((2,)), dma((STEPS,)), dma((3,)),
        dma((2,)), dma((STEPS, 2)),
        dma, dma((X_PIECES,)),
        dma, dma((X_PIECES,)),
        dma, dma((X_PIECES,)),
        dma, dma((Z_PIECES,)),
        dma, dma((Z_PIECES,)),
        dma, dma((Z_PIECES,)),
        dma, dma((2,)),
        dma, dma,
        dma, dma,
        dma, dma((GATHERS, 5)),
        dma, dma((GATHERS, 9)),
        dma, dma,
    ]
    anywhere = pl.BlockSpec(memory_space=pl.ANY)
    inside = pl.BlockSpec(memory_space=pltpu.VMEM)
    return pl.pallas_call(
        kernel,
        out_shape=(
            vmem((rows, LANES), F32),
            vmem((rows, LANES), F32),
            vmem((rows, LANES), F32),
            vmem((16, rows, LANES), BF16),
        ),
        in_specs=[anywhere] * 5,
        out_specs=(inside,) * 4,
        scratch_shapes=scratch,
        compiler_params=pltpu.CompilerParams(
            collective_id=0, has_side_effects=True, vmem_limit_bytes=50 * 1024 * 1024
        ),
    )(acts, grads, master, first, second)


def store_kernel(master, first, second, weights, master_out, first_out, second_out, weights_out, sems):
    copies = [
        pltpu.make_async_copy(weights.at[pl.ds(4 * n, 4)], weights_out.at[pl.ds(4 * n, 4)], sems.at[n])
        for n in range(4)
    ]
    for n, (value, out) in enumerate(((master, master_out), (first, first_out), (second, second_out))):
        copies.append(pltpu.make_async_copy(value, out, sems.at[4 + n]))
    for copy in copies:
        copy.start()
    for copy in copies:
        copy.wait()


def stored(master, first, second, weights):
    return pl.pallas_call(
        store_kernel,
        out_shape=tuple(jax.ShapeDtypeStruct(v.shape, v.dtype) for v in (master, first, second, weights)),
        in_specs=[pl.BlockSpec(memory_space=pltpu.VMEM)] * 4,
        out_specs=(pl.BlockSpec(memory_space=pltpu.HBM),) * 4,
        scratch_shapes=[pltpu.SemaphoreType.DMA((7,))],
        compiler_params=pltpu.CompilerParams(vmem_limit_bytes=2 * 1024 * 1024),
    )(master, first, second, weights)


def to_rows(array):
    own = array.shape[0]
    return array.reshape(own, 2, 16, LANES).swapaxes(1, 2).reshape(own * 32, LANES)


def from_rows(array):
    own = array.shape[0] // 32
    return array.reshape(own, 16, 2, LANES).swapaxes(1, 2).reshape(own, 2, 2048)


def on_device(activations, out_grads, master, first_moment, second_moment):
    new_master, new_first, new_second, weights = stored(
        *fused(activations, out_grads, to_rows(master), to_rows(first_moment), to_rows(second_moment))
    )
    return (
        from_rows(new_master),
        from_rows(new_first),
        from_rows(new_second),
        from_rows(weights.reshape(-1, LANES)),
    )


def solution(mesh):
    finer = Mesh(mesh.devices.reshape(4, 2, 4, 2, 2), ("tp_0", "tp_1", "dp_0", "dp_1", "dp_2"))
    in_specs = (
        P(None, DP, TP),
        P(None, DP, None),
        P(TP_DP, None, None),
        P(TP_DP, None, None),
        P(TP_DP, None, None),
    )
    out_specs = (
        P(TP_DP, None, None),
        P(TP_DP, None, None),
        P(TP_DP, None, None),
        P(TP, None, None),
    )
    return jax.shard_map(
        on_device, mesh=finer, in_specs=in_specs, out_specs=out_specs, check_vma=False
    )
```

```python
import functools
import math

import jax
import jax.numpy as jnp
from jax import lax
from jax.experimental import pallas as pl
from jax.experimental.pallas import tpu as pltpu
from jax.sharding import Mesh
from jax.sharding import PartitionSpec as P

DP = ("dp_0", "dp_1", "dp_2")
TP_DP = ("tp_0", "tp_1", "dp_0", "dp_1", "dp_2")
TP = ("tp_0", "tp_1")
MESH = pl.DeviceIdType.MESH
F32 = jnp.float32
BF16 = jnp.bfloat16


beta_first = 0.9
beta_second = 0.95
first_fix = 1.0 - 0.9**10
second_fix = 1.0 - 0.95**10
learn_rate = 0.01
decay_rate = 0.1
epsilon = 1e-08
limit_scale = 2.0

OWN = 64
WIDE = 256
HALF = WIDE // 2
STEPS = 8
X_PIECES = STEPS - 1
Z_PIECES = STEPS + 1
LANES = 128
GATHERS = 2
X_ROWS = 576
Z_ROWS = 448
X_SUB = 96
Z_SUB = 112
LAG_TWO = 3
LAG_THREE = 5
LAG_END = 8
TOP = 2.0**120
TINY = 1e-37


def encode(value):
    square = value * value
    fourth = square * square
    return (fourth * (square * (value * jnp.abs(value)))).astype(BF16)


def decode(code):
    power = code.astype(F32)
    half = lax.rsqrt(jnp.maximum(jnp.abs(power), TINY))
    eighth = lax.rsqrt(lax.rsqrt(half))
    return (power * half) * (eighth * (eighth * eighth))


def kernel(
    acts_hbm, grads_hbm, master_hbm, first_hbm, second_hbm,
    master_out, first_out, second_out, weights_out,
    acts, turned, outs, master, first, second, own_grad,
    pair_send, pair_recv, total,
    x1_send, x1_recv, xz1_send, xz1_recv, xz2_send, xz2_recv,
    zz1_send, zz1_recv, zz2_send, zz2_recv, zx_send, zx_recv,
    bound, bounds, norm_dp, norm_tp, squares_ref,
    load_sem, out_sem, state_sem, pair_ssem, pair_rsem, x1_ssem, x1_rsem, xz1_ssem, xz1_rsem, xz2_ssem, xz2_rsem,
    zz1_ssem, zz1_rsem, zz2_ssem, zz2_rsem, zx_ssem, zx_rsem,
    bound_ssem, bound_rsem, ndp_ssem, ndp_rsem, ntp_ssem, ntp_rsem,
    gx_ssem, gx_rsem, gz_ssem, gz_rsem, gd_ssem, gd_rsem,
):
    ny, nh = lax.axis_size("tp_0"), lax.axis_size("tp_1")
    y, h = lax.axis_index("tp_0"), lax.axis_index("tp_1")
    z, x, c = lax.axis_index("dp_0"), lax.axis_index("dp_1"), lax.axis_index("dp_2")
    nt = ny * nh
    dp_me = z * 4 + x * 2 + c
    tp_me = y * nh + h
    za, zb, zo = lax.rem(z + 1, 4), lax.rem(z + 3, 4), lax.rem(z + 2, 4)
    xo = 1 - x
    tokens = acts_hbm.shape[1]
    to_core = {"dp_2": 1 - c}
    to_x = {"dp_1": xo}
    to_za = {"dp_0": za}
    to_zb = {"dp_0": zb}

    def dp_of(k):
        other = lax.rem(dp_me + k, 16)
        return other, {"dp_0": other // 4, "dp_1": lax.rem(other // 2, 2), "dp_2": lax.rem(other, 2)}

    def tp_of(k):
        other = lax.rem(tp_me + k, nt)
        return other, {"tp_0": other // nh, "tp_1": lax.rem(other, nh)}

    def remote(src, dst, ssem, rsem, device):
        return pltpu.make_async_remote_copy(
            src_ref=src, dst_ref=dst, send_sem=ssem, recv_sem=rsem, device_id=device, device_id_type=MESH
        )

    def arrived(ref, rsem):
        remote(ref, ref, gd_ssem, rsem, to_core).wait_recv()

    def left(ref, ssem):
        remote(ref, ref, ssem, gd_rsem, to_core).wait_send()

    def acts_load(l):
        return pltpu.make_async_copy(acts_hbm.at[l], acts.at[l], load_sem.at[l])

    def outs_load(i):
        return pltpu.make_async_copy(
            grads_hbm.at[i // 4, :, pl.ds(pl.multiple_of(lax.rem(i, 4) * (2 * WIDE), 2 * WIDE), 2 * WIDE)],
            outs.at[i],
            out_sem.at[i],
        )

    states = (
        pltpu.make_async_copy(master_hbm, master, state_sem.at[0]),
        pltpu.make_async_copy(first_hbm, first, state_sem.at[1]),
        pltpu.make_async_copy(second_hbm, second, state_sem.at[2]),
    )
    acts_load(0).start()
    outs_load(0).start()
    acts_load(1).start()

    def start_outs(i, carry):
        outs_load(i).start()
        return carry

    lax.fori_loop(1, STEPS, start_outs, 0)
    for copy in states:
        copy.start()

    barrier = pltpu.get_barrier_semaphore()

    def greet_dp(k, carry):
        pl.semaphore_signal(barrier, inc=1, device_id=dp_of(k)[1], device_id_type=MESH)
        return carry

    def greet_tp(k, carry):
        pl.semaphore_signal(barrier, inc=1, device_id=tp_of(k)[1], device_id_type=MESH)
        return carry

    lax.fori_loop(1, 16, greet_dp, 0)
    lax.fori_loop(1, nt, greet_tp, 0)

    def turn(l):
        for q in range(8):
            flipped = acts[l, :, q * LANES : (q + 1) * LANES].T
            turned[l, 0, q * OWN : (q + 1) * OWN, :] = flipped[:OWN]
            turned[l, 1, q * OWN : (q + 1) * OWN, :] = flipped[OWN:]

    def largest(ref, lead):
        rows, wide = ref.shape[1], ref.shape[2]

        def step(r, best):
            part = jnp.abs(ref[lead, pl.ds(pl.multiple_of(r * 64, 64), 64), :])
            return jnp.maximum(best, jnp.max(part.reshape(4, 16, wide), axis=0))

        return lax.fori_loop(0, rows // 64, step, jnp.zeros((16, wide), BF16))

    acts_load(0).wait()
    turn(0)

    def product(l, core, i, p):
        return jnp.dot(
            turned[l, core], outs[i, :, p * WIDE : (p + 1) * WIDE], preferred_element_type=F32
        ).reshape(8, OWN, WIDE)

    def pair_copy(i, p):
        slot = lax.rem(i, 2)
        return remote(pair_send.at[slot, p], pair_recv.at[i, p], pair_ssem.at[slot], pair_rsem.at[i, p], to_core)

    def multiply(i):
        l = i // 4
        slot = lax.rem(i, 2)

        @pl.when(i >= 2)
        def _():
            left(pair_send.at[slot], pair_ssem.at[slot])

        pair_send[slot, 0] = product(l, 1 - c, i, 0)
        pair_send[slot, 1] = product(l, 1 - c, i, 1)
        pair_copy(i, 0).start()
        total[i, 0] = product(l, c, i, 0)
        pair_copy(i, 1).start()
        total[i, 1] = product(l, c, i, 1)

    outs_load(0).wait()
    for p in range(2):
        pair_send[0, p] = product(0, 1 - c, 0, p)
        total[0, p] = product(0, c, 0, p)

    acts_load(1).wait()
    turn(1)
    biggest_act = jnp.maximum(jnp.max(largest(acts, 0).astype(F32)), jnp.max(largest(acts, 1).astype(F32)))
    best = largest(outs, 0)

    def widen(i, best):
        outs_load(i).wait()
        return jnp.maximum(best, largest(outs, i))

    best = lax.fori_loop(1, STEPS, widen, best)
    biggest_out = jnp.max(best.astype(F32))
    own_bound = jnp.maximum(biggest_act * biggest_out * (1.01 * tokens), 1e-30)
    bounds[dp_me] = jnp.full((8, LANES), own_bound, F32)
    bound[...] = jnp.full((8, LANES), own_bound, F32)
    mate = z * 4 + x * 2 + 1 - c

    pl.semaphore_wait(barrier, 15 + nt - 1)
    remote(bound, bounds.at[dp_me], bound_ssem, bound_rsem.at[0], to_core).start()
    for p in range(2):
        pair_copy(0, p).start()

    def bound_send(k, carry):
        other, device = dp_of(k)

        @pl.when(other != mate)
        def _():
            remote(bound, bounds.at[dp_me], bound_ssem, bound_rsem.at[1], device).start()

        return carry

    lax.fori_loop(1, 16, bound_send, 0)

    top = TOP**0.125

    def chip_scale():
        return top / (bounds[dp_me] + bounds[mate])[0:1, 0:1]

    def paired(i, p, q):
        return total[i, p, q] + pair_recv[i, p, q]

    def x1_copy(i):
        return remote(x1_send.at[i], x1_recv.at[i], x1_ssem, x1_rsem.at[i], to_x)

    def send_z(send, recv, ssem, rsem, n):
        remote(send.at[n, 0], recv.at[n, 0], ssem, rsem.at[n], to_za).start()
        remote(send.at[n, 1], recv.at[n, 1], ssem, rsem.at[n], to_zb).start()

    def zx_copy(n):
        return remote(zx_send.at[n], zx_recv.at[n], zx_ssem, zx_rsem.at[n], to_x)

    lo, hi = slice(0, HALF), slice(HALF, WIDE)

    def z_pieces(work, i):
        def one(k, carry):
            work(i + k, i, 1 - k)
            return carry

        lax.fori_loop(0, 1 + i // (STEPS - 1), one, 0)

    def x_one(i):
        scale = chip_scale()
        pair_copy(i, 0).wait_recv()
        for zz in range(4):
            x1_send[i, zz] = encode(paired(i, 0, zz * 2 + xo) * scale)
        x1_copy(i).start()

    def z_one(n, i, p):
        scale = chip_scale()
        pair_copy(i, p).wait_recv()
        for xx in range(2):
            far = encode(paired(i, p, zo * 2 + xx) * scale)
            zz1_send[n, 0, 0, xx] = far[:, lo]
            zz1_send[n, 1, 0, xx] = far[:, hi]
            q = za * 2 + xx
            zz1_send[n, 0, 1, xx] = encode((total[i, p, q, :, hi] + pair_recv[i, p, q, :, hi]) * scale)
            q = zb * 2 + xx
            zz1_send[n, 1, 1, xx] = encode((total[i, p, q, :, lo] + pair_recv[i, p, q, :, lo]) * scale)
        send_z(zz1_send, zz1_recv, zz1_ssem, zz1_rsem, n)

    def bound_of(zz, xx):
        return (bounds[zz * 4 + xx * 2] + bounds[zz * 4 + xx * 2 + 1])[0:1, 0:1]

    def scales():
        whole = jnp.sum(bounds[...], axis=0)[0:1, 0:1] * 1.01
        return top / whole, whole * (1.0 / top)

    def from_z():
        return bound_of(za, x) * (1.0 / top), bound_of(zb, x) * (1.0 / top)

    def x_two(i):
        scale, unscale = scales()
        from_x = bound_of(z, xo) * (1.0 / top)
        x1_copy(i).wait_recv()
        for zz in range(4):
            q = zz * 2 + x
            total[i, 0, q] = paired(i, 0, q) + decode(x1_recv[i, zz]) * from_x
        far = encode(total[i, 0, zo * 2 + x] * scale)
        xz1_send[i, 0, 0] = far[:, lo]
        xz1_send[i, 1, 0] = far[:, hi]
        xz1_send[i, 0, 1] = encode(total[i, 0, za * 2 + x, :, hi] * scale)
        xz1_send[i, 1, 1] = encode(total[i, 0, zb * 2 + x, :, lo] * scale)
        send_z(xz1_send, xz1_recv, xz1_ssem, xz1_rsem, i)

    def z_two(n, i, p):
        scale, unscale = scales()
        from_za, from_zb = from_z()
        arrived(zz1_recv.at[n], zz1_rsem.at[n])
        for xx in range(2):
            q = za * 2 + xx
            mine = total[i, p, q, :, lo] + pair_recv[i, p, q, :, lo]
            zz2_send[n, 0, xx] = encode((mine + decode(zz1_recv[n, 0, 0, xx]) * from_zb) * scale)
            q = zb * 2 + xx
            mine = total[i, p, q, :, hi] + pair_recv[i, p, q, :, hi]
            zz2_send[n, 1, xx] = encode((mine + decode(zz1_recv[n, 1, 0, xx]) * from_za) * scale)
        send_z(zz2_send, zz2_recv, zz2_ssem, zz2_rsem, n)

    def x_three(i):
        scale, unscale = scales()
        arrived(xz1_recv.at[i], xz1_rsem.at[i])
        xz2_send[i, 0] = encode(total[i, 0, za * 2 + x, :, lo] * scale + decode(xz1_recv[i, 0, 0]))
        xz2_send[i, 1] = encode(total[i, 0, zb * 2 + x, :, hi] * scale + decode(xz1_recv[i, 1, 0]))
        send_z(xz2_send, xz2_recv, xz2_ssem, xz2_rsem, i)

    def z_three(n, i, p):
        scale, unscale = scales()
        from_za, from_zb = from_z()
        arrived(zz2_recv.at[n], zz2_rsem.at[n])

        def summed(xx):
            q = z * 2 + xx
            low = (
                total[i, p, q, :, lo] + pair_recv[i, p, q, :, lo]
                + decode(zz1_recv[n, 1, 1, xx]) * from_za + decode(zz2_recv[n, 0, xx]) * unscale
            )
            high = (
                total[i, p, q, :, hi] + pair_recv[i, p, q, :, hi]
                + decode(zz1_recv[n, 0, 1, xx]) * from_zb + decode(zz2_recv[n, 1, xx]) * unscale
            )
            return low, high

        low, high = summed(xo)
        zx_send[n, :, lo] = encode(low * scale)
        zx_send[n, :, hi] = encode(high * scale)
        zx_copy(n).start()
        low, high = summed(x)
        total[i, p, z * 2 + x, :, lo] = low
        total[i, p, z * 2 + x, :, hi] = high

    def put(i, j, value):
        base = (lax.rem(i, 4) * 4 + j) * 2 + i // 4
        for r in range(OWN // 8):
            own_grad[pl.ds(base + r * 8 * 32, 8, stride=32), :] = value[r * 8 : (r + 1) * 8]
        return jnp.sum((value * value).reshape(OWN // 8, 8, LANES), axis=0)

    def x_end(i):
        unscale = scales()[1]
        arrived(xz2_recv.at[i], xz2_rsem.at[i])
        q = z * 2 + x
        g = total[i, 0, q, :, lo] + (decode(xz1_recv[i, 1, 1]) + decode(xz2_recv[i, 0])) * unscale
        squares = squares_ref[...] + put(i, 0, g)
        g = total[i, 0, q, :, hi] + (decode(xz1_recv[i, 0, 1]) + decode(xz2_recv[i, 1])) * unscale
        squares_ref[...] = squares + put(i, 1, g)

    def z_end(n, i, p):
        unscale = scales()[1]
        zx_copy(n).wait_recv()
        g = total[i, p, z * 2 + x] + decode(zx_recv[n]) * unscale
        squares = squares_ref[...] + put(i, 2 * p, g[:, lo])
        squares_ref[...] = squares + put(i, 2 * p + 1, g[:, hi])

    def turn_of(t, carry):
        def during(lag, count, work):
            @pl.when((t >= lag) & (t < lag + count))
            def _():
                work(t - lag)

        during(0, STEPS, multiply)

        @pl.when(t == 1)
        def _():
            arrived(bound, bound_rsem.at[0])

        during(1, X_PIECES, x_one)
        during(1, STEPS, functools.partial(z_pieces, z_one))

        @pl.when(t == LAG_TWO)
        def _():
            arrived(bounds.at[pl.ds(0, 14)], bound_rsem.at[1])

        during(LAG_TWO, STEPS, functools.partial(z_pieces, z_two))
        during(LAG_THREE, STEPS, functools.partial(z_pieces, z_three))
        during(LAG_END, STEPS, functools.partial(z_pieces, z_end))
        during(LAG_TWO, X_PIECES, x_two)
        during(LAG_THREE, X_PIECES, x_three)
        during(LAG_END, X_PIECES, x_end)
        return carry

    squares_ref[...] = jnp.zeros((8, LANES), F32)
    lax.fori_loop(1, LAG_END + STEPS, turn_of, 0)

    norm_dp[dp_me] = squares_ref[...]

    def ndp_send(k, carry):
        place = norm_dp.at[dp_me]
        remote(place, place, ndp_ssem, ndp_rsem, dp_of(k)[1]).start()
        return carry

    def ntp_send(k, carry):
        place = norm_tp.at[tp_me]
        remote(place, place, ntp_ssem, ntp_rsem, tp_of(k)[1]).start()
        return carry

    for k in range(1, 16):
        ndp_send(k, 0)
    arrived(norm_dp.at[pl.ds(0, 15)], ndp_rsem)
    norm_tp[tp_me] = jnp.sum(norm_dp[...], axis=0)
    for k in range(1, nt):
        ntp_send(k, 0)
    for copy in states:
        copy.wait()
    if nt > 1:
        arrived(norm_tp.at[pl.ds(0, nt - 1)], ntp_rsem)
    sum_squares = jnp.sum(jnp.sum(norm_tp[...], axis=0), keepdims=True)
    entries = OWN * 16 * nt * 2 * 2048
    limit = limit_scale * math.sqrt(entries)
    clip_factor = limit / jnp.maximum(jnp.sqrt(sum_squares), limit)

    def update(start, count):
        rows = pl.ds(pl.multiple_of(start, 16), count)
        clipped = clip_factor * own_grad[rows, :]
        new_first = beta_first * first[rows, :] + (1.0 - beta_first) * clipped
        new_second = beta_second * second[rows, :] + (1.0 - beta_second) * clipped * clipped
        step_dir = new_first * (1.0 / first_fix) / (jnp.sqrt(new_second * (1.0 / second_fix)) + epsilon)
        old = master[rows, :]
        new_master = old - learn_rate * (step_dir + decay_rate * old)
        first_out[rows, :] = new_first
        second_out[rows, :] = new_second
        master_out[rows, :] = new_master
        weights_out[dp_me, rows, :] = new_master.astype(BF16)

    def x_part(k):
        return pl.ds(pl.multiple_of(k * X_ROWS, 16), X_ROWS)

    def z_part(k):
        return pl.ds(pl.multiple_of(GATHERS * X_ROWS + k * Z_ROWS, 16), Z_ROWS)

    def x_half(k, n):
        return pl.ds(pl.multiple_of(k * X_ROWS + n * (X_ROWS // 2), 16), X_ROWS // 2)

    def z_half(k, n):
        return pl.ds(pl.multiple_of(GATHERS * X_ROWS + k * Z_ROWS + n * (Z_ROWS // 2), 16), Z_ROWS // 2)

    def move(zz, xx, rows, ssem, rsem, device):
        place = weights_out.at[zz * 4 + xx * 2 + c, rows, :]
        return remote(place, place, ssem, rsem, device)

    def gx(k, n, zz, xx, rows):
        return move(zz, xx, rows, gx_ssem, gx_rsem.at[k, n], to_x)

    def gz(k, n, zz, xx, rows, device):
        return move(zz, xx, rows, gz_ssem, gz_rsem.at[k, n], device)

    def gd(zz, xx, rows):
        return move(zz, xx, rows, gd_ssem, gd_rsem, to_core)

    def z_cross(k, n, zz):
        gx(k, n, zz, x, z_part(k)).start()

    def blocks(count, rows):
        return weights_out.at[pl.ds(0, count), pl.ds(0, rows), :]

    def spread(k, n, xx, rows):
        gz(k, n, z, xx, rows, to_za).start()
        gz(k, n + 1, z, xx, rows, to_zb).start()

    def update_loop(k, carry):
        def in_x(s, carry):
            update(k * X_ROWS + s * X_SUB, X_SUB)
            return carry

        def in_z(s, carry):
            update(GATHERS * X_ROWS + k * Z_ROWS + s * Z_SUB, Z_SUB)
            return carry

        lax.fori_loop(0, X_ROWS // X_SUB, in_x, 0)
        gx(k, 0, z, x, x_part(k)).start()
        gd(z, x, x_part(k)).start()
        lax.fori_loop(0, Z_ROWS // Z_SUB, in_z, 0)
        spread(k, 4, x, z_part(k))
        gd(z, x, z_part(k)).start()
        return carry

    lax.fori_loop(0, GATHERS, update_loop, 0)

    def own_loop(k, carry):
        z_cross(k, 1, z)
        spread(k, 0, x, x_part(k))
        return carry

    lax.fori_loop(0, GATHERS, own_loop, 0)

    def hop_one(k):
        arrived(blocks(1, X_ROWS), gx_rsem.at[k, 0])
        spread(k, 2, xo, x_part(k))
        gd(z, xo, x_part(k)).start()
        arrived(blocks(1, Z_ROWS), gz_rsem.at[k, 4])
        gz(k, 8, zb, x, z_half(k, 0), to_za).start()
        z_cross(k, 2, zb)
        gd(zb, x, z_part(k)).start()
        arrived(blocks(1, Z_ROWS), gz_rsem.at[k, 5])
        gz(k, 8, za, x, z_half(k, 1), to_zb).start()
        z_cross(k, 3, za)
        gd(za, x, z_part(k)).start()

    def hop_two(k):
        for n, xx in ((0, x), (1, xo)):
            arrived(blocks(1, X_ROWS), gz_rsem.at[k, 2 * n])
            gz(k, 6 + n, zb, xx, x_half(k, 0), to_za).start()
            gd(zb, xx, x_part(k)).start()
            arrived(blocks(1, X_ROWS), gz_rsem.at[k, 2 * n + 1])
            gz(k, 6 + n, za, xx, x_half(k, 1), to_zb).start()
            gd(za, xx, x_part(k)).start()
        arrived(blocks(1, Z_ROWS), gz_rsem.at[k, 8])
        z_cross(k, 4, zo)
        gd(zo, x, z_part(k)).start()

    def hop_three(k):
        for n, zz in ((1, z), (2, zb), (3, za), (4, zo)):
            arrived(blocks(1, Z_ROWS), gx_rsem.at[k, n])
            gd(zz, xo, z_part(k)).start()
        for n, xx in ((6, x), (7, xo)):
            arrived(blocks(1, X_ROWS), gz_rsem.at[k, n])
            gd(zo, xx, x_part(k)).start()

    def first_hops(k, carry):
        hop_one(k)
        return carry

    lax.fori_loop(0, GATHERS, first_hops, 0)
    hop_two(0)
    hop_two(1)

    def gather_loop(k, carry):
        hop_two(k)
        hop_three(k - 2)
        return carry

    lax.fori_loop(2, GATHERS, gather_loop, 0)
    hop_three(GATHERS - 2)
    hop_three(GATHERS - 1)

    for slot in range(2):
        left(pair_send.at[slot], pair_ssem.at[slot])
    for sent, ssem in (
        (x1_send, x1_ssem), (xz1_send, xz1_ssem), (xz2_send, xz2_ssem), (zz1_send, zz1_ssem), (zz2_send, zz2_ssem),
        (zx_send, zx_ssem), (bounds.at[pl.ds(0, 15)], bound_ssem), (norm_dp.at[pl.ds(0, 15)], ndp_ssem),
        (blocks(8, GATHERS * (X_ROWS + 4 * Z_ROWS) // 8), gx_ssem), (blocks(8, GATHERS * (6 * X_ROWS + 3 * Z_ROWS) // 8), gz_ssem),
        (blocks(8, OWN * 32), gd_ssem),
    ):
        left(sent, ssem)
    if nt > 1:
        left(norm_tp.at[pl.ds(0, nt - 1)], ntp_ssem)
    arrived(blocks(8, OWN * 32), gd_rsem)


def fused(acts, grads, master, first, second):
    tokens = acts.shape[1]
    rows = OWN * 32
    dma = pltpu.SemaphoreType.DMA
    vmem = pltpu.VMEM
    scratch = [
        vmem((2, tokens, 1024), BF16),
        vmem((2, 2, 512, tokens), BF16),
        vmem((STEPS, tokens, 2 * WIDE), BF16),
        vmem((rows, LANES), F32),
        vmem((rows, LANES), F32),
        vmem((rows, LANES), F32),
        vmem((rows, LANES), F32),
        vmem((2, 2, 8, OWN, WIDE), F32),
        vmem((STEPS, 2, 8, OWN, WIDE), F32),
        vmem((STEPS, 2, 8, OWN, WIDE), F32),
    ]
    for shape in (
        (X_PIECES, 4, OWN, WIDE),
        (X_PIECES, 2, 2, OWN, HALF),
        (X_PIECES, 2, OWN, HALF),
        (Z_PIECES, 2, 2, 2, OWN, HALF),
        (Z_PIECES, 2, 2, OWN, HALF),
        (Z_PIECES, OWN, WIDE),
    ):
        scratch += [vmem(shape, BF16), vmem(shape, BF16)]
    tp = lax.axis_size("tp_0") * lax.axis_size("tp_1")
    scratch += [
        vmem((8, LANES), F32),
        vmem((16, 8, LANES), F32),
        vmem((16, 8, LANES), F32),
        vmem((tp, 8, LANES), F32),
        vmem((8, LANES), F32),
        dma((2,)), dma((STEPS,)), dma((3,)),
        dma((2,)), dma((STEPS, 2)),
        dma, dma((X_PIECES,)),
        dma, dma((X_PIECES,)),
        dma, dma((X_PIECES,)),
        dma, dma((Z_PIECES,)),
        dma, dma((Z_PIECES,)),
        dma, dma((Z_PIECES,)),
        dma, dma((2,)),
        dma, dma,
        dma, dma,
        dma, dma((GATHERS, 5)),
        dma, dma((GATHERS, 9)),
        dma, dma,
    ]
    anywhere = pl.BlockSpec(memory_space=pl.ANY)
    inside = pl.BlockSpec(memory_space=pltpu.VMEM)
    return pl.pallas_call(
        kernel,
        out_shape=(
            vmem((rows, LANES), F32),
            vmem((rows, LANES), F32),
            vmem((rows, LANES), F32),
            vmem((16, rows, LANES), BF16),
        ),
        in_specs=[anywhere] * 5,
        out_specs=(inside,) * 4,
        scratch_shapes=scratch,
        compiler_params=pltpu.CompilerParams(
            collective_id=0, has_side_effects=True, vmem_limit_bytes=50 * 1024 * 1024
        ),
    )(acts, grads, master, first, second)


def store_kernel(master, first, second, weights, master_out, first_out, second_out, weights_out, sems):
    copies = [
        pltpu.make_async_copy(weights.at[pl.ds(4 * n, 4)], weights_out.at[pl.ds(4 * n, 4)], sems.at[n])
        for n in range(4)
    ]
    for n, (value, out) in enumerate(((master, master_out), (first, first_out), (second, second_out))):
        copies.append(pltpu.make_async_copy(value, out, sems.at[4 + n]))
    for copy in copies:
        copy.start()
    for copy in copies:
        copy.wait()


def stored(master, first, second, weights):
    return pl.pallas_call(
        store_kernel,
        out_shape=tuple(jax.ShapeDtypeStruct(v.shape, v.dtype) for v in (master, first, second, weights)),
        in_specs=[pl.BlockSpec(memory_space=pltpu.VMEM)] * 4,
        out_specs=(pl.BlockSpec(memory_space=pltpu.HBM),) * 4,
        scratch_shapes=[pltpu.SemaphoreType.DMA((7,))],
        compiler_params=pltpu.CompilerParams(vmem_limit_bytes=2 * 1024 * 1024),
    )(master, first, second, weights)


def to_rows(array):
    own = array.shape[0]
    return array.reshape(own, 2, 16, LANES).swapaxes(1, 2).reshape(own * 32, LANES)


def from_rows(array):
    own = array.shape[0] // 32
    return array.reshape(own, 16, 2, LANES).swapaxes(1, 2).reshape(own, 2, 2048)


def on_device(activations, out_grads, master, first_moment, second_moment):
    new_master, new_first, new_second, weights = stored(
        *fused(activations, out_grads, to_rows(master), to_rows(first_moment), to_rows(second_moment))
    )
    return (
        from_rows(new_master),
        from_rows(new_first),
        from_rows(new_second),
        from_rows(weights.reshape(-1, LANES)),
    )


def solution(mesh):
    finer = Mesh(mesh.devices.reshape(4, 2, 4, 2, 2), ("tp_0", "tp_1", "dp_0", "dp_1", "dp_2"))
    in_specs = (
        P(None, DP, TP),
        P(None, DP, None),
        P(TP_DP, None, None),
        P(TP_DP, None, None),
        P(TP_DP, None, None),
    )
    out_specs = (
        P(TP_DP, None, None),
        P(TP_DP, None, None),
        P(TP_DP, None, None),
        P(TP, None, None),
    )
    return jax.shard_map(
        on_device, mesh=finer, in_specs=in_specs, out_specs=out_specs, check_vma=False
    )
```
